128 devices in a mesh: ctx: 16 (over y, x), tp: 8 (over z, core).
Axes of the slice: x: 4, y: 4, z: 4, core: 2. Of those that a mesh axis runs over, the one named last changes fastest.
Arguments:
- tokens: bfloat16 [8192, 4096], P('ctx'), may hold values from -48 to 48
- w_query: bfloat16 [4096, 4096], P(None, 'tp'), may hold values from -0.09375 to 0.09375
- w_key: bfloat16 [4096, 4096], P(None, 'tp'), may hold values from -0.09375 to 0.09375
- w_value: bfloat16 [4096, 4096], P(None, 'tp'), may hold values from -0.09375 to 0.09375
- w_out: bfloat16 [4096, 4096], P('tp'), may hold values from -0.09375 to 0.09375
- block_doc: int32 [128], replicated, may hold values from 0 to 1, never falling along the last dimension, each value on 1 to 112 neighbouring positions
- grad_out: bfloat16 [8192, 4096], P('ctx', 'tp'), may hold values from -6 to 6
Outputs:
- output: bfloat16 [8192, 4096], P('ctx', 'tp')
- grad_tokens: bfloat16 [8192, 4096], P('ctx', 'tp')
- grad_query_weight: float32 [4096, 4096], P('ctx', 'tp')
- grad_key_weight: float32 [4096, 4096], P('ctx', 'tp')
- grad_value_weight: float32 [4096, 4096], P('ctx', 'tp')
- grad_out_weight: float32 [4096, 4096], P('tp', 'ctx')
The draws below stay inside these ranges and needn't reach their ends.
Inputs may be any that keep to these rules, and one draw needn't show every extreme that they name: block_doc never falls along the blocks; each document covers 1 to 112 consecutive blocks.
All inputs are finite; a program needn't handle non-finite values.
Results may differ from the reference program's by a relative error of at most 0.024.
The reference program's roundings to bfloat16 on the way count: a program that leaves them out, or rounds other values in their place, can miss the bound.
Values may be sent and summed in bfloat16 or wider, within the bound.
A program may use at most 192 MiB of HBM per device.

```python
import math
import jax
import jax.numpy as jnp
import numpy as np
from jax import lax

D = 4096
HEADS = 32
HDIM = 128
BLOCK = 64
SEQ = 8192
NBLK = 128
N_CTX = 16


def draw_tokens(key, part):
    normal_part = jnp.clip(jax.random.normal(key, (SEQ, D), jnp.float32), -6.0, 6.0)
    return normal_part.astype(jnp.bfloat16)


def level_of(own_key, shape, shards, least, top_value):
    def one(axis_at, shards_of):
        draws = jax.random.uniform(jax.random.fold_in(jax.random.fold_in(own_key, 6), axis_at), (shards_of,), jnp.float32, least / len(shards), top_value / len(shards))
        return jnp.repeat(jnp.exp(draws), shape[axis_at] // shards_of).reshape((-1,) + (1,) * (len(shape) - axis_at - 1))

    gain = one(*shards[0])
    for cut in shards[1:]:
        gain = gain * one(*cut)
    return gain


def profile(number_of, total, reach, lean):
    loads = [(1 << 20) // math.isqrt(standing ** lean) + 1 for standing in range(2, number_of + 1)]
    spare, given = total - reach - (number_of - 1), [1] * (number_of - 1)
    while spare > 0:
        candidates = [i for i in range(number_of - 1) if given[i] < reach]
        mass, budget = sum([loads[i] for i in candidates]), spare
        for i in candidates:
            extra = min(reach - given[i], max(1, budget * loads[i] // mass), spare)
            given[i] = given[i] + extra
            spare = spare - extra
    return np.array([reach] + given)


def ragged(own_key, number_of, total, reach, slope):
    if number_of == 2:
        one = jax.random.randint(own_key, (), max(1, total - reach), min(reach, total - 1) + 1)
        return jnp.stack([one, total - one])
    lengths = jnp.asarray(profile(number_of, total, reach, slope), jnp.int32)
    pairs = (number_of - 1) // 2
    giver, receiver = lengths[1:1 + 2 * pairs:2], lengths[2:2 + 2 * pairs:2]
    margin = jnp.minimum(giver - 1, reach - receiver)
    moved = jax.random.randint(jax.random.fold_in(own_key, 1), (pairs,), 0, 1 << 20) % (margin + 1)
    lengths = lengths.at[1:1 + 2 * pairs:2].set(giver - moved).at[2:2 + 2 * pairs:2].set(receiver + moved)
    return lengths[jax.random.permutation(jax.random.fold_in(own_key, 2), number_of)]


def bell_draw(key, shape, spread, limit, split=(), kind=jnp.bfloat16):
    loudness = level_of(key, shape, split, -0.22, 0.18) if split else 1.0
    entries = jax.random.normal(key, shape, jnp.float32) * spread * loudness
    return jnp.minimum(jnp.maximum(entries, -limit), limit).astype(kind)


def setup_inputs(seed: int = 0) -> dict:
    seeds = jax.random.split(jax.random.key(seed), 8)
    tokens = draw_tokens(jax.random.fold_in(seeds[7], 71), 0)
    w_query = bell_draw(seeds[1], (D, D), D ** -0.5, 0.09375, ((1, 8),))
    w_key = bell_draw(seeds[2], (D, D), D ** -0.5, 0.09375, ((1, 8),))
    w_value = bell_draw(seeds[3], (D, D), D ** -0.5, 0.09375, ((1, 8),))
    w_out = bell_draw(seeds[4], (D, D), D ** -0.5, 0.09375, ((0, 8),))
    block_doc = jnp.searchsorted(jnp.cumsum(ragged(seeds[5], 2, NBLK, NBLK - NBLK // 8, 1)), jnp.arange(NBLK), side="right").astype(jnp.int32)
    grad_out = bell_draw(seeds[6], (SEQ, D), 1.0, 6.0, ((0, 16), (1, 8)))
    return {"tokens": tokens, "w_query": w_query, "w_key": w_key, "w_value": w_value, "w_out": w_out, "block_doc": block_doc, "grad_out": grad_out}


big_negative = -1e+30

def elementwise_product(pattern, left_side, right_side):
    left_side, right_side = lax.optimization_barrier((left_side, right_side))
    return jnp.einsum(pattern, left_side.astype(jnp.float32), right_side.astype(jnp.float32), precision=lax.Precision.HIGHEST)

def attend(query_row_matrix, key_row_matrix, value_row_matrix, summary_key, summary_value, allowed, causal, score_scale_factor):
    near_scores = elementwise_product('nqhd,nkhd->nhqk', query_row_matrix, key_row_matrix) * score_scale_factor
    near_scores = jnp.where(causal[None, None], near_scores, big_negative)
    distant_score_matrix = elementwise_product('yzxo,lxo->yzxl', query_row_matrix, summary_key) * score_scale_factor
    distant_score_matrix = jnp.where(allowed[:, None, None, :], distant_score_matrix, big_negative)
    row_top = jnp.maximum(jnp.transpose(lax.optimization_barrier(jnp.max(near_scores, axis=3)), (0, 2, 1)), lax.optimization_barrier(jnp.max(distant_score_matrix, axis=3)))
    near_exp = jnp.exp(near_scores - jnp.transpose(row_top, (0, 2, 1))[..., None])
    far_exp = jnp.exp(distant_score_matrix - row_top[..., None])
    denom_sum = jnp.transpose(lax.optimization_barrier(jnp.sum(near_exp, axis=3)), (0, 2, 1)) + lax.optimization_barrier(jnp.sum(far_exp, axis=3))
    local_weight = (near_exp / jnp.transpose(denom_sum, (0, 2, 1))[..., None]).astype(jnp.bfloat16)
    distant_weight = (far_exp / denom_sum[..., None]).astype(jnp.bfloat16)
    combined_output = elementwise_product('jvyb,jbvo->jyvo', local_weight, value_row_matrix) + elementwise_product('gtuv,vuk->gtuk', distant_weight, summary_value)
    return (combined_output.astype(jnp.bfloat16), local_weight, distant_weight)

def attend_back(query_row_matrix, key_row_matrix, value_row_matrix, summary_key, summary_value, combined_output, local_weight, distant_weight, incoming_gradient, score_scale_factor):
    pair = lax.optimization_barrier((combined_output, incoming_gradient))
    row_delta = lax.optimization_barrier(jnp.sum(pair[0].astype(jnp.float32) * pair[1].astype(jnp.float32), axis=3))
    near_d = elementwise_product('nqhd,nkhd->nhqk', incoming_gradient, value_row_matrix)
    distant_gradient_term = elementwise_product('yzxo,lxo->yzxl', incoming_gradient, summary_value)
    weights = lax.optimization_barrier((local_weight, distant_weight))
    local_score_sum = (weights[0].astype(jnp.float32) * (near_d - jnp.transpose(row_delta, (0, 2, 1))[..., None])).astype(jnp.bfloat16)
    distant_score_sum = (weights[1].astype(jnp.float32) * (distant_gradient_term - row_delta[..., None])).astype(jnp.bfloat16)
    query_gradient = (elementwise_product('jvyb,jbvo->jyvo', local_score_sum, key_row_matrix) + elementwise_product('gtuv,vuk->gtuk', distant_score_sum, summary_key)) * score_scale_factor
    d_key = elementwise_product('nhqk,nqhd->nkhd', local_score_sum, query_row_matrix) * score_scale_factor
    d_value = elementwise_product('nhqk,nqhd->nkhd', local_weight, incoming_gradient)
    summary_key_gradient = elementwise_product('agwi,agwu->iwu', distant_score_sum, query_row_matrix) * score_scale_factor
    summary_value_gradient = elementwise_product('agwi,agwu->iwu', distant_weight, incoming_gradient)
    return (query_gradient, d_key, d_value, summary_key_gradient, summary_value_gradient)

def shard_sum(left_side, right_side):
    shard_rows = left_side.shape[0] // N_CTX

    def add_shard(shard_index, running):
        begin = (shard_index * shard_rows).astype(jnp.int32)
        left_part = lax.dynamic_slice_in_dim(left_side, begin, shard_rows, 0)
        right_part = lax.dynamic_slice_in_dim(right_side, begin, shard_rows, 0)
        term_rows = lax.dot_general(left_part, right_part, (((0,), (0,)), ((), ())), preferred_element_type=jnp.float32)
        term_rows = lax.optimization_barrier(term_rows.astype(jnp.bfloat16))
        return running + term_rows.astype(jnp.float32)
    start_value = jnp.zeros((left_side.shape[1], right_side.shape[1]), jnp.float32)
    return lax.fori_loop(0, N_CTX, add_shard, start_value)

def back_project(grad_rows, weight):
    return lax.dot_general(grad_rows, weight, (((1,), (1,)), ((), ())), preferred_element_type=jnp.float32)

def reference(tokens, w_query, w_key, w_value, w_out, block_doc, grad_out):
    score_scale_factor = 1.0 / math.sqrt(HDIM)
    tok_rows = tokens.shape[0]
    blocks = tok_rows // BLOCK
    block_shape = (blocks, BLOCK, HEADS, HDIM)

    def project(weight):
        return jnp.dot(tokens, weight, preferred_element_type=jnp.float32).astype(jnp.bfloat16)
    query_row_matrix = project(w_query).reshape(block_shape)
    key_row_matrix = project(w_key).reshape(block_shape)
    value_row_matrix = project(w_value).reshape(block_shape)
    summary_key = key_row_matrix[:, BLOCK - 1]
    summary_value = value_row_matrix[:, BLOCK - 1]
    block_ids = jnp.arange(blocks, dtype=jnp.int32)
    allowed = (block_ids[None, :] < block_ids[:, None]) & (block_doc[None, :] == block_doc[:, None])
    positions = jnp.arange(BLOCK, dtype=jnp.int32)
    causal = positions[None, :] <= positions[:, None]
    combined_output, local_weight, distant_weight = attend(query_row_matrix, key_row_matrix, value_row_matrix, summary_key, summary_value, allowed, causal, score_scale_factor)
    attn = combined_output.reshape(tok_rows, D)
    output = (tokens.astype(jnp.float32) + jnp.dot(attn, w_out, preferred_element_type=jnp.float32)).astype(jnp.bfloat16)
    d_attn = back_project(grad_out, w_out).astype(jnp.bfloat16)
    grads = attend_back(query_row_matrix, key_row_matrix, value_row_matrix, summary_key, summary_value, combined_output, local_weight, distant_weight, d_attn.reshape(block_shape), score_scale_factor)
    query_gradient, d_key, d_value, summary_key_gradient, summary_value_gradient = grads
    query_gradient = query_gradient.astype(jnp.bfloat16).reshape(tok_rows, D)
    d_key = d_key.at[:, BLOCK - 1].add(summary_key_gradient).astype(jnp.bfloat16).reshape(tok_rows, D)
    d_value = d_value.at[:, BLOCK - 1].add(summary_value_gradient).astype(jnp.bfloat16).reshape(tok_rows, D)
    grad_tokens = grad_out.astype(jnp.float32) + back_project(query_gradient, w_query) + back_project(d_key, w_key) + back_project(d_value, w_value)
    grad_tokens = grad_tokens.astype(jnp.bfloat16)
    return (output, grad_tokens, shard_sum(tokens, query_gradient), shard_sum(tokens, d_key), shard_sum(tokens, d_value), shard_sum(attn, grad_out))
```

```python
import math

import jax
import jax.numpy as jnp
from jax import lax
from jax.sharding import PartitionSpec as P

HDIM = 128
BLOCK = 64


big_negative = -1e30


def cut_along(shard, dim, length):
    dims = shard.shape
    blocks = shard.reshape(*dims[:dim], length, dims[dim] // length, *dims[dim + 1 :])
    return jnp.moveaxis(blocks, dim, 0)


def summed_on_arrival(shard, axis, dim):
    length = lax.axis_size(axis)
    blocks = lax.all_to_all(cut_along(shard, dim, length), axis, 0, 0, tiled=True)
    return jnp.sum(blocks, axis=0)


def in_one_piece(arrays, axis, dim, along):
    widths = [a.shape[along] for a in arrays]
    both = jnp.concatenate(arrays, axis=along)
    out = summed_on_arrival(both, axis, dim)
    return tuple(jnp.split(out, [sum(widths[:k]) for k in range(1, len(widths))], axis=along))


def sent_and_summed(shard, axis, dim):
    length = lax.axis_size(axis)
    blocks = lax.all_to_all(cut_along(shard, dim, length), axis, 0, 0, tiled=True)
    return jnp.sum(blocks.astype(jnp.float32), axis=0)


def elementwise_product(pattern, left_side, right_side):
    return jnp.einsum(pattern, left_side, right_side, preferred_element_type=jnp.float32)


def attend(
    query_row_matrix,
    key_row_matrix,
    value_row_matrix,
    summary_key,
    summary_value,
    allowed,
    causal,
    score_scale_factor,
):
    near_scores = (
        elementwise_product("nqhd,nkhd->nhqk", query_row_matrix, key_row_matrix)
        * score_scale_factor
    )
    near_scores = jnp.where(causal[None, None], near_scores, big_negative)
    distant_score_matrix = (
        elementwise_product("yzxo,lxo->yzxl", query_row_matrix, summary_key) * score_scale_factor
    )
    distant_score_matrix = jnp.where(allowed[:, None, None, :], distant_score_matrix, big_negative)
    row_top = jnp.maximum(
        jnp.transpose(jnp.max(near_scores, axis=3), (0, 2, 1)),
        jnp.max(distant_score_matrix, axis=3),
    )
    near_exp = jnp.exp(near_scores - jnp.transpose(row_top, (0, 2, 1))[..., None])
    far_exp = jnp.exp(distant_score_matrix - row_top[..., None])
    denom_sum = jnp.transpose(jnp.sum(near_exp, axis=3), (0, 2, 1)) + jnp.sum(far_exp, axis=3)
    local_weight = (near_exp / jnp.transpose(denom_sum, (0, 2, 1))[..., None]).astype(jnp.bfloat16)
    distant_weight = (far_exp / denom_sum[..., None]).astype(jnp.bfloat16)
    combined_output = elementwise_product(
        "jvyb,jbvo->jyvo", local_weight, value_row_matrix
    ) + elementwise_product("gtuv,vuk->gtuk", distant_weight, summary_value)
    return (combined_output.astype(jnp.bfloat16), local_weight, distant_weight)


def attend_back(
    query_row_matrix,
    key_row_matrix,
    value_row_matrix,
    summary_key,
    summary_value,
    combined_output,
    local_weight,
    distant_weight,
    incoming_gradient,
    score_scale_factor,
):
    row_delta = jnp.sum(
        combined_output.astype(jnp.float32) * incoming_gradient.astype(jnp.float32), axis=3
    )
    near_d = elementwise_product("nqhd,nkhd->nhqk", incoming_gradient, value_row_matrix)
    distant_gradient_term = elementwise_product("yzxo,lxo->yzxl", incoming_gradient, summary_value)
    local_score_sum = (
        local_weight.astype(jnp.float32) * (near_d - jnp.transpose(row_delta, (0, 2, 1))[..., None])
    ).astype(jnp.bfloat16)
    distant_score_sum = (
        distant_weight.astype(jnp.float32) * (distant_gradient_term - row_delta[..., None])
    ).astype(jnp.bfloat16)
    query_gradient = (
        elementwise_product("jvyb,jbvo->jyvo", local_score_sum, key_row_matrix)
        + elementwise_product("gtuv,vuk->gtuk", distant_score_sum, summary_key)
    ) * score_scale_factor
    d_key = (
        elementwise_product("nhqk,nqhd->nkhd", local_score_sum, query_row_matrix)
        * score_scale_factor
    )
    d_value = elementwise_product("nhqk,nqhd->nkhd", local_weight, incoming_gradient)
    summary_key_gradient = (
        elementwise_product("agwi,agwu->iwu", distant_score_sum, query_row_matrix)
        * score_scale_factor
    )
    summary_value_gradient = elementwise_product(
        "agwi,agwu->iwu", distant_weight, incoming_gradient
    )
    return (query_gradient, d_key, d_value, summary_key_gradient, summary_value_gradient)


def back_project(grad_rows, weight):
    return lax.dot_general(
        grad_rows, weight, (((1,), (1,)), ((), ())), preferred_element_type=jnp.float32
    )


def term_maker(tokens, grad_rows):
    return lax.dot_general(
        tokens, grad_rows, (((0,), (0,)), ((), ())), preferred_element_type=jnp.float32
    )


def per_device(tokens, w_query, w_key, w_value, w_out, block_doc, grad_out):
    score_scale_factor = 1.0 / math.sqrt(HDIM)
    tok_rows = tokens.shape[0]
    col_count = w_query.shape[1]
    blocks = tok_rows // BLOCK
    head_count = col_count // HDIM
    block_shape = (blocks, BLOCK, head_count, HDIM)

    def project(weight):
        return jnp.dot(tokens, weight, preferred_element_type=jnp.float32).astype(jnp.bfloat16)

    query_row_matrix = project(w_query).reshape(block_shape)
    key_row_matrix = project(w_key).reshape(block_shape)
    value_row_matrix = project(w_value).reshape(block_shape)
    own_key = key_row_matrix[:, BLOCK - 1].reshape(blocks, col_count)
    own_value = value_row_matrix[:, BLOCK - 1].reshape(blocks, col_count)
    own_both = jnp.concatenate([own_key, own_value], axis=1)
    summary_both = lax.all_gather(own_both, "ctx", axis=0, tiled=True)
    summary_key, summary_value = summary_both[:, :col_count], summary_both[:, col_count:]
    total_blocks = summary_key.shape[0]
    summary_key = summary_key.reshape(total_blocks, head_count, HDIM)
    summary_value = summary_value.reshape(total_blocks, head_count, HDIM)
    first_block = lax.axis_index("ctx") * blocks
    query_ids = first_block + jnp.arange(blocks, dtype=jnp.int32)
    own_doc = lax.dynamic_slice_in_dim(block_doc, first_block, blocks, 0)
    block_ids = jnp.arange(total_blocks, dtype=jnp.int32)
    allowed = (block_ids[None, :] < query_ids[:, None]) & (block_doc[None, :] == own_doc[:, None])
    positions = jnp.arange(BLOCK, dtype=jnp.int32)
    causal = positions[None, :] <= positions[:, None]
    combined_output, local_weight, distant_weight = attend(
        query_row_matrix,
        key_row_matrix,
        value_row_matrix,
        summary_key,
        summary_value,
        allowed,
        causal,
        score_scale_factor,
    )
    attn = combined_output.reshape(tok_rows, col_count)
    partial_value = jnp.dot(attn, w_out, preferred_element_type=jnp.float32)
    summed = lax.psum_scatter(
        partial_value.astype(jnp.bfloat16), "tp", scatter_dimension=1, tiled=True
    ).astype(jnp.float32)
    shard_width = summed.shape[1]
    residual = lax.dynamic_slice_in_dim(tokens, lax.axis_index("tp") * shard_width, shard_width, 1)
    output = (residual.astype(jnp.float32) + summed).astype(jnp.bfloat16)
    upstream_full = lax.all_gather(grad_out, "tp", axis=1, tiled=True)
    d_attn = back_project(upstream_full, w_out).astype(jnp.bfloat16)
    grads = attend_back(
        query_row_matrix,
        key_row_matrix,
        value_row_matrix,
        summary_key,
        summary_value,
        combined_output,
        local_weight,
        distant_weight,
        d_attn.reshape(block_shape),
        score_scale_factor,
    )
    query_gradient, d_key, d_value, summary_key_gradient, summary_value_gradient = grads
    flat_key = summary_key_gradient.reshape(total_blocks, col_count)
    flat_value = summary_value_gradient.reshape(total_blocks, col_count)
    back_key, back_value = in_one_piece((flat_key, flat_value), "ctx", 0, 1)
    query_gradient = query_gradient.astype(jnp.bfloat16).reshape(tok_rows, col_count)
    d_key = (
        d_key.at[:, BLOCK - 1]
        .add(back_key.reshape(blocks, head_count, HDIM))
        .astype(jnp.bfloat16)
        .reshape(tok_rows, col_count)
    )
    d_value = (
        d_value.at[:, BLOCK - 1]
        .add(back_value.reshape(blocks, head_count, HDIM))
        .astype(jnp.bfloat16)
        .reshape(tok_rows, col_count)
    )
    d_partial = (
        back_project(query_gradient, w_query)
        + back_project(d_key, w_key)
        + back_project(d_value, w_value)
    )
    d_summed = lax.psum_scatter(
        d_partial.astype(jnp.bfloat16), "tp", scatter_dimension=1, tiled=True
    ).astype(jnp.float32)
    grad_tokens = (grad_out.astype(jnp.float32) + d_summed).astype(jnp.bfloat16)
    stacked = jnp.concatenate([query_gradient, d_key, d_value], axis=1)
    joined = lax.psum_scatter(
        term_maker(tokens, stacked).astype(jnp.bfloat16), "ctx", scatter_dimension=0, tiled=True
    ).astype(jnp.float32)
    grad_query_weight = joined[:, :col_count]
    grad_key_weight = joined[:, col_count : 2 * col_count]
    grad_value_weight = joined[:, 2 * col_count :]
    out_term = lax.dot_general(
        attn, upstream_full, (((0,), (0,)), ((), ())), preferred_element_type=jnp.float32
    )
    grad_out_weight = sent_and_summed(out_term.astype(jnp.bfloat16), "ctx", 1)
    return (
        output,
        grad_tokens,
        grad_query_weight,
        grad_key_weight,
        grad_value_weight,
        grad_out_weight,
    )


def solution(mesh):
    in_specs = (
        P("ctx", None),
        P(None, "tp"),
        P(None, "tp"),
        P(None, "tp"),
        P("tp", None),
        P(),
        P("ctx", "tp"),
    )
    out_specs = (
        P("ctx", "tp"),
        P("ctx", "tp"),
        P("ctx", "tp"),
        P("ctx", "tp"),
        P("ctx", "tp"),
        P("tp", "ctx"),
    )
    return jax.shard_map(
        per_device, mesh=mesh, in_specs=in_specs, out_specs=out_specs, check_vma=False
    )
```

```python
import functools
import math

import jax
import jax.numpy as jnp
from jax import lax
from jax.experimental import pallas as pl
from jax.experimental.pallas import tpu as pltpu
from jax.sharding import PartitionSpec as P

HDIM = 128
BLOCK = 64
PAIR = 2 * BLOCK
MESH = pl.DeviceIdType.MESH
BF = jnp.bfloat16
F32 = jnp.float32
big_negative = -1e30


def dot_nn(a, b):
    return lax.dot_general(a, b, (((1,), (0,)), ((), ())), preferred_element_type=F32)


def dot_nt(a, b):
    return lax.dot_general(a, b, (((1,), (1,)), ((), ())), preferred_element_type=F32)


def dot_tn(a, b):
    return lax.dot_general(a, b, (((0,), (0,)), ((), ())), preferred_element_type=F32)


def iota(shape, dim):
    return lax.broadcasted_iota(jnp.int32, shape, dim)


def one_hot(hit):
    return jnp.where(hit, 1.0, 0.0).astype(BF)


def core_kernel(
    nctx,
    ntp,
    tok_h,
    wq_h,
    wk_h,
    wv_h,
    wo_h,
    doc_ref,
    go_h,
    attn_o,
    dq_o,
    dk_o,
    dv_o,
    gf_o,
    tok,
    w3,
    wo,
    qkv,
    gfull,
    land,
    lk,
    lv,
    pw,
    attn,
    da,
    dqv,
    dkv,
    dvv,
    dkf,
    dvf,
    dlk,
    dlv,
    dls,
    dlr,
    ld,
    st,
    g_s,
    g_r,
    f_s,
    l_s,
    l_r,
    d_s,
    d_r,
):
    ctx = lax.axis_index("ctx")
    tp = lax.axis_index("tp")
    nz = ntp // 2
    core = lax.rem(tp, 2)
    z = lax.div(tp, 2)
    partner = tp + 1 - 2 * core
    rows, width = tok.shape
    cols = qkv.shape[2]
    heads = cols // HDIM
    own_blocks = rows // BLOCK
    all_blocks = nctx * own_blocks
    per = 2 * own_blocks
    scale = 1.0 / math.sqrt(HDIM)

    def shard(t):
        return pl.ds(pl.multiple_of(t * cols, cols), cols)

    def mate(j, side):
        return lax.rem(z + j, nz) * 2 + side

    load_tok = pltpu.make_async_copy(tok_h, tok, ld.at[0])
    load_tok.start()
    for i, w_h in enumerate((wk_h, wv_h, wq_h)):
        pltpu.make_async_copy(w_h, w3.at[i], ld.at[1 + i]).start()
    load_wo = pltpu.make_async_copy(wo_h, wo, ld.at[4])
    load_wo.start()
    load_go = pltpu.make_async_copy(go_h, gfull.at[:, shard(tp)], ld.at[5])
    load_go.start()

    barrier = pltpu.get_barrier_semaphore()

    def greet(i, carry):
        pl.semaphore_signal(
            barrier, inc=1, device_id={"ctx": lax.rem(ctx + i, nctx)}, device_id_type=MESH
        )
        return carry

    lax.fori_loop(1, nctx, greet, 0)
    pl.semaphore_signal(barrier, inc=1, device_id={"tp": partner}, device_id_type=MESH)
    for j in range(1, nz):
        pl.semaphore_signal(barrier, inc=1, device_id={"tp": mate(j, core)}, device_id_type=MESH)
    pl.semaphore_wait(barrier, nctx - 1 + nz)

    def grad_copy(source, owner, send, target):
        return pltpu.make_async_remote_copy(
            src_ref=source,
            dst_ref=gfull.at[:, shard(owner)],
            send_sem=send,
            recv_sem=g_r.at[owner],
            device_id={"tp": target},
            device_id_type=MESH,
        )

    first_sends = [grad_copy(go_h, tp, g_s.at[j - 1], mate(j, core)) for j in range(1, nz)]
    first_sends.append(grad_copy(go_h, tp, g_s.at[nz - 1], partner))
    for send in first_sends:
        send.start()

    load_tok.wait()

    half = cols // 2

    def project(i, carry):
        pltpu.make_async_copy(wk_h, w3.at[i], ld.at[1 + i]).wait()

        def piece(n, inner):
            at = pl.ds(pl.multiple_of(n * half, half), half)
            qkv[i, :, at] = dot_nn(tok[...], w3[i, :, at]).astype(BF)
            return inner

        lax.fori_loop(0, 2, piece, 0)

        @pl.when(i == 1)
        def _():
            r = iota((per, rows), 0)
            c = iota((per, rows), 1)
            pick_k = one_hot(c == r * BLOCK + BLOCK - 1)
            pick_v = one_hot(c == (r - own_blocks) * BLOCK + BLOCK - 1)
            pick_k = jnp.where(r < own_blocks, pick_k, jnp.zeros_like(pick_k))
            pick_v = jnp.where(r >= own_blocks, pick_v, jnp.zeros_like(pick_v))
            land[ctx] = (dot_nn(pick_k, qkv[0]) + dot_nn(pick_v, qkv[1])).astype(BF)

            def spread(j, inner):
                pltpu.make_async_remote_copy(
                    src_ref=land.at[ctx],
                    dst_ref=land.at[ctx],
                    send_sem=l_s.at[j - 1],
                    recv_sem=l_r.at[ctx],
                    device_id={"ctx": lax.rem(ctx + j, nctx)},
                    device_id_type=MESH,
                ).start()
                return inner

            lax.fori_loop(1, nctx, spread, 0)

        return carry

    lax.fori_loop(0, 3, project, 0)

    def land_wait(j, carry):
        source = lax.rem(ctx + j, nctx)
        copy = pltpu.make_async_remote_copy(
            src_ref=land.at[ctx],
            dst_ref=land.at[source],
            send_sem=l_s.at[j - 1],
            recv_sem=l_r.at[source],
            device_id={"ctx": source},
            device_id_type=MESH,
        )
        copy.wait_send()
        copy.wait_recv()
        return carry

    lax.fori_loop(1, nctx, land_wait, 0)

    b = iota((all_blocks, nctx * per), 0)
    c = iota((all_blocks, nctx * per), 1)
    shift = b // own_blocks * own_blocks
    landed = land[...].reshape(nctx * per, cols)
    lk[...] = dot_nn(one_hot(c == b + shift), landed).astype(BF)
    lv[...] = dot_nn(one_hot(c == b + shift + own_blocks), landed).astype(BF)

    span = PAIR + all_blocks
    doc = doc_ref[...]
    doc_lane = iota(doc.shape, 1)
    doc_wide = jnp.concatenate([jnp.zeros((1, PAIR), jnp.int32), doc], axis=1)

    def forward(sb, carry):
        at = pl.ds(pl.multiple_of(sb * PAIR, PAIR), PAIR)
        row = iota((PAIR, span), 0)
        col = iota((PAIR, span), 1)
        upper = jnp.where(row >= BLOCK, 1, 0)
        col_upper = jnp.where(col >= BLOCK, 1, 0)
        first = ctx * own_blocks + sb * 2
        doc_a = jnp.sum(jnp.where(doc_lane == first, doc, 0), axis=1, keepdims=True)
        doc_b = jnp.sum(jnp.where(doc_lane == first + 1, doc, 0), axis=1, keepdims=True)
        own_doc = jnp.where(row >= BLOCK, doc_b, doc_a)
        near = (col < PAIR) & (upper == col_upper) & (col <= row)
        far = (col >= PAIR) & (col - PAIR < first + upper) & (doc_wide == own_doc)
        mask = near | far
        for h in range(heads):
            hs = pl.ds(h * HDIM, HDIM)
            keys = jnp.concatenate([qkv[0, at, hs], lk[:, hs]], axis=0)
            values = jnp.concatenate([qkv[1, at, hs], lv[:, hs]], axis=0)
            scores = dot_nt(qkv[2, at, hs], keys) * scale
            scores = jnp.where(mask, scores, big_negative)
            top = jnp.max(scores, axis=1, keepdims=True)
            e = jnp.exp(scores - top)
            weight = (e / jnp.sum(e, axis=1, keepdims=True)).astype(BF)
            pw[sb * heads + h] = weight
            attn[at, hs] = dot_nn(weight, values).astype(BF)
        return carry

    lax.fori_loop(0, rows // PAIR, forward, 0)
    out_attn = pltpu.make_async_copy(attn, attn_o, st.at[0])
    out_attn.start()

    forwards = []
    for j in range(1, nz):
        owner = mate(j, core)
        grad_copy(gfull.at[:, shard(owner)], owner, f_s.at[j - 1], partner).wait_recv()
        onward = grad_copy(gfull.at[:, shard(owner)], owner, f_s.at[j - 1], partner)
        onward.start()
        forwards.append(onward)
    grad_copy(go_h, partner, g_s.at[nz - 1], partner).wait_recv()
    for j in range(1, nz):
        owner = mate(j, 1 - core)
        grad_copy(gfull.at[:, shard(owner)], owner, f_s.at[j - 1], partner).wait_recv()
    load_go.wait()
    load_wo.wait()
    out_gf = pltpu.make_async_copy(gfull, gf_o, st.at[4])
    out_gf.start()

    def d_piece(n, carry):
        at = pl.ds(pl.multiple_of(n * half, half), half)
        da[:, at] = dot_nt(gfull[...], wo[at, :]).astype(BF)
        return carry

    lax.fori_loop(0, 2, d_piece, 0)

    dlk[...] = jnp.zeros_like(dlk)
    dlv[...] = jnp.zeros_like(dlv)

    def backward(sb, carry):
        at = pl.ds(pl.multiple_of(sb * PAIR, PAIR), PAIR)
        for h in range(heads):
            hs = pl.ds(h * HDIM, HDIM)
            keys = jnp.concatenate([qkv[0, at, hs], lk[:, hs]], axis=0)
            values = jnp.concatenate([qkv[1, at, hs], lv[:, hs]], axis=0)
            weight = pw[sb * heads + h]
            d_out = da[at, hs]
            delta = jnp.sum(
                attn[at, hs].astype(F32) * d_out.astype(F32), axis=1, keepdims=True
            )
            d_weight = dot_nt(d_out, values)
            ds = (weight.astype(F32) * (d_weight - delta)).astype(BF)
            dqv[at, hs] = (dot_nn(ds, keys) * scale).astype(BF)
            d_keys = dot_tn(ds, qkv[2, at, hs]) * scale
            d_values = dot_tn(weight, d_out)
            dkf[at, hs] = d_keys[:PAIR]
            dvf[at, hs] = d_values[:PAIR]
            dlk[:, hs] += d_keys[PAIR:]
            dlv[:, hs] += d_values[PAIR:]
        return carry

    lax.fori_loop(0, rows // PAIR, backward, 0)
    out_dq = pltpu.make_async_copy(dqv, dq_o, st.at[1])
    out_dq.start()

    r = iota((nctx * per, all_blocks), 0)
    b = iota((nctx * per, all_blocks), 1)
    shift = b // own_blocks * own_blocks
    packed = dot_nn(one_hot(r == b + shift), dlk[...].astype(BF)) + dot_nn(
        one_hot(r == b + shift + own_blocks), dlv[...].astype(BF)
    )
    dls[...] = packed.astype(BF).reshape(nctx, per, cols)

    def give(j, carry):
        target = lax.rem(ctx + j, nctx)
        pltpu.make_async_remote_copy(
            src_ref=dls.at[target],
            dst_ref=dlr.at[ctx],
            send_sem=d_s.at[j - 1],
            recv_sem=d_r.at[ctx],
            device_id={"ctx": target},
            device_id_type=MESH,
        ).start()
        return carry

    lax.fori_loop(1, nctx, give, 0)
    dlr[ctx] = dls[ctx]

    def take(j, carry):
        source = lax.rem(ctx + j, nctx)
        copy = pltpu.make_async_remote_copy(
            src_ref=dls.at[source],
            dst_ref=dlr.at[source],
            send_sem=d_s.at[j - 1],
            recv_sem=d_r.at[source],
            device_id={"ctx": source},
            device_id_type=MESH,
        )
        copy.wait_send()
        copy.wait_recv()
        return carry

    lax.fori_loop(1, nctx, take, 0)
    total = jnp.zeros((per, cols), F32)
    for i in range(nctx):
        total = total + dlr[i].astype(F32)
    for i in range(own_blocks):
        last = pl.ds(i * BLOCK + BLOCK - 1, 1)
        dkf[last, :] += total[i : i + 1]
        dvf[last, :] += total[own_blocks + i : own_blocks + i + 1]
    dkv[...] = dkf[...].astype(BF)
    dvv[...] = dvf[...].astype(BF)
    out_dk = pltpu.make_async_copy(dkv, dk_o, st.at[2])
    out_dk.start()
    out_dv = pltpu.make_async_copy(dvv, dv_o, st.at[3])
    out_dv.start()
    for send in first_sends + forwards:
        send.wait_send()
    for copy in (out_attn, out_dq, out_dk, out_dv, out_gf):
        copy.wait()


def attention_core(nctx, ntp, tokens, w_query, w_key, w_value, w_out, block_doc, grad_out):
    rows, width = tokens.shape
    cols = w_query.shape[1]
    heads = cols // HDIM
    own_blocks = rows // BLOCK
    all_blocks = nctx * own_blocks
    per = 2 * own_blocks
    units = rows // PAIR * heads
    small = jax.ShapeDtypeStruct((rows, cols), BF)
    hbm = pl.BlockSpec(memory_space=pl.ANY)
    dma = pltpu.SemaphoreType.DMA
    return pl.pallas_call(
        functools.partial(core_kernel, nctx, ntp),
        out_shape=(small, small, small, small, jax.ShapeDtypeStruct((rows, width), BF)),
        in_specs=[hbm] * 5 + [pl.BlockSpec(memory_space=pltpu.VMEM), hbm],
        out_specs=(hbm,) * 5,
        scratch_shapes=[
            pltpu.VMEM((rows, width), BF),
            pltpu.VMEM((3, width, cols), BF),
            pltpu.VMEM((cols, width), BF),
            pltpu.VMEM((3, rows, cols), BF),
            pltpu.VMEM((rows, width), BF),
            pltpu.VMEM((nctx, per, cols), BF),
            pltpu.VMEM((all_blocks, cols), BF),
            pltpu.VMEM((all_blocks, cols), BF),
            pltpu.VMEM((units, PAIR, PAIR + all_blocks), BF),
            pltpu.VMEM((rows, cols), BF),
            pltpu.VMEM((rows, cols), BF),
            pltpu.VMEM((rows, cols), BF),
            pltpu.VMEM((rows, cols), BF),
            pltpu.VMEM((rows, cols), BF),
            pltpu.VMEM((rows, cols), F32),
            pltpu.VMEM((rows, cols), F32),
            pltpu.VMEM((all_blocks, cols), F32),
            pltpu.VMEM((all_blocks, cols), F32),
            pltpu.VMEM((nctx, per, cols), BF),
            pltpu.VMEM((nctx, per, cols), BF),
            dma((6,)),
            dma((5,)),
            dma((ntp // 2,)),
            dma((ntp,)),
            dma((ntp // 2,)),
            dma((nctx - 1,)),
            dma((nctx,)),
            dma((nctx - 1,)),
            dma((nctx,)),
        ],
        compiler_params=pltpu.CompilerParams(
            collective_id=1, has_side_effects=True, vmem_limit_bytes=64 * 1024 * 1024 - 65536
        ),
        name="attention_core",
    )(tokens, w_query, w_key, w_value, w_out, block_doc.reshape(1, -1), grad_out)


def cut_along(shard, dim, length):
    dims = shard.shape
    blocks = shard.reshape(*dims[:dim], length, dims[dim] // length, *dims[dim + 1 :])
    return jnp.moveaxis(blocks, dim, 0)


def sent_and_summed(shard, axis, dim):
    length = lax.axis_size(axis)
    blocks = lax.all_to_all(cut_along(shard, dim, length), axis, 0, 0, tiled=True)
    return jnp.sum(blocks.astype(jnp.float32), axis=0)


def per_device(nctx, ntp, tokens, w_query, w_key, w_value, w_out, block_doc, grad_out):
    col_count = w_query.shape[1]
    attn, d_query, d_key, d_value, upstream = attention_core(
        nctx, ntp, tokens, w_query, w_key, w_value, w_out, block_doc, grad_out
    )
    stacked = jnp.concatenate([d_query, d_key, d_value], axis=1)
    joined = lax.psum_scatter(
        dot_tn(tokens, stacked).astype(BF), "ctx", scatter_dimension=0, tiled=True
    ).astype(F32)
    grad_query_weight = joined[:, :col_count]
    grad_key_weight = joined[:, col_count : 2 * col_count]
    grad_value_weight = joined[:, 2 * col_count :]
    summed = lax.psum_scatter(
        dot_nn(attn, w_out).astype(BF), "tp", scatter_dimension=1, tiled=True
    ).astype(F32)
    shard_width = summed.shape[1]
    residual = lax.dynamic_slice_in_dim(tokens, lax.axis_index("tp") * shard_width, shard_width, 1)
    output = (residual.astype(F32) + summed).astype(BF)
    d_partial = dot_nt(d_query, w_query) + dot_nt(d_key, w_key) + dot_nt(d_value, w_value)
    d_summed = lax.psum_scatter(
        d_partial.astype(BF), "tp", scatter_dimension=1, tiled=True
    ).astype(F32)
    grad_tokens = (grad_out.astype(F32) + d_summed).astype(BF)
    grad_out_weight = sent_and_summed(dot_tn(attn, upstream).astype(BF), "ctx", 1)
    return (
        output,
        grad_tokens,
        grad_query_weight,
        grad_key_weight,
        grad_value_weight,
        grad_out_weight,
    )


def solution(mesh):
    in_specs = (
        P("ctx", None),
        P(None, "tp"),
        P(None, "tp"),
        P(None, "tp"),
        P("tp", None),
        P(),
        P("ctx", "tp"),
    )
    out_specs = (
        P("ctx", "tp"),
        P("ctx", "tp"),
        P("ctx", "tp"),
        P("ctx", "tp"),
        P("ctx", "tp"),
        P("tp", "ctx"),
    )
    return jax.shard_map(
        functools.partial(per_device, mesh.shape["ctx"], mesh.shape["tp"]),
        mesh=mesh,
        in_specs=in_specs,
        out_specs=out_specs,
        check_vma=False,
    )
```

```python
import functools
import math

import jax
import jax.numpy as jnp
from jax import lax
from jax.experimental import pallas as pl
from jax.experimental.pallas import tpu as pltpu
from jax.sharding import PartitionSpec as P

HDIM = 128
BLOCK = 64
PAIR = 2 * BLOCK
MESH = pl.DeviceIdType.MESH
BF = jnp.bfloat16
F32 = jnp.float32
big_negative = -1e30


def dot_nn(a, b):
    return lax.dot_general(a, b, (((1,), (0,)), ((), ())), preferred_element_type=F32)


def dot_nt(a, b):
    return lax.dot_general(a, b, (((1,), (1,)), ((), ())), preferred_element_type=F32)


def dot_tn(a, b):
    return lax.dot_general(a, b, (((0,), (0,)), ((), ())), preferred_element_type=F32)


def iota(shape, dim):
    return lax.broadcasted_iota(jnp.int32, shape, dim)


def one_hot(hit):
    return jnp.where(hit, 1.0, 0.0).astype(BF)


def core_kernel(
    nctx,
    ntp,
    nx,
    tok_h,
    wq_h,
    wk_h,
    wv_h,
    wo_h,
    doc_ref,
    go_h,
    attn_o,
    dq_o,
    dk_o,
    dv_o,
    wos_o,
    tx_o,
    ty_o,
    tok,
    w3,
    wo,
    qkv,
    gfull,
    land,
    lk,
    lv,
    pw,
    attn,
    da,
    dqv,
    dkv,
    dvv,
    dkf,
    dvf,
    dlk,
    dlv,
    dls,
    dlr,
    wos,
    ld,
    st,
    g_s,
    g_r,
    f_s,
    l_s,
    l_r,
    d_s,
    d_r,
    tx_s,
    tx_r,
    ty_s,
    ty_r,
    t_l,
    fx_s,
    fx_r,
    fy_s,
    fy_r,
):
    ctx = lax.axis_index("ctx")
    ny = nctx // nx
    y = lax.div(ctx, nx)
    x = lax.rem(ctx, nx)
    tp = lax.axis_index("tp")
    nz = ntp // 2
    core = lax.rem(tp, 2)
    z = lax.div(tp, 2)
    partner = tp + 1 - 2 * core
    rows, width = tok.shape
    cols = qkv.shape[2]
    heads = cols // HDIM
    own_blocks = rows // BLOCK
    all_blocks = nctx * own_blocks
    per = 2 * own_blocks
    scale = 1.0 / math.sqrt(HDIM)

    def shard(t):
        return pl.ds(pl.multiple_of(t * cols, cols), cols)

    def mate(j, side):
        return lax.rem(z + j, nz) * 2 + side

    load_tok = pltpu.make_async_copy(tok_h, tok, ld.at[0])
    load_tok.start()
    for i, w_h in enumerate((wk_h, wv_h, wq_h)):
        pltpu.make_async_copy(w_h, w3.at[i], ld.at[1 + i]).start()
    load_wo = pltpu.make_async_copy(wo_h, wo, ld.at[4])
    load_wo.start()
    load_go = pltpu.make_async_copy(go_h, gfull.at[:, shard(tp)], ld.at[5])
    load_go.start()

    barrier = pltpu.get_barrier_semaphore()

    def greet(i, carry):
        pl.semaphore_signal(
            barrier, inc=1, device_id={"ctx": lax.rem(ctx + i, nctx)}, device_id_type=MESH
        )
        return carry

    lax.fori_loop(1, nctx, greet, 0)
    pl.semaphore_signal(barrier, inc=1, device_id={"tp": partner}, device_id_type=MESH)
    for j in range(1, nz):
        pl.semaphore_signal(barrier, inc=1, device_id={"tp": mate(j, core)}, device_id_type=MESH)
    pl.semaphore_wait(barrier, nctx - 1 + nz)

    def grad_copy(source, owner, send, target):
        return pltpu.make_async_remote_copy(
            src_ref=source,
            dst_ref=gfull.at[:, shard(owner)],
            send_sem=send,
            recv_sem=g_r.at[owner],
            device_id={"tp": target},
            device_id_type=MESH,
        )

    first_sends = [grad_copy(go_h, tp, g_s.at[j - 1], mate(j, core)) for j in range(1, nz)]
    first_sends.append(grad_copy(go_h, tp, g_s.at[nz - 1], partner))
    for send in first_sends:
        send.start()

    load_tok.wait()

    half = cols // 2

    def project(i, carry):
        pltpu.make_async_copy(wk_h, w3.at[i], ld.at[1 + i]).wait()

        def piece(n, inner):
            at = pl.ds(pl.multiple_of(n * half, half), half)
            qkv[i, :, at] = dot_nn(tok[...], w3[i, :, at]).astype(BF)
            return inner

        lax.fori_loop(0, 2, piece, 0)

        @pl.when(i == 1)
        def _():
            r = iota((per, rows), 0)
            c = iota((per, rows), 1)
            pick_k = one_hot(c == r * BLOCK + BLOCK - 1)
            pick_v = one_hot(c == (r - own_blocks) * BLOCK + BLOCK - 1)
            pick_k = jnp.where(r < own_blocks, pick_k, jnp.zeros_like(pick_k))
            pick_v = jnp.where(r >= own_blocks, pick_v, jnp.zeros_like(pick_v))
            land[ctx] = (dot_nn(pick_k, qkv[0]) + dot_nn(pick_v, qkv[1])).astype(BF)

            def spread(j, inner):
                pltpu.make_async_remote_copy(
                    src_ref=land.at[ctx],
                    dst_ref=land.at[ctx],
                    send_sem=l_s.at[j - 1],
                    recv_sem=l_r.at[ctx],
                    device_id={"ctx": lax.rem(ctx + j, nctx)},
                    device_id_type=MESH,
                ).start()
                return inner

            lax.fori_loop(1, nctx, spread, 0)

        return carry

    lax.fori_loop(0, 3, project, 0)

    def land_wait(j, carry):
        source = lax.rem(ctx + j, nctx)
        copy = pltpu.make_async_remote_copy(
            src_ref=land.at[ctx],
            dst_ref=land.at[source],
            send_sem=l_s.at[j - 1],
            recv_sem=l_r.at[source],
            device_id={"ctx": source},
            device_id_type=MESH,
        )
        copy.wait_send()
        copy.wait_recv()
        return carry

    lax.fori_loop(1, nctx, land_wait, 0)

    strip = width // nctx
    own_half = pl.ds(pl.multiple_of(core * (rows // 2), rows // 2), rows // 2)

    def strip_at(i):
        return pl.ds(pl.multiple_of(i * strip, strip), strip)

    def x_copy(j, i, owner):
        return pltpu.make_async_remote_copy(
            src_ref=tok.at[own_half, strip_at(i * nx + lax.rem(x + j, nx))],
            dst_ref=tx_o.at[owner, own_half, strip_at(i)],
            send_sem=tx_s.at[j - 1, i],
            recv_sem=tx_r.at[owner, i],
            device_id={"ctx": y * nx + lax.rem(x + j, nx)},
            device_id_type=MESH,
        )

    def y_copy(j, owner):
        there = lax.rem(y + j, ny)
        return pltpu.make_async_remote_copy(
            src_ref=tok.at[own_half, pl.ds(pl.multiple_of(there * nx * strip, strip), nx * strip)],
            dst_ref=ty_o.at[owner, own_half],
            send_sem=ty_s.at[j - 1],
            recv_sem=ty_r.at[owner],
            device_id={"ctx": there * nx + x},
            device_id_type=MESH,
        )

    def pass_on(ref, owner, send, recv):
        return pltpu.make_async_remote_copy(
            src_ref=ref.at[owner, own_half],
            dst_ref=ref.at[owner, own_half],
            send_sem=send,
            recv_sem=recv,
            device_id={"tp": partner},
            device_id_type=MESH,
        )

    for j in (1, 3, 2):
        for i in range(ny):
            x_copy(j, i, x).start()
        y_copy(j, y).start()
    own_strips = [
        pltpu.make_async_copy(
            tok.at[:, strip_at(i * nx + x)], tx_o.at[x, :, strip_at(i)], t_l.at[i]
        )
        for i in range(ny)
    ]
    own_strips.append(
        pltpu.make_async_copy(
            tok.at[:, pl.ds(pl.multiple_of(y * nx * strip, strip), nx * strip)],
            ty_o.at[y],
            t_l.at[ny],
        )
    )
    for copy in own_strips:
        copy.start()

    b = iota((all_blocks, nctx * per), 0)
    c = iota((all_blocks, nctx * per), 1)
    shift = b // own_blocks * own_blocks
    landed = land[...].reshape(nctx * per, cols)
    lk[...] = dot_nn(one_hot(c == b + shift), landed).astype(BF)
    lv[...] = dot_nn(one_hot(c == b + shift + own_blocks), landed).astype(BF)

    span = PAIR + all_blocks
    doc = doc_ref[...]
    doc_lane = iota(doc.shape, 1)
    doc_wide = jnp.concatenate([jnp.zeros((1, PAIR), jnp.int32), doc], axis=1)

    def forward(sb, carry):
        at = pl.ds(pl.multiple_of(sb * PAIR, PAIR), PAIR)
        row = iota((PAIR, span), 0)
        col = iota((PAIR, span), 1)
        upper = jnp.where(row >= BLOCK, 1, 0)
        col_upper = jnp.where(col >= BLOCK, 1, 0)
        first = ctx * own_blocks + sb * 2
        doc_a = jnp.sum(jnp.where(doc_lane == first, doc, 0), axis=1, keepdims=True)
        doc_b = jnp.sum(jnp.where(doc_lane == first + 1, doc, 0), axis=1, keepdims=True)
        own_doc = jnp.where(row >= BLOCK, doc_b, doc_a)
        near = (col < PAIR) & (upper == col_upper) & (col <= row)
        far = (col >= PAIR) & (col - PAIR < first + upper) & (doc_wide == own_doc)
        mask = near | far
        for h in range(heads):
            hs = pl.ds(h * HDIM, HDIM)
            keys = jnp.concatenate([qkv[0, at, hs], lk[:, hs]], axis=0)
            values = jnp.concatenate([qkv[1, at, hs], lv[:, hs]], axis=0)
            scores = dot_nt(qkv[2, at, hs], keys) * scale
            scores = jnp.where(mask, scores, big_negative)
            top = jnp.max(scores, axis=1, keepdims=True)
            e = jnp.exp(scores - top)
            weight = (e / jnp.sum(e, axis=1, keepdims=True)).astype(BF)
            pw[sb * heads + h] = weight
            attn[at, hs] = dot_nn(weight, values).astype(BF)
        return carry

    lax.fori_loop(0, rows // PAIR, forward, 0)
    out_attn = pltpu.make_async_copy(attn, attn_o, st.at[0])
    out_attn.start()

    forwards = []
    for j in range(1, nz):
        owner = mate(j, core)
        grad_copy(gfull.at[:, shard(owner)], owner, f_s.at[j - 1], partner).wait_recv()
        onward = grad_copy(gfull.at[:, shard(owner)], owner, f_s.at[j - 1], partner)
        onward.start()
        forwards.append(onward)
    grad_copy(go_h, partner, g_s.at[nz - 1], partner).wait_recv()
    for j in range(1, nz):
        owner = mate(j, 1 - core)
        grad_copy(gfull.at[:, shard(owner)], owner, f_s.at[j - 1], partner).wait_recv()
    load_go.wait()
    load_wo.wait()

    def d_piece(n, carry):
        at = pl.ds(pl.multiple_of(n * half, half), half)
        da[:, at] = dot_nt(gfull[...], wo[at, :]).astype(BF)
        return carry

    lax.fori_loop(0, 2, d_piece, 0)

    dlk[...] = jnp.zeros_like(dlk)
    dlv[...] = jnp.zeros_like(dlv)

    def backward(sb, carry):
        at = pl.ds(pl.multiple_of(sb * PAIR, PAIR), PAIR)
        for h in range(heads):
            hs = pl.ds(h * HDIM, HDIM)
            keys = jnp.concatenate([qkv[0, at, hs], lk[:, hs]], axis=0)
            values = jnp.concatenate([qkv[1, at, hs], lv[:, hs]], axis=0)
            weight = pw[sb * heads + h]
            d_out = da[at, hs]
            delta = jnp.sum(
                attn[at, hs].astype(F32) * d_out.astype(F32), axis=1, keepdims=True
            )
            d_weight = dot_nt(d_out, values)
            ds = (weight.astype(F32) * (d_weight - delta)).astype(BF)
            dqv[at, hs] = (dot_nn(ds, keys) * scale).astype(BF)
            d_keys = dot_tn(ds, qkv[2, at, hs]) * scale
            d_values = dot_tn(weight, d_out)
            dkf[at, hs] = d_keys[:PAIR]
            dvf[at, hs] = d_values[:PAIR]
            dlk[:, hs] += d_keys[PAIR:]
            dlv[:, hs] += d_values[PAIR:]
        return carry

    lax.fori_loop(0, rows // PAIR, backward, 0)
    out_dq = pltpu.make_async_copy(dqv, dq_o, st.at[1])
    out_dq.start()

    r = iota((nctx * per, all_blocks), 0)
    b = iota((nctx * per, all_blocks), 1)
    shift = b // own_blocks * own_blocks
    packed = dot_nn(one_hot(r == b + shift), dlk[...].astype(BF)) + dot_nn(
        one_hot(r == b + shift + own_blocks), dlv[...].astype(BF)
    )
    dls[...] = packed.astype(BF).reshape(nctx, per, cols)

    def give(j, carry):
        target = lax.rem(ctx + j, nctx)
        pltpu.make_async_remote_copy(
            src_ref=dls.at[target],
            dst_ref=dlr.at[ctx],
            send_sem=d_s.at[j - 1],
            recv_sem=d_r.at[ctx],
            device_id={"ctx": target},
            device_id_type=MESH,
        ).start()
        return carry

    lax.fori_loop(1, nctx, give, 0)
    dlr[ctx] = dls[ctx]

    def out_weight(i, carry):
        part = dot_tn(attn[...], gfull[:, strip_at(i)]).astype(BF)
        there_y = lax.div(i, nx)
        there_x = lax.rem(i, nx)
        wos[0, there_x, there_y] = part[: cols // 2]
        wos[1, there_y, there_x] = part[cols // 2 :]
        return carry

    lax.fori_loop(0, nctx, out_weight, 0)
    out_wos = pltpu.make_async_copy(wos, wos_o, st.at[4])
    out_wos.start()

    for j in range(1, nx):
        owner = lax.rem(x + j, nx)
        for i in range(ny):
            x_copy(j, i, owner).wait_recv()
        pass_on(tx_o, owner, fx_s.at[j - 1], fx_r.at[j - 1]).start()
    for j in range(1, ny):
        owner = lax.rem(y + j, ny)
        y_copy(j, owner).wait_recv()
        pass_on(ty_o, owner, fy_s.at[j - 1], fy_r.at[j - 1]).start()

    def take(j, carry):
        source = lax.rem(ctx + j, nctx)
        copy = pltpu.make_async_remote_copy(
            src_ref=dls.at[source],
            dst_ref=dlr.at[source],
            send_sem=d_s.at[j - 1],
            recv_sem=d_r.at[source],
            device_id={"ctx": source},
            device_id_type=MESH,
        )
        copy.wait_send()
        copy.wait_recv()
        return carry

    lax.fori_loop(1, nctx, take, 0)
    total = jnp.zeros((per, cols), F32)
    for i in range(nctx):
        total = total + dlr[i].astype(F32)
    for i in range(own_blocks):
        last = pl.ds(i * BLOCK + BLOCK - 1, 1)
        dkf[last, :] += total[i : i + 1]
        dvf[last, :] += total[own_blocks + i : own_blocks + i + 1]
    dkv[...] = dkf[...].astype(BF)
    dvv[...] = dvf[...].astype(BF)
    out_dk = pltpu.make_async_copy(dkv, dk_o, st.at[2])
    out_dk.start()
    out_dv = pltpu.make_async_copy(dvv, dv_o, st.at[3])
    out_dv.start()
    for send in first_sends + forwards:
        send.wait_send()
    for copy in [out_attn, out_dq, out_dk, out_dv, out_wos] + own_strips:
        copy.wait()
    for j in range(1, nx):
        for i in range(ny):
            x_copy(j, i, x).wait_send()
        passed = pass_on(tx_o, lax.rem(x + j, nx), fx_s.at[j - 1], fx_r.at[j - 1])
        passed.wait_send()
        other_half = pl.ds(pl.multiple_of((1 - core) * (rows // 2), rows // 2), rows // 2)
        pltpu.make_async_remote_copy(
            src_ref=tx_o.at[lax.rem(x + j, nx), other_half],
            dst_ref=tx_o.at[lax.rem(x + j, nx), other_half],
            send_sem=fx_s.at[j - 1],
            recv_sem=fx_r.at[j - 1],
            device_id={"tp": partner},
            device_id_type=MESH,
        ).wait_recv()
    for j in range(1, ny):
        y_copy(j, y).wait_send()
        passed = pass_on(ty_o, lax.rem(y + j, ny), fy_s.at[j - 1], fy_r.at[j - 1])
        passed.wait_send()
        other_half = pl.ds(pl.multiple_of((1 - core) * (rows // 2), rows // 2), rows // 2)
        pltpu.make_async_remote_copy(
            src_ref=ty_o.at[lax.rem(y + j, ny), other_half],
            dst_ref=ty_o.at[lax.rem(y + j, ny), other_half],
            send_sem=fy_s.at[j - 1],
            recv_sem=fy_r.at[j - 1],
            device_id={"tp": partner},
            device_id_type=MESH,
        ).wait_recv()


def attention_core(nctx, ntp, nx, tokens, w_query, w_key, w_value, w_out, block_doc, grad_out):
    rows, width = tokens.shape
    cols = w_query.shape[1]
    heads = cols // HDIM
    own_blocks = rows // BLOCK
    all_blocks = nctx * own_blocks
    per = 2 * own_blocks
    units = rows // PAIR * heads
    ny = nctx // nx
    small = jax.ShapeDtypeStruct((rows, cols), BF)
    hbm = pl.BlockSpec(memory_space=pl.ANY)
    dma = pltpu.SemaphoreType.DMA
    return pl.pallas_call(
        functools.partial(core_kernel, nctx, ntp, nx),
        out_shape=(
            small,
            small,
            small,
            small,
            jax.ShapeDtypeStruct((2, nx, ny, cols // 2, width // nctx), BF),
            jax.ShapeDtypeStruct((nx, rows, width // nx), BF),
            jax.ShapeDtypeStruct((ny, rows, width // ny), BF),
        ),
        in_specs=[hbm] * 5 + [pl.BlockSpec(memory_space=pltpu.VMEM), hbm],
        out_specs=(hbm,) * 7,
        scratch_shapes=[
            pltpu.VMEM((rows, width), BF),
            pltpu.VMEM((3, width, cols), BF),
            pltpu.VMEM((cols, width), BF),
            pltpu.VMEM((3, rows, cols), BF),
            pltpu.VMEM((rows, width), BF),
            pltpu.VMEM((nctx, per, cols), BF),
            pltpu.VMEM((all_blocks, cols), BF),
            pltpu.VMEM((all_blocks, cols), BF),
            pltpu.VMEM((units, PAIR, PAIR + all_blocks), BF),
            pltpu.VMEM((rows, cols), BF),
            pltpu.VMEM((rows, cols), BF),
            pltpu.VMEM((rows, cols), BF),
            pltpu.VMEM((rows, cols), BF),
            pltpu.VMEM((rows, cols), BF),
            pltpu.VMEM((rows, cols), F32),
            pltpu.VMEM((rows, cols), F32),
            pltpu.VMEM((all_blocks, cols), F32),
            pltpu.VMEM((all_blocks, cols), F32),
            pltpu.VMEM((nctx, per, cols), BF),
            pltpu.VMEM((nctx, per, cols), BF),
            pltpu.VMEM((2, nx, ny, cols // 2, width // nctx), BF),
            dma((6,)),
            dma((5,)),
            dma((ntp // 2,)),
            dma((ntp,)),
            dma((ntp // 2,)),
            dma((nctx - 1,)),
            dma((nctx,)),
            dma((nctx - 1,)),
            dma((nctx,)),
            dma((nx - 1, ny)),
            dma((nx, ny)),
            dma((ny - 1,)),
            dma((ny,)),
            dma((ny + 1,)),
            dma((nx - 1,)),
            dma((nx - 1,)),
            dma((ny - 1,)),
            dma((ny - 1,)),
        ],
        compiler_params=pltpu.CompilerParams(
            collective_id=1, has_side_effects=True, vmem_limit_bytes=64 * 1024 * 1024 - 65536
        ),
        name="attention_core",
    )(tokens, w_query, w_key, w_value, w_out, block_doc.reshape(1, -1), grad_out)


def grad_kernel(
    nctx,
    ntp,
    nx,
    dq_h,
    dk_h,
    dv_h,
    attn_h,
    wos_h,
    tx_h,
    ty_h,
    wq_h,
    wk_h,
    wv_h,
    wo_h,
    tok_h,
    go_h,
    out_o,
    gt_o,
    gq_o,
    gk_o,
    gv_o,
    gwo_o,
    w3,
    wo,
    dcat,
    attn,
    rest,
    rest_g,
    gq,
    gk,
    gvx,
    gvy,
    o_p,
    o_q,
    o_z,
    o_a,
    d_p,
    d_q,
    d_z,
    d_a,
    sq,
    sk,
    sv,
    rq,
    rk,
    rv,
    oq,
    ok,
    ov,
    wo_r,
    wo_t,
    wo_u,
    wo_a,
    ld,
    ag_s,
    ag_r,
    op_s,
    op_r,
    oz_s,
    oz_r,
    dp_s,
    dp_r,
    dz_s,
    dz_r,
    rs_s,
    rs_r,
    w1_s,
    w1_r,
    w2_s,
    w2_r,
):
    ctx = lax.axis_index("ctx")
    tp = lax.axis_index("tp")
    ny = nctx // nx
    nz = ntp // 2
    y = lax.div(ctx, nx)
    x = lax.rem(ctx, nx)
    core = lax.rem(tp, 2)
    z = lax.div(tp, 2)
    partner = tp + 1 - 2 * core
    rows, cols = attn.shape
    width = wo.shape[1]
    strip = width // nctx
    gathered = nx * rows
    half = cols // 2

    def block(t):
        return pl.ds(pl.multiple_of(t * cols, cols), cols)

    def strip_at(i):
        return pl.ds(pl.multiple_of(i * strip, strip), strip)

    def at_x(i):
        return {"ctx": y * nx + i}

    def at_y(i):
        return {"ctx": i * nx + x}

    def remote(source, target, send, recv, where):
        return pltpu.make_async_remote_copy(
            src_ref=source,
            dst_ref=target,
            send_sem=send,
            recv_sem=recv,
            device_id=where,
            device_id_type=MESH,
        )

    loads = [
        pltpu.make_async_copy(attn_h, attn, ld.at[0]),
        pltpu.make_async_copy(wo_h, wo, ld.at[1]),
    ]
    for i, (d_h, w_h) in enumerate(((dq_h, wq_h), (dk_h, wk_h), (dv_h, wv_h))):
        lanes = pl.ds(i * cols, cols)
        loads.append(pltpu.make_async_copy(d_h, dcat.at[:, lanes], ld.at[2 + 2 * i]))
        loads.append(pltpu.make_async_copy(w_h, w3.at[:, lanes], ld.at[3 + 2 * i]))
    loads.append(pltpu.make_async_copy(tok_h.at[:, block(tp)], rest, ld.at[8]))
    loads.append(pltpu.make_async_copy(go_h, rest_g, ld.at[9]))
    lo = pl.ds(0, half)
    hi = pl.ds(half, half)
    gathers = (
        (dq_h, gq, x, at_x, 0),
        (dk_h, gk, y, at_y, 1),
        (dv_h.at[:, lo], gvx, x, at_x, 2),
        (dv_h.at[:, hi], gvy, y, at_y, 3),
    )
    for source, buf, pos, at, i in gathers:
        loads.append(pltpu.make_async_copy(source, buf.at[pos], ld.at[10 + i]))
    loads.append(pltpu.make_async_copy(wos_h.at[0, x], wo_r.at[0, x], ld.at[14]))
    loads.append(pltpu.make_async_copy(wos_h.at[1, y], wo_r.at[1, y], ld.at[15]))
    for load in loads:
        load.start()

    barrier = pltpu.get_barrier_semaphore()
    for j in range(1, nx):
        pl.semaphore_signal(
            barrier, inc=1, device_id=at_x(lax.rem(x + j, nx)), device_id_type=MESH
        )
    for j in range(1, ny):
        pl.semaphore_signal(
            barrier, inc=1, device_id=at_y(lax.rem(y + j, ny)), device_id_type=MESH
        )
    for j in range(1, nz):
        pl.semaphore_signal(
            barrier,
            inc=1,
            device_id={"tp": lax.rem(z + j, nz) * 2 + core},
            device_id_type=MESH,
        )
    pl.semaphore_signal(barrier, inc=1, device_id={"tp": partner}, device_id_type=MESH)
    pl.semaphore_wait(barrier, nx + ny + nz - 2)

    def near_send(gather, step):
        source, buf, pos, at, i = gather
        n = buf.shape[0]
        there = lax.rem(pos + (1 if step == 0 else n - 1), n)
        return remote(source, buf.at[pos], ag_s.at[i, step], ag_r.at[i, step], at(there))

    def near_recv(gather, step):
        source, buf, pos, at, i = gather
        n = buf.shape[0]
        owner = lax.rem(pos + (n - 1 if step == 0 else 1), n)
        return remote(source, buf.at[owner], ag_s.at[i, step], ag_r.at[i, step], at(owner))

    def relay(gather, step):
        source, buf, pos, at, i = gather
        n = buf.shape[0]
        part = pl.ds(0, rows // 2) if step == 0 else pl.ds(rows // 2, rows // 2)
        owner = lax.rem(pos + (n - 1 if step == 0 else 1), n)
        there = lax.rem(pos + (1 if step == 0 else n - 1), n)
        return remote(
            buf.at[owner, part],
            buf.at[owner, part],
            ag_s.at[i, 2 + step],
            ag_r.at[i, 2 + step],
            at(there),
        )

    def relay_recv(gather, step):
        source, buf, pos, at, i = gather
        n = buf.shape[0]
        part = pl.ds(0, rows // 2) if step == 0 else pl.ds(rows // 2, rows // 2)
        owner = lax.rem(pos + 2, n)
        return remote(
            buf.at[owner, part],
            buf.at[owner, part],
            ag_s.at[i, 2 + step],
            ag_r.at[i, 2 + step],
            at(owner),
        )

    for gather in gathers:
        near_send(gather, 0).start()
        near_send(gather, 1).start()

    def out_chunk(t):
        return dot_nn(attn[...], wo[:, block(t)])

    def tok_chunk(t):
        return dot_nt(dcat[...], w3[block(t), :])

    def to_partner(i, chunk, p, q, p_s, p_r):
        return remote(p.at[i], q.at[i], p_s.at[i], p_r.at[i], {"tp": partner})

    def summed_over_heads(chunk, p, q, zb, acc, p_s, p_r, z_s, z_r):
        def first(i, carry):
            p[i] = chunk(i * 2 + 1 - core).astype(BF)
            to_partner(i, chunk, p, q, p_s, p_r).start()
            return carry

        lax.fori_loop(0, nz, first, 0)

        def second(j, carry):
            i = lax.rem(z + j, nz)
            part = chunk(i * 2 + core)
            copy = to_partner(i, chunk, p, q, p_s, p_r)
            copy.wait_send()
            copy.wait_recv()
            part = part + q[i].astype(F32)

            @pl.when(j < nz)
            def _():
                p[i] = part.astype(BF)
                remote(
                    p.at[i], zb.at[z], z_s.at[j - 1], z_r.at[z], {"tp": i * 2 + core}
                ).start()

            @pl.when(j == nz)
            def _():
                acc[...] = part

            return carry

        lax.fori_loop(1, nz + 1, second, 0)

    def from_heads(p, zb, acc, z_s, z_r):
        total = acc[...]
        for j in range(1, nz):
            i = lax.rem(z + j, nz)
            copy = remote(p.at[i], zb.at[i], z_s.at[j - 1], z_r.at[i], {"tp": i * 2 + core})
            copy.wait_send()
            copy.wait_recv()
            total = total + zb[i].astype(F32)
        return total

    loads[0].wait()
    loads[1].wait()
    summed_over_heads(out_chunk, o_p, o_q, o_z, o_a, op_s, op_r, oz_s, oz_r)
    for load in loads[2:8]:
        load.wait()
    summed_over_heads(tok_chunk, d_p, d_q, d_z, d_a, dp_s, dp_r, dz_s, dz_r)
    t_x = w3.at[pl.ds(0, gathered), pl.ds(0, width // nx)]
    t_y = w3.at[pl.ds(gathered, gathered), pl.ds(0, width // ny)]
    late = []
    for i in range(nx):
        part = pl.ds(i * rows, rows)
        late.append(pltpu.make_async_copy(tx_h.at[i], t_x.at[part], ld.at[16 + i]))
        late.append(pltpu.make_async_copy(ty_h.at[i], t_y.at[part], ld.at[16 + nx + i]))
    for load in late:
        load.start()

    for gather in gathers:
        for step in range(2):
            near_recv(gather, step).wait_recv()
            relay(gather, step).start()

    def first_hop(j, side, owner):
        pos, n, at = ((x, nx, at_x), (y, ny, at_y))[side]
        there = lax.rem(pos + j, n)
        return remote(
            wos_h.at[side, there],
            wo_r.at[side, owner],
            w1_s.at[side, j - 1],
            w1_r.at[side, owner],
            at(there),
        )

    for j in (1, 3, 2):
        first_hop(j, 0, x).start()
        first_hop(j, 1, y).start()

    for load in loads[8:] + late:
        load.wait()

    sends = (
        (gathers[0], 0, sq, rq, oq, y, at_y, 0),
        (gathers[1], 1, sk, rk, ok, x, at_x, 1),
        (gathers[2], 0, sv.at[:, :, lo], rv.at[:, :, lo], ov.at[:, lo], y, at_y, 2),
        (gathers[3], 1, sv.at[:, :, hi], rv.at[:, :, hi], ov.at[:, hi], x, at_x, 3),
    )

    def weight_send(item, there, slot, owner):
        gather, side, s, r, o, pos, at, i = item
        return remote(s.at[there], r.at[owner], rs_s.at[i, slot], rs_r.at[i, owner], at(there))

    for item in sends:
        gather, side, s, r, o, pos, at, i = item
        for step in range(2):
            relay_recv(gather, step).wait_recv()
        buf = gather[1]
        n = buf.shape[0]
        base = pl.ds(side * gathered, gathered)

        def weight_piece(j, carry):
            there = lax.rem(pos + j, n)
            part = dot_tn(
                w3[base, strip_at(there)], buf[...].reshape(gathered, buf.shape[2])
            )

            @pl.when(j < n)
            def _():
                s[there] = part.astype(BF)
                weight_send(item, there, j - 1, pos).start()

            @pl.when(j == n)
            def _():
                o[...] = part

            return carry

        lax.fori_loop(1, n + 1, weight_piece, 0)

    out_o[...] = (rest[...].astype(F32) + from_heads(o_p, o_z, o_a, oz_s, oz_r)).astype(BF)
    gt_o[...] = (rest_g[...].astype(F32) + from_heads(d_p, d_z, d_a, dz_s, dz_r)).astype(BF)

    def second_hop(side, there, slot, owner):
        pos, n, at = ((y, ny, at_y), (x, nx, at_x))[side]
        return remote(
            wo_t.at[side, there],
            wo_u.at[side, owner],
            w2_s.at[side, slot],
            w2_r.at[side, owner],
            at(there),
        )

    for side in range(2):
        here, n = ((x, nx), (y, ny))[side]
        pos, m = ((y, ny), (x, nx))[side]
        for j in range(1, n):
            copy = first_hop(j, side, lax.rem(here + j, n))
            copy.wait_send()
            copy.wait_recv()

        def add_up(j, carry):
            there = lax.rem(pos + j, m)
            total = wo_r[side, 0, there].astype(F32)
            for k in range(1, n):
                total = total + wo_r[side, k, there].astype(F32)

            @pl.when(j < m)
            def _():
                wo_t[side, there] = total.astype(BF)
                second_hop(side, there, j - 1, pos).start()

            @pl.when(j == m)
            def _():
                wo_a[pl.ds(side * half, half), :] = total

            return carry

        lax.fori_loop(1, m + 1, add_up, 0)

    for item, target in zip(sends, (gq_o, gk_o, gv_o.at[:, lo], gv_o.at[:, hi])):
        gather, side, s, r, o, pos, at, i = item
        n = r.shape[0]
        total = o[...]
        for j in range(1, n):
            there = lax.rem(pos + j, n)
            copy = weight_send(item, there, j - 1, there)
            copy.wait_send()
            copy.wait_recv()
            total = total + r[there].astype(F32)
        target[...] = total
        for step in range(2):
            near_send(gather, step).wait_send()
            relay(gather, step).wait_send()

    for side in range(2):
        pos, m = ((y, ny), (x, nx))[side]
        total = wo_a[pl.ds(side * half, half), :]
        for j in range(1, m):
            there = lax.rem(pos + j, m)
            copy = second_hop(side, there, j - 1, there)
            copy.wait_send()
            copy.wait_recv()
            total = total + wo_u[side, there].astype(F32)
        gwo_o[pl.ds(side * half, half), :] = total


def gradients(nctx, ntp, nx, core_out, tokens, w_query, w_key, w_value, w_out, grad_out):
    attn, d_query, d_key, d_value, wos, tx, ty = core_out
    rows, width = tokens.shape
    cols = w_query.shape[1]
    ny = nctx // nx
    nz = ntp // 2
    strip = width // nctx
    half = cols // 2
    hbm = pl.BlockSpec(memory_space=pl.ANY)
    vmem = pl.BlockSpec(memory_space=pltpu.VMEM)
    dma = pltpu.SemaphoreType.DMA
    small = jax.ShapeDtypeStruct((rows, cols), BF)
    piece = jax.ShapeDtypeStruct((strip, cols), F32)
    heads_scratch = [
        pltpu.VMEM((nz, rows, cols), BF),
        pltpu.VMEM((nz, rows, cols), BF),
        pltpu.VMEM((nz, rows, cols), BF),
        pltpu.VMEM((rows, cols), F32),
    ]
    return pl.pallas_call(
        functools.partial(grad_kernel, nctx, ntp, nx),
        out_shape=(
            small,
            small,
            piece,
            piece,
            piece,
            jax.ShapeDtypeStruct((cols, strip), F32),
        ),
        in_specs=[hbm] * 13,
        out_specs=(vmem,) * 6,
        scratch_shapes=[
            pltpu.VMEM((width, 3 * cols), BF),
            pltpu.VMEM((cols, width), BF),
            pltpu.VMEM((rows, 3 * cols), BF),
            pltpu.VMEM((rows, cols), BF),
            pltpu.VMEM((rows, cols), BF),
            pltpu.VMEM((rows, cols), BF),
            pltpu.VMEM((nx, rows, cols), BF),
            pltpu.VMEM((ny, rows, cols), BF),
            pltpu.VMEM((nx, rows, half), BF),
            pltpu.VMEM((ny, rows, half), BF),
            *heads_scratch,
            *heads_scratch,
            pltpu.VMEM((ny, strip, cols), BF),
            pltpu.VMEM((nx, strip, cols), BF),
            pltpu.VMEM((ny, strip, cols), BF),
            pltpu.VMEM((ny, strip, cols), BF),
            pltpu.VMEM((nx, strip, cols), BF),
            pltpu.VMEM((ny, strip, cols), BF),
            pltpu.VMEM((strip, cols), F32),
            pltpu.VMEM((strip, cols), F32),
            pltpu.VMEM((strip, cols), F32),
            pltpu.VMEM((2, nx, ny, half, strip), BF),
            pltpu.VMEM((2, ny, half, strip), BF),
            pltpu.VMEM((2, ny, half, strip), BF),
            pltpu.VMEM((cols, strip), F32),
            dma((16 + nx + ny,)),
            dma((4, 4)),
            dma((4, 4)),
            dma((nz,)),
            dma((nz,)),
            dma((nz - 1,)),
            dma((nz,)),
            dma((nz,)),
            dma((nz,)),
            dma((nz - 1,)),
            dma((nz,)),
            dma((4, nx - 1)),
            dma((4, nx)),
            dma((2, nx - 1)),
            dma((2, nx)),
            dma((2, nx - 1)),
            dma((2, nx)),
        ],
        compiler_params=pltpu.CompilerParams(
            collective_id=2, has_side_effects=True, vmem_limit_bytes=64 * 1024 * 1024 - 65536
        ),
        name="gradients",
    )(
        d_query,
        d_key,
        d_value,
        attn,
        wos,
        tx,
        ty,
        w_query,
        w_key,
        w_value,
        w_out,
        tokens,
        grad_out,
    )


def per_device(nctx, ntp, nx, tokens, w_query, w_key, w_value, w_out, block_doc, grad_out):
    core_out = attention_core(
        nctx, ntp, nx, tokens, w_query, w_key, w_value, w_out, block_doc, grad_out
    )
    return tuple(
        gradients(nctx, ntp, nx, core_out, tokens, w_query, w_key, w_value, w_out, grad_out)
    )


def solution(mesh):
    in_specs = (
        P("ctx", None),
        P(None, "tp"),
        P(None, "tp"),
        P(None, "tp"),
        P("tp", None),
        P(),
        P("ctx", "tp"),
    )
    out_specs = (
        P("ctx", "tp"),
        P("ctx", "tp"),
        P("ctx", "tp"),
        P("ctx", "tp"),
        P("ctx", "tp"),
        P("tp", "ctx"),
    )
    return jax.shard_map(
        functools.partial(per_device, mesh.shape["ctx"], mesh.shape["tp"], math.isqrt(mesh.shape["ctx"])),
        mesh=mesh,
        in_specs=in_specs,
        out_specs=out_specs,
        check_vma=False,
    )
```

```python
import functools
import math

import jax
import jax.numpy as jnp
from jax import lax
from jax.experimental import pallas as pl
from jax.experimental.pallas import tpu as pltpu
from jax.sharding import PartitionSpec as P

HDIM = 128
BLOCK = 64
PAIR = 2 * BLOCK
MESH = pl.DeviceIdType.MESH
BF = jnp.bfloat16
F32 = jnp.float32
big_negative = -1e30


def dot_nn(a, b):
    return lax.dot_general(a, b, (((1,), (0,)), ((), ())), preferred_element_type=F32)


def dot_nt(a, b):
    return lax.dot_general(a, b, (((1,), (1,)), ((), ())), preferred_element_type=F32)


def dot_tn(a, b):
    return lax.dot_general(a, b, (((0,), (0,)), ((), ())), preferred_element_type=F32)


def iota(shape, dim):
    return lax.broadcasted_iota(jnp.int32, shape, dim)


def one_hot(hit):
    return jnp.where(hit, 1.0, 0.0).astype(BF)


def core_kernel(
    nctx,
    ntp,
    nx,
    tok_h,
    wq_h,
    wk_h,
    wv_h,
    wo_h,
    doc_ref,
    go_h,
    attn_o,
    dq_o,
    dk_o,
    dv_o,
    wos_o,
    tx_o,
    ty_o,
    tok,
    w3,
    wo,
    qkv,
    gfull,
    land,
    lk,
    lv,
    pw,
    attn,
    da,
    dqv,
    dkv,
    dvv,
    dkf,
    dvf,
    dlk,
    dlv,
    dls,
    dlr,
    wos,
    ld,
    st,
    g_s,
    g_r,
    f_s,
    l_s,
    l_r,
    d_s,
    d_r,
    tx_s,
    tx_r,
    ty_s,
    ty_r,
    t_l,
    fx_s,
    fx_r,
    fy_s,
    fy_r,
):
    ctx = lax.axis_index("ctx")
    ny = nctx // nx
    y = lax.div(ctx, nx)
    x = lax.rem(ctx, nx)
    tp = lax.axis_index("tp")
    nz = ntp // 2
    core = lax.rem(tp, 2)
    z = lax.div(tp, 2)
    partner = tp + 1 - 2 * core
    rows, width = tok.shape
    cols = qkv.shape[2]
    heads = cols // HDIM
    own_blocks = rows // BLOCK
    all_blocks = nctx * own_blocks
    per = 2 * own_blocks
    scale = 1.0 / math.sqrt(HDIM)

    def shard(t):
        return pl.ds(pl.multiple_of(t * cols, cols), cols)

    def mate(j, side):
        return lax.rem(z + j, nz) * 2 + side

    load_tok = pltpu.make_async_copy(tok_h, tok, ld.at[0])
    load_tok.start()
    for i, w_h in enumerate((wk_h, wv_h, wq_h)):
        pltpu.make_async_copy(w_h, w3.at[i], ld.at[1 + i]).start()
    load_wo = pltpu.make_async_copy(wo_h, wo, ld.at[4])
    load_wo.start()
    load_go = pltpu.make_async_copy(go_h, gfull.at[:, shard(tp)], ld.at[5])
    load_go.start()

    barrier = pltpu.get_barrier_semaphore()

    def greet(i, carry):
        pl.semaphore_signal(
            barrier, inc=1, device_id={"ctx": lax.rem(ctx + i, nctx)}, device_id_type=MESH
        )
        return carry

    lax.fori_loop(1, nctx, greet, 0)
    pl.semaphore_signal(barrier, inc=1, device_id={"tp": partner}, device_id_type=MESH)
    for j in range(1, nz):
        pl.semaphore_signal(barrier, inc=1, device_id={"tp": mate(j, core)}, device_id_type=MESH)
    pl.semaphore_wait(barrier, nctx - 1 + nz)

    def grad_copy(source, owner, send, target):
        return pltpu.make_async_remote_copy(
            src_ref=source,
            dst_ref=gfull.at[:, shard(owner)],
            send_sem=send,
            recv_sem=g_r.at[owner],
            device_id={"tp": target},
            device_id_type=MESH,
        )

    first_sends = [grad_copy(go_h, tp, g_s.at[j - 1], mate(j, core)) for j in range(1, nz)]
    first_sends.append(grad_copy(go_h, tp, g_s.at[nz - 1], partner))
    for send in first_sends:
        send.start()

    load_tok.wait()

    half = cols // 2

    def project(i, carry):
        pltpu.make_async_copy(wk_h, w3.at[i], ld.at[1 + i]).wait()

        def piece(n, inner):
            at = pl.ds(pl.multiple_of(n * half, half), half)
            qkv[i, :, at] = dot_nn(tok[...], w3[i, :, at]).astype(BF)
            return inner

        lax.fori_loop(0, 2, piece, 0)

        @pl.when(i == 1)
        def _():
            r = iota((per, rows), 0)
            c = iota((per, rows), 1)
            pick_k = one_hot(c == r * BLOCK + BLOCK - 1)
            pick_v = one_hot(c == (r - own_blocks) * BLOCK + BLOCK - 1)
            pick_k = jnp.where(r < own_blocks, pick_k, jnp.zeros_like(pick_k))
            pick_v = jnp.where(r >= own_blocks, pick_v, jnp.zeros_like(pick_v))
            land[ctx] = (dot_nn(pick_k, qkv[0]) + dot_nn(pick_v, qkv[1])).astype(BF)

            def spread(j, inner):
                pltpu.make_async_remote_copy(
                    src_ref=land.at[ctx],
                    dst_ref=land.at[ctx],
                    send_sem=l_s.at[j - 1],
                    recv_sem=l_r.at[ctx],
                    device_id={"ctx": lax.rem(ctx + j, nctx)},
                    device_id_type=MESH,
                ).start()
                return inner

            lax.fori_loop(1, nctx, spread, 0)

        return carry

    lax.fori_loop(0, 3, project, 0)

    def land_wait(j, carry):
        source = lax.rem(ctx + j, nctx)
        copy = pltpu.make_async_remote_copy(
            src_ref=land.at[ctx],
            dst_ref=land.at[source],
            send_sem=l_s.at[j - 1],
            recv_sem=l_r.at[source],
            device_id={"ctx": source},
            device_id_type=MESH,
        )
        copy.wait_send()
        copy.wait_recv()
        return carry

    lax.fori_loop(1, nctx, land_wait, 0)

    strip = width // nctx
    own_half = pl.ds(pl.multiple_of(core * (rows // 2), rows // 2), rows // 2)

    def strip_at(i):
        return pl.ds(pl.multiple_of(i * strip, strip), strip)

    def x_copy(j, i, owner):
        return pltpu.make_async_remote_copy(
            src_ref=tok.at[own_half, strip_at(i * nx + lax.rem(x + j, nx))],
            dst_ref=tx_o.at[owner, own_half, strip_at(i)],
            send_sem=tx_s.at[j - 1, i],
            recv_sem=tx_r.at[owner, i],
            device_id={"ctx": y * nx + lax.rem(x + j, nx)},
            device_id_type=MESH,
        )

    def y_copy(j, owner):
        there = lax.rem(y + j, ny)
        return pltpu.make_async_remote_copy(
            src_ref=tok.at[own_half, pl.ds(pl.multiple_of(there * nx * strip, strip), nx * strip)],
            dst_ref=ty_o.at[owner, own_half],
            send_sem=ty_s.at[j - 1],
            recv_sem=ty_r.at[owner],
            device_id={"ctx": there * nx + x},
            device_id_type=MESH,
        )

    def pass_on(ref, owner, send, recv):
        return pltpu.make_async_remote_copy(
            src_ref=ref.at[owner, own_half],
            dst_ref=ref.at[owner, own_half],
            send_sem=send,
            recv_sem=recv,
            device_id={"tp": partner},
            device_id_type=MESH,
        )

    for j in (1, 3, 2):
        for i in range(ny):
            x_copy(j, i, x).start()
        y_copy(j, y).start()
    own_strips = [
        pltpu.make_async_copy(
            tok.at[:, strip_at(i * nx + x)], tx_o.at[x, :, strip_at(i)], t_l.at[i]
        )
        for i in range(ny)
    ]
    own_strips.append(
        pltpu.make_async_copy(
            tok.at[:, pl.ds(pl.multiple_of(y * nx * strip, strip), nx * strip)],
            ty_o.at[y],
            t_l.at[ny],
        )
    )
    for copy in own_strips:
        copy.start()

    b = iota((all_blocks, nctx * per), 0)
    c = iota((all_blocks, nctx * per), 1)
    shift = b // own_blocks * own_blocks
    landed = land[...].reshape(nctx * per, cols)
    lk[...] = dot_nn(one_hot(c == b + shift), landed).astype(BF)
    lv[...] = dot_nn(one_hot(c == b + shift + own_blocks), landed).astype(BF)

    span = PAIR + all_blocks
    doc = doc_ref[...]
    doc_lane = iota(doc.shape, 1)
    doc_wide = jnp.concatenate([jnp.zeros((1, PAIR), jnp.int32), doc], axis=1)

    def forward(sb, carry):
        at = pl.ds(pl.multiple_of(sb * PAIR, PAIR), PAIR)
        row = iota((PAIR, span), 0)
        col = iota((PAIR, span), 1)
        upper = jnp.where(row >= BLOCK, 1, 0)
        col_upper = jnp.where(col >= BLOCK, 1, 0)
        first = ctx * own_blocks + sb * 2
        doc_a = jnp.sum(jnp.where(doc_lane == first, doc, 0), axis=1, keepdims=True)
        doc_b = jnp.sum(jnp.where(doc_lane == first + 1, doc, 0), axis=1, keepdims=True)
        own_doc = jnp.where(row >= BLOCK, doc_b, doc_a)
        near = (col < PAIR) & (upper == col_upper) & (col <= row)
        far = (col >= PAIR) & (col - PAIR < first + upper) & (doc_wide == own_doc)
        mask = near | far
        for h in range(heads):
            hs = pl.ds(h * HDIM, HDIM)
            keys = jnp.concatenate([qkv[0, at, hs], lk[:, hs]], axis=0)
            values = jnp.concatenate([qkv[1, at, hs], lv[:, hs]], axis=0)
            scores = dot_nt(qkv[2, at, hs], keys) * scale
            scores = jnp.where(mask, scores, big_negative)
            top = jnp.max(scores, axis=1, keepdims=True)
            e = jnp.exp(scores - top)
            weight = (e / jnp.sum(e, axis=1, keepdims=True)).astype(BF)
            pw[sb * heads + h] = weight
            attn[at, hs] = dot_nn(weight, values).astype(BF)
        return carry

    lax.fori_loop(0, rows // PAIR, forward, 0)
    out_attn = pltpu.make_async_copy(attn, attn_o, st.at[0])
    out_attn.start()

    forwards = []
    for j in range(1, nz):
        owner = mate(j, core)
        grad_copy(gfull.at[:, shard(owner)], owner, f_s.at[j - 1], partner).wait_recv()
        onward = grad_copy(gfull.at[:, shard(owner)], owner, f_s.at[j - 1], partner)
        onward.start()
        forwards.append(onward)
    grad_copy(go_h, partner, g_s.at[nz - 1], partner).wait_recv()
    for j in range(1, nz):
        owner = mate(j, 1 - core)
        grad_copy(gfull.at[:, shard(owner)], owner, f_s.at[j - 1], partner).wait_recv()
    load_go.wait()
    load_wo.wait()

    def d_piece(n, carry):
        at = pl.ds(pl.multiple_of(n * half, half), half)
        da[:, at] = dot_nt(gfull[...], wo[at, :]).astype(BF)
        return carry

    lax.fori_loop(0, 2, d_piece, 0)

    dlk[...] = jnp.zeros_like(dlk)
    dlv[...] = jnp.zeros_like(dlv)

    def backward(sb, carry):
        at = pl.ds(pl.multiple_of(sb * PAIR, PAIR), PAIR)
        for h in range(heads):
            hs = pl.ds(h * HDIM, HDIM)
            keys = jnp.concatenate([qkv[0, at, hs], lk[:, hs]], axis=0)
            values = jnp.concatenate([qkv[1, at, hs], lv[:, hs]], axis=0)
            weight = pw[sb * heads + h]
            d_out = da[at, hs]
            delta = jnp.sum(
                attn[at, hs].astype(F32) * d_out.astype(F32), axis=1, keepdims=True
            )
            d_weight = dot_nt(d_out, values)
            ds = (weight.astype(F32) * (d_weight - delta)).astype(BF)
            dqv[at, hs] = (dot_nn(ds, keys) * scale).astype(BF)
            d_keys = dot_tn(ds, qkv[2, at, hs]) * scale
            d_values = dot_tn(weight, d_out)
            dkf[at, hs] = d_keys[:PAIR]
            dvf[at, hs] = d_values[:PAIR]
            dlk[:, hs] += d_keys[PAIR:]
            dlv[:, hs] += d_values[PAIR:]
        return carry

    lax.fori_loop(0, rows // PAIR, backward, 0)
    out_dq = pltpu.make_async_copy(dqv, dq_o, st.at[1])
    out_dq.start()

    r = iota((nctx * per, all_blocks), 0)
    b = iota((nctx * per, all_blocks), 1)
    shift = b // own_blocks * own_blocks
    packed = dot_nn(one_hot(r == b + shift), dlk[...].astype(BF)) + dot_nn(
        one_hot(r == b + shift + own_blocks), dlv[...].astype(BF)
    )
    dls[...] = packed.astype(BF).reshape(nctx, per, cols)

    def give(j, carry):
        target = lax.rem(ctx + j, nctx)
        pltpu.make_async_remote_copy(
            src_ref=dls.at[target],
            dst_ref=dlr.at[ctx],
            send_sem=d_s.at[j - 1],
            recv_sem=d_r.at[ctx],
            device_id={"ctx": target},
            device_id_type=MESH,
        ).start()
        return carry

    lax.fori_loop(1, nctx, give, 0)
    dlr[ctx] = dls[ctx]

    def out_weight(i, carry):
        part = dot_tn(attn[...], gfull[:, strip_at(i)]).astype(BF)
        there_y = lax.div(i, nx)
        there_x = lax.rem(i, nx)
        wos[0, there_x, there_y] = part[: cols // 2]
        wos[1, there_y, there_x] = part[cols // 2 :]
        return carry

    lax.fori_loop(0, nctx, out_weight, 0)
    out_wos = pltpu.make_async_copy(wos, wos_o, st.at[4])
    out_wos.start()

    for j in range(1, nx):
        owner = lax.rem(x + j, nx)
        for i in range(ny):
            x_copy(j, i, owner).wait_recv()
        pass_on(tx_o, owner, fx_s.at[j - 1], fx_r.at[j - 1]).start()
    for j in range(1, ny):
        owner = lax.rem(y + j, ny)
        y_copy(j, owner).wait_recv()
        pass_on(ty_o, owner, fy_s.at[j - 1], fy_r.at[j - 1]).start()

    def take(j, carry):
        source = lax.rem(ctx + j, nctx)
        copy = pltpu.make_async_remote_copy(
            src_ref=dls.at[source],
            dst_ref=dlr.at[source],
            send_sem=d_s.at[j - 1],
            recv_sem=d_r.at[source],
            device_id={"ctx": source},
            device_id_type=MESH,
        )
        copy.wait_send()
        copy.wait_recv()
        return carry

    lax.fori_loop(1, nctx, take, 0)
    total = jnp.zeros((per, cols), F32)
    for i in range(nctx):
        total = total + dlr[i].astype(F32)
    for i in range(own_blocks):
        last = pl.ds(i * BLOCK + BLOCK - 1, 1)
        dkf[last, :] += total[i : i + 1]
        dvf[last, :] += total[own_blocks + i : own_blocks + i + 1]
    dkv[...] = dkf[...].astype(BF)
    dvv[...] = dvf[...].astype(BF)
    out_dk = pltpu.make_async_copy(dkv, dk_o, st.at[2])
    out_dk.start()
    out_dv = pltpu.make_async_copy(dvv, dv_o, st.at[3])
    out_dv.start()
    for send in first_sends + forwards:
        send.wait_send()
    for copy in [out_attn, out_dq, out_dk, out_dv, out_wos] + own_strips:
        copy.wait()
    for j in range(1, nx):
        for i in range(ny):
            x_copy(j, i, x).wait_send()
        passed = pass_on(tx_o, lax.rem(x + j, nx), fx_s.at[j - 1], fx_r.at[j - 1])
        passed.wait_send()
        other_half = pl.ds(pl.multiple_of((1 - core) * (rows // 2), rows // 2), rows // 2)
        pltpu.make_async_remote_copy(
            src_ref=tx_o.at[lax.rem(x + j, nx), other_half],
            dst_ref=tx_o.at[lax.rem(x + j, nx), other_half],
            send_sem=fx_s.at[j - 1],
            recv_sem=fx_r.at[j - 1],
            device_id={"tp": partner},
            device_id_type=MESH,
        ).wait_recv()
    for j in range(1, ny):
        y_copy(j, y).wait_send()
        passed = pass_on(ty_o, lax.rem(y + j, ny), fy_s.at[j - 1], fy_r.at[j - 1])
        passed.wait_send()
        other_half = pl.ds(pl.multiple_of((1 - core) * (rows // 2), rows // 2), rows // 2)
        pltpu.make_async_remote_copy(
            src_ref=ty_o.at[lax.rem(y + j, ny), other_half],
            dst_ref=ty_o.at[lax.rem(y + j, ny), other_half],
            send_sem=fy_s.at[j - 1],
            recv_sem=fy_r.at[j - 1],
            device_id={"tp": partner},
            device_id_type=MESH,
        ).wait_recv()


def attention_core(nctx, ntp, nx, tokens, w_query, w_key, w_value, w_out, block_doc, grad_out):
    rows, width = tokens.shape
    cols = w_query.shape[1]
    heads = cols // HDIM
    own_blocks = rows // BLOCK
    all_blocks = nctx * own_blocks
    per = 2 * own_blocks
    units = rows // PAIR * heads
    ny = nctx // nx
    small = jax.ShapeDtypeStruct((rows, cols), BF)
    hbm = pl.BlockSpec(memory_space=pl.ANY)
    dma = pltpu.SemaphoreType.DMA
    return pl.pallas_call(
        functools.partial(core_kernel, nctx, ntp, nx),
        out_shape=(
            small,
            small,
            small,
            small,
            jax.ShapeDtypeStruct((2, nx, ny, cols // 2, width // nctx), BF),
            jax.ShapeDtypeStruct((nx, rows, width // nx), BF),
            jax.ShapeDtypeStruct((ny, rows, width // ny), BF),
        ),
        in_specs=[hbm] * 5 + [pl.BlockSpec(memory_space=pltpu.VMEM), hbm],
        out_specs=(hbm,) * 7,
        scratch_shapes=[
            pltpu.VMEM((rows, width), BF),
            pltpu.VMEM((3, width, cols), BF),
            pltpu.VMEM((cols, width), BF),
            pltpu.VMEM((3, rows, cols), BF),
            pltpu.VMEM((rows, width), BF),
            pltpu.VMEM((nctx, per, cols), BF),
            pltpu.VMEM((all_blocks, cols), BF),
            pltpu.VMEM((all_blocks, cols), BF),
            pltpu.VMEM((units, PAIR, PAIR + all_blocks), BF),
            pltpu.VMEM((rows, cols), BF),
            pltpu.VMEM((rows, cols), BF),
            pltpu.VMEM((rows, cols), BF),
            pltpu.VMEM((rows, cols), BF),
            pltpu.VMEM((rows, cols), BF),
            pltpu.VMEM((rows, cols), F32),
            pltpu.VMEM((rows, cols), F32),
            pltpu.VMEM((all_blocks, cols), F32),
            pltpu.VMEM((all_blocks, cols), F32),
            pltpu.VMEM((nctx, per, cols), BF),
            pltpu.VMEM((nctx, per, cols), BF),
            pltpu.VMEM((2, nx, ny, cols // 2, width // nctx), BF),
            dma((6,)),
            dma((5,)),
            dma((ntp // 2,)),
            dma((ntp,)),
            dma((ntp // 2,)),
            dma((nctx - 1,)),
            dma((nctx,)),
            dma((nctx - 1,)),
            dma((nctx,)),
            dma((nx - 1, ny)),
            dma((nx, ny)),
            dma((ny - 1,)),
            dma((ny,)),
            dma((ny + 1,)),
            dma((nx - 1,)),
            dma((nx - 1,)),
            dma((ny - 1,)),
            dma((ny - 1,)),
        ],
        compiler_params=pltpu.CompilerParams(
            collective_id=1, has_side_effects=True, vmem_limit_bytes=64 * 1024 * 1024 - 65536
        ),
        name="attention_core",
    )(tokens, w_query, w_key, w_value, w_out, block_doc.reshape(1, -1), grad_out)


def grad_kernel(
    nctx,
    ntp,
    nx,
    dq_h,
    dk_h,
    dv_h,
    attn_h,
    wos_h,
    tx_h,
    ty_h,
    wq_h,
    wk_h,
    wv_h,
    wo_h,
    tok_h,
    go_h,
    out_o,
    gt_o,
    gq_o,
    gk_o,
    gv_o,
    gwo_o,
    w3,
    wo,
    dcat,
    attn,
    rest,
    rest_g,
    gq,
    gk,
    gvx,
    gvy,
    o_p,
    o_q,
    o_z,
    o_a,
    d_p,
    d_q,
    d_z,
    d_a,
    sq,
    sk,
    sv,
    rq,
    rk,
    rv,
    oq,
    ok,
    ov,
    wo_own,
    wo_nb,
    wo_far,
    wo_r,
    wo_t,
    wo_u,
    wo_a,
    ld,
    ag_s,
    ag_r,
    op_s,
    op_r,
    oz_s,
    oz_r,
    dp_s,
    dp_r,
    dz_s,
    dz_r,
    rf_s,
    rf_r,
    rs_s,
    rs_r,
    w0_s,
    w0_r,
    w1_s,
    w1_r,
    w2_s,
    w2_r,
):
    ctx = lax.axis_index("ctx")
    tp = lax.axis_index("tp")
    ny = nctx // nx
    nz = ntp // 2
    y = lax.div(ctx, nx)
    x = lax.rem(ctx, nx)
    core = lax.rem(tp, 2)
    z = lax.div(tp, 2)
    partner = tp + 1 - 2 * core
    rows, cols = attn.shape
    width = wo.shape[1]
    strip = width // nctx
    gathered = nx * rows
    half = cols // 2

    def block(t):
        return pl.ds(pl.multiple_of(t * cols, cols), cols)

    def strip_at(i):
        return pl.ds(pl.multiple_of(i * strip, strip), strip)

    def at_x(i):
        return {"ctx": y * nx + i}

    def at_y(i):
        return {"ctx": i * nx + x}

    def remote(source, target, send, recv, where):
        return pltpu.make_async_remote_copy(
            src_ref=source,
            dst_ref=target,
            send_sem=send,
            recv_sem=recv,
            device_id=where,
            device_id_type=MESH,
        )

    loads = [
        pltpu.make_async_copy(attn_h, attn, ld.at[0]),
        pltpu.make_async_copy(wo_h, wo, ld.at[1]),
    ]
    for i, (d_h, w_h) in enumerate(((dq_h, wq_h), (dk_h, wk_h), (dv_h, wv_h))):
        lanes = pl.ds(i * cols, cols)
        loads.append(pltpu.make_async_copy(d_h, dcat.at[:, lanes], ld.at[2 + 2 * i]))
        loads.append(pltpu.make_async_copy(w_h, w3.at[:, lanes], ld.at[3 + 2 * i]))
    loads.append(pltpu.make_async_copy(tok_h.at[:, block(tp)], rest, ld.at[8]))
    loads.append(pltpu.make_async_copy(go_h, rest_g, ld.at[9]))
    lo = pl.ds(0, half)
    hi = pl.ds(half, half)
    gathers = (
        (dq_h, gq, x, at_x, 0),
        (dk_h, gk, y, at_y, 1),
        (dv_h.at[:, lo], gvx, x, at_x, 2),
        (dv_h.at[:, hi], gvy, y, at_y, 3),
    )
    for source, buf, pos, at, i in gathers:
        loads.append(pltpu.make_async_copy(source, buf.at[pos], ld.at[10 + i]))
    rings = ((x, nx, at_x), (y, ny, at_y))
    for side in range(2):
        pos, n, at = rings[side]
        for k, target in ((0, wo_own), (1, wo_nb.at[:, 0]), (n - 1, wo_nb.at[:, 1])):
            loads.append(
                pltpu.make_async_copy(
                    wos_h.at[side, lax.rem(pos + k, n)],
                    target.at[side],
                    ld.at[14 + 3 * side + min(k, 2)],
                )
            )
    for load in loads:
        load.start()

    barrier = pltpu.get_barrier_semaphore()
    for j in range(1, nx):
        pl.semaphore_signal(
            barrier, inc=1, device_id=at_x(lax.rem(x + j, nx)), device_id_type=MESH
        )
    for j in range(1, ny):
        pl.semaphore_signal(
            barrier, inc=1, device_id=at_y(lax.rem(y + j, ny)), device_id_type=MESH
        )
    for j in range(1, nz):
        pl.semaphore_signal(
            barrier,
            inc=1,
            device_id={"tp": lax.rem(z + j, nz) * 2 + core},
            device_id_type=MESH,
        )
    pl.semaphore_signal(barrier, inc=1, device_id={"tp": partner}, device_id_type=MESH)
    pl.semaphore_wait(barrier, nx + ny + nz - 2)

    def near_send(gather, step):
        source, buf, pos, at, i = gather
        n = buf.shape[0]
        there = lax.rem(pos + (1 if step == 0 else n - 1), n)
        return remote(source, buf.at[pos], ag_s.at[i, step], ag_r.at[i, step], at(there))

    def near_recv(gather, step):
        source, buf, pos, at, i = gather
        n = buf.shape[0]
        owner = lax.rem(pos + (n - 1 if step == 0 else 1), n)
        return remote(source, buf.at[owner], ag_s.at[i, step], ag_r.at[i, step], at(owner))

    def relay(gather, step):
        source, buf, pos, at, i = gather
        n = buf.shape[0]
        part = pl.ds(0, rows // 2) if step == 0 else pl.ds(rows // 2, rows // 2)
        owner = lax.rem(pos + (n - 1 if step == 0 else 1), n)
        there = lax.rem(pos + (1 if step == 0 else n - 1), n)
        return remote(
            buf.at[owner, part],
            buf.at[owner, part],
            ag_s.at[i, 2 + step],
            ag_r.at[i, 2 + step],
            at(there),
        )

    def relay_recv(gather, step):
        source, buf, pos, at, i = gather
        n = buf.shape[0]
        part = pl.ds(0, rows // 2) if step == 0 else pl.ds(rows // 2, rows // 2)
        owner = lax.rem(pos + 2, n)
        return remote(
            buf.at[owner, part],
            buf.at[owner, part],
            ag_s.at[i, 2 + step],
            ag_r.at[i, 2 + step],
            at(owner),
        )

    for gather in gathers:
        near_send(gather, 0).start()
        near_send(gather, 1).start()

    subs = (pl.ds(0, nx // 2), pl.ds(nx // 2, nx // 2))

    def far_hop(side, way):
        pos, n, at = rings[side]
        return remote(
            wos_h.at[side, lax.rem(pos + 2, n), subs[way]],
            wo_far.at[side, subs[way]],
            w0_s.at[side, way],
            w0_r.at[side, way],
            at(lax.rem(pos + (1 if way == 0 else n - 1), n)),
        )

    def near_hop(side, way, added):
        pos, n, at = rings[side]
        part = subs[way if added else 1 - way]
        return remote(
            wo_nb.at[side, way, part],
            wo_r.at[side, way, part],
            w1_s.at[side, way, 1 if added else 0],
            w1_r.at[side, way, 1 if added else 0],
            at(lax.rem(pos + (1 if way == 0 else n - 1), n)),
        )

    for way in range(2):
        for side in range(2):
            far_hop(side, way).start()

    def out_chunk(t):
        return dot_nn(attn[...], wo[:, block(t)])

    def tok_chunk(t):
        return dot_nt(dcat[...], w3[block(t), :])

    def to_partner(i, chunk, p, q, p_s, p_r):
        return remote(p.at[i], q.at[i], p_s.at[i], p_r.at[i], {"tp": partner})

    def summed_over_heads(chunk, p, q, zb, acc, p_s, p_r, z_s, z_r):
        def first(i, carry):
            p[i] = chunk(i * 2 + 1 - core).astype(BF)
            to_partner(i, chunk, p, q, p_s, p_r).start()
            return carry

        lax.fori_loop(0, nz, first, 0)

        def second(j, carry):
            i = lax.rem(z + j, nz)
            part = chunk(i * 2 + core)
            copy = to_partner(i, chunk, p, q, p_s, p_r)
            copy.wait_send()
            copy.wait_recv()
            part = part + q[i].astype(F32)

            @pl.when(j < nz)
            def _():
                p[i] = part.astype(BF)
                remote(
                    p.at[i], zb.at[z], z_s.at[j - 1], z_r.at[z], {"tp": i * 2 + core}
                ).start()

            @pl.when(j == nz)
            def _():
                acc[...] = part

            return carry

        lax.fori_loop(1, nz + 1, second, 0)

    def from_heads(p, zb, acc, z_s, z_r):
        total = acc[...]
        for j in range(1, nz):
            i = lax.rem(z + j, nz)
            copy = remote(p.at[i], zb.at[i], z_s.at[j - 1], z_r.at[i], {"tp": i * 2 + core})
            copy.wait_send()
            copy.wait_recv()
            total = total + zb[i].astype(F32)
        return total

    loads[0].wait()
    loads[1].wait()
    summed_over_heads(out_chunk, o_p, o_q, o_z, o_a, op_s, op_r, oz_s, oz_r)
    for load in loads[2:8]:
        load.wait()
    summed_over_heads(tok_chunk, d_p, d_q, d_z, d_a, dp_s, dp_r, dz_s, dz_r)
    t_x = w3.at[pl.ds(0, gathered), pl.ds(0, width // nx)]
    t_y = w3.at[pl.ds(gathered, gathered), pl.ds(0, width // ny)]
    late = []
    for i in range(nx):
        part = pl.ds(i * rows, rows)
        late.append(pltpu.make_async_copy(tx_h.at[i], t_x.at[part], ld.at[20 + i]))
        late.append(pltpu.make_async_copy(ty_h.at[i], t_y.at[part], ld.at[20 + nx + i]))
    for load in late:
        load.start()

    for gather in gathers:
        for step in range(2):
            near_recv(gather, step).wait_recv()
            relay(gather, step).start()

    for load in loads[8:] + late:
        load.wait()

    for side in range(2):
        for way in range(2):
            near_hop(side, way, False).start()
    for side in range(2):
        for way in range(2):
            far_hop(side, way).wait_recv()
            part = subs[way]
            wo_nb[side, way, part] = (
                wo_nb[side, way, part].astype(F32) + wo_far[side, part].astype(F32)
            ).astype(BF)
            near_hop(side, way, True).start()

    sends = (
        (gathers[0], 0, sq, rq, oq, y, at_y, 0),
        (gathers[1], 1, sk, rk, ok, x, at_x, 1),
        (gathers[2], 0, sv.at[:, :, lo], rv.at[:, :, lo], ov.at[:, lo], y, at_y, 2),
        (gathers[3], 1, sv.at[:, :, hi], rv.at[:, :, hi], ov.at[:, hi], x, at_x, 3),
    )
    ends = (pl.ds(0, strip // 2), pl.ds(strip // 2, strip // 2))

    def weight_far(item, way):
        gather, side, s, r, o, pos, at, i = item
        n = nx
        return remote(
            s.at[0, ends[way]],
            r.at[0, ends[way]],
            rf_s.at[i, way],
            rf_r.at[i, way],
            at(lax.rem(pos + (1 if way == 0 else n - 1), n)),
        )

    def weight_near(item, way, added):
        gather, side, s, r, o, pos, at, i = item
        n = nx
        part = ends[way if added else 1 - way]
        return remote(
            s.at[1 + way, part],
            r.at[1 + way, part],
            rs_s.at[i, way, 1 if added else 0],
            rs_r.at[i, way, 1 if added else 0],
            at(lax.rem(pos + (1 if way == 0 else n - 1), n)),
        )

    for item in sends:
        gather, side, s, r, o, pos, at, i = item
        for step in range(2):
            relay_recv(gather, step).wait_recv()
        buf = gather[1]
        n = buf.shape[0]
        base = pl.ds(side * gathered, gathered)

        def weight_piece(k, carry):
            there = lax.rem(pos + 6 - k, n)
            part = dot_tn(
                w3[base, strip_at(there)], buf[...].reshape(gathered, buf.shape[2])
            )

            @pl.when(k == 0)
            def _():
                s[0] = part.astype(BF)
                weight_far(item, 0).start()
                weight_far(item, 1).start()

            @pl.when(k == 1)
            def _():
                s[1] = part.astype(BF)
                weight_near(item, 0, False).start()

            @pl.when(k == 2)
            def _():
                o[...] = part

            @pl.when(k == 3)
            def _():
                s[2] = part.astype(BF)
                weight_near(item, 1, False).start()

            return carry

        lax.fori_loop(0, n, weight_piece, 0)

    for item in sends:
        gather, side, s, r, o, pos, at, i = item
        for way in range(2):
            weight_far(item, way).wait_recv()
            part = ends[way]
            s[1 + way, part] = (
                s[1 + way, part].astype(F32) + r[0, part].astype(F32)
            ).astype(BF)
            weight_near(item, way, True).start()

    out_o[...] = (rest[...].astype(F32) + from_heads(o_p, o_z, o_a, oz_s, oz_r)).astype(BF)
    gt_o[...] = (rest_g[...].astype(F32) + from_heads(d_p, d_z, d_a, dz_s, dz_r)).astype(BF)

    def second_hop(side, there, slot, owner):
        pos, n, at = ((y, ny, at_y), (x, nx, at_x))[side]
        return remote(
            wo_t.at[side, there],
            wo_u.at[side, owner],
            w2_s.at[side, slot],
            w2_r.at[side, owner],
            at(there),
        )

    for side in range(2):
        pos, m = ((y, ny), (x, nx))[side]
        for way in range(2):
            far_hop(side, way).wait_send()
            for added in (False, True):
                copy = near_hop(side, way, added)
                copy.wait_send()
                copy.wait_recv()

        def add_up(j, carry):
            there = lax.rem(pos + j, m)
            total = wo_own[side, there].astype(F32)
            for way in range(2):
                total = total + wo_r[side, way, there].astype(F32)

            @pl.when(j < m)
            def _():
                wo_t[side, there] = total.astype(BF)
                second_hop(side, there, j - 1, pos).start()

            @pl.when(j == m)
            def _():
                wo_a[pl.ds(side * half, half), :] = total

            return carry

        lax.fori_loop(1, m + 1, add_up, 0)

    for item, target in zip(sends, (gq_o, gk_o, gv_o.at[:, lo], gv_o.at[:, hi])):
        gather, side, s, r, o, pos, at, i = item
        for way in range(2):
            weight_far(item, way).wait_send()
            for added in (False, True):
                copy = weight_near(item, way, added)
                copy.wait_send()
                copy.wait_recv()
        target[...] = o[...] + r[1].astype(F32) + r[2].astype(F32)
        for step in range(2):
            near_send(gather, step).wait_send()
            relay(gather, step).wait_send()

    for side in range(2):
        pos, m = ((y, ny), (x, nx))[side]
        total = wo_a[pl.ds(side * half, half), :]
        for j in range(1, m):
            there = lax.rem(pos + j, m)
            copy = second_hop(side, there, j - 1, there)
            copy.wait_send()
            copy.wait_recv()
            total = total + wo_u[side, there].astype(F32)
        gwo_o[pl.ds(side * half, half), :] = total


def gradients(nctx, ntp, nx, core_out, tokens, w_query, w_key, w_value, w_out, grad_out):
    attn, d_query, d_key, d_value, wos, tx, ty = core_out
    rows, width = tokens.shape
    cols = w_query.shape[1]
    ny = nctx // nx
    nz = ntp // 2
    strip = width // nctx
    half = cols // 2
    hbm = pl.BlockSpec(memory_space=pl.ANY)
    vmem = pl.BlockSpec(memory_space=pltpu.VMEM)
    dma = pltpu.SemaphoreType.DMA
    small = jax.ShapeDtypeStruct((rows, cols), BF)
    piece = jax.ShapeDtypeStruct((strip, cols), F32)
    heads_scratch = [
        pltpu.VMEM((nz, rows, cols), BF),
        pltpu.VMEM((nz, rows, cols), BF),
        pltpu.VMEM((nz, rows, cols), BF),
        pltpu.VMEM((rows, cols), F32),
    ]
    return pl.pallas_call(
        functools.partial(grad_kernel, nctx, ntp, nx),
        out_shape=(
            small,
            small,
            piece,
            piece,
            piece,
            jax.ShapeDtypeStruct((cols, strip), F32),
        ),
        in_specs=[hbm] * 13,
        out_specs=(vmem,) * 6,
        scratch_shapes=[
            pltpu.VMEM((width, 3 * cols), BF),
            pltpu.VMEM((cols, width), BF),
            pltpu.VMEM((rows, 3 * cols), BF),
            pltpu.VMEM((rows, cols), BF),
            pltpu.VMEM((rows, cols), BF),
            pltpu.VMEM((rows, cols), BF),
            pltpu.VMEM((nx, rows, cols), BF),
            pltpu.VMEM((ny, rows, cols), BF),
            pltpu.VMEM((nx, rows, half), BF),
            pltpu.VMEM((ny, rows, half), BF),
            *heads_scratch,
            *heads_scratch,
            pltpu.VMEM((3, strip, cols), BF),
            pltpu.VMEM((3, strip, cols), BF),
            pltpu.VMEM((3, strip, cols), BF),
            pltpu.VMEM((3, strip, cols), BF),
            pltpu.VMEM((3, strip, cols), BF),
            pltpu.VMEM((3, strip, cols), BF),
            pltpu.VMEM((strip, cols), F32),
            pltpu.VMEM((strip, cols), F32),
            pltpu.VMEM((strip, cols), F32),
            pltpu.VMEM((2, ny, half, strip), BF),
            pltpu.VMEM((2, 2, ny, half, strip), BF),
            pltpu.VMEM((2, ny, half, strip), BF),
            pltpu.VMEM((2, 2, ny, half, strip), BF),
            pltpu.VMEM((2, ny, half, strip), BF),
            pltpu.VMEM((2, ny, half, strip), BF),
            pltpu.VMEM((cols, strip), F32),
            dma((20 + nx + ny,)),
            dma((4, 4)),
            dma((4, 4)),
            dma((nz,)),
            dma((nz,)),
            dma((nz - 1,)),
            dma((nz,)),
            dma((nz,)),
            dma((nz,)),
            dma((nz - 1,)),
            dma((nz,)),
            dma((4, 2)),
            dma((4, 2)),
            dma((4, 2, 2)),
            dma((4, 2, 2)),
            dma((2, 2)),
            dma((2, 2)),
            dma((2, 2, 2)),
            dma((2, 2, 2)),
            dma((2, nx - 1)),
            dma((2, nx)),
        ],
        compiler_params=pltpu.CompilerParams(
            collective_id=2, has_side_effects=True, vmem_limit_bytes=64 * 1024 * 1024 - 65536
        ),
        name="gradients",
    )(
        d_query,
        d_key,
        d_value,
        attn,
        wos,
        tx,
        ty,
        w_query,
        w_key,
        w_value,
        w_out,
        tokens,
        grad_out,
    )


def settle_kernel(count, *refs):
    ins, outs, bufs = refs[:count], refs[count : 2 * count], refs[2 * count : 3 * count]
    come, go = refs[3 * count :]
    first = [pltpu.make_async_copy(ins[i], bufs[i], come.at[i]) for i in range(count)]
    second = [pltpu.make_async_copy(bufs[i], outs[i], go.at[i]) for i in range(count)]
    for copy in first:
        copy.start()
    for i in range(count):
        first[i].wait()
        second[i].start()
    for copy in second:
        copy.wait()


def settled(arrays):
    count = len(arrays)
    hbm = pl.BlockSpec(memory_space=pl.ANY)
    shapes = [(a.shape, a.dtype) for a in arrays]
    return pl.pallas_call(
        functools.partial(settle_kernel, count),
        out_shape=tuple(jax.ShapeDtypeStruct(*s) for s in shapes),
        in_specs=[hbm] * count,
        out_specs=(hbm,) * count,
        scratch_shapes=[pltpu.VMEM(*s) for s in shapes]
        + [pltpu.SemaphoreType.DMA((count,)), pltpu.SemaphoreType.DMA((count,))],
        name="settled",
    )(*arrays)


def per_device(nctx, ntp, nx, tokens, w_query, w_key, w_value, w_out, block_doc, grad_out):
    core_out = attention_core(
        nctx, ntp, nx, tokens, w_query, w_key, w_value, w_out, block_doc, grad_out
    )
    return settled(
        gradients(nctx, ntp, nx, core_out, tokens, w_query, w_key, w_value, w_out, grad_out)
    )


def solution(mesh):
    in_specs = (
        P("ctx", None),
        P(None, "tp"),
        P(None, "tp"),
        P(None, "tp"),
        P("tp", None),
        P(),
        P("ctx", "tp"),
    )
    out_specs = (
        P("ctx", "tp"),
        P("ctx", "tp"),
        P("ctx", "tp"),
        P("ctx", "tp"),
        P("ctx", "tp"),
        P("tp", "ctx"),
    )
    return jax.shard_map(
        functools.partial(per_device, mesh.shape["ctx"], mesh.shape["tp"], math.isqrt(mesh.shape["ctx"])),
        mesh=mesh,
        in_specs=in_specs,
        out_specs=out_specs,
        check_vma=False,
    )
```

```python
import functools
import math

import jax
import jax.numpy as jnp
from jax import lax
from jax.experimental import pallas as pl
from jax.experimental.pallas import tpu as pltpu
from jax.sharding import PartitionSpec as P

HDIM = 128
BLOCK = 64
PAIR = 2 * BLOCK
MESH = pl.DeviceIdType.MESH
BF = jnp.bfloat16
F32 = jnp.float32
big_negative = -1e30


def dot_nn(a, b):
    return lax.dot_general(a, b, (((1,), (0,)), ((), ())), preferred_element_type=F32)


def dot_nt(a, b):
    return lax.dot_general(a, b, (((1,), (1,)), ((), ())), preferred_element_type=F32)


def dot_tn(a, b):
    return lax.dot_general(a, b, (((0,), (0,)), ((), ())), preferred_element_type=F32)


def iota(shape, dim):
    return lax.broadcasted_iota(jnp.int32, shape, dim)


def one_hot(hit):
    return jnp.where(hit, 1.0, 0.0).astype(BF)


def core_kernel(
    nctx,
    ntp,
    nx,
    tok_h,
    wq_h,
    wk_h,
    wv_h,
    wo_h,
    doc_ref,
    go_h,
    attn_o,
    dq_o,
    dk_o,
    dv_o,
    wos_o,
    tx_o,
    ty_o,
    tok,
    w3,
    wo,
    qkv,
    gfull,
    land,
    lk,
    lv,
    pw,
    attn,
    da,
    dqv,
    dkv,
    dvv,
    dkf,
    dvf,
    dlk,
    dlv,
    dls,
    dlr,
    wos,
    acc,
    ld,
    st,
    g_s,
    g_r,
    f_s,
    l_s,
    l_r,
    d_s,
    d_r,
    tx_s,
    tx_r,
    ty_s,
    ty_r,
    t_l,
    fx_s,
    fx_r,
    fy_s,
    fy_r,
    h_s,
    h_r,
):
    ctx = lax.axis_index("ctx")
    ny = nctx // nx
    y = lax.div(ctx, nx)
    x = lax.rem(ctx, nx)
    tp = lax.axis_index("tp")
    nz = ntp // 2
    core = lax.rem(tp, 2)
    z = lax.div(tp, 2)
    partner = tp + 1 - 2 * core
    rows, width = tok.shape
    cols = qkv.shape[2]
    heads = cols // HDIM
    own_blocks = rows // BLOCK
    all_blocks = nctx * own_blocks
    per = 2 * own_blocks
    scale = 1.0 / math.sqrt(HDIM)

    def shard(t):
        return pl.ds(pl.multiple_of(t * cols, cols), cols)

    def mate(j, side):
        return lax.rem(z + j, nz) * 2 + side

    load_tok = pltpu.make_async_copy(tok_h, tok, ld.at[0])
    load_tok.start()
    for i, w_h in enumerate((wk_h, wv_h, wq_h)):
        pltpu.make_async_copy(w_h, w3.at[i], ld.at[1 + i]).start()
    load_wo = pltpu.make_async_copy(wo_h, wo, ld.at[4])
    load_wo.start()
    load_go = pltpu.make_async_copy(go_h, gfull.at[:, shard(tp)], ld.at[5])
    load_go.start()

    barrier = pltpu.get_barrier_semaphore()

    def greet(i, carry):
        pl.semaphore_signal(
            barrier, inc=1, device_id={"ctx": lax.rem(ctx + i, nctx)}, device_id_type=MESH
        )
        return carry

    lax.fori_loop(1, nctx, greet, 0)
    pl.semaphore_signal(barrier, inc=1, device_id={"tp": partner}, device_id_type=MESH)
    for j in range(1, nz):
        pl.semaphore_signal(barrier, inc=1, device_id={"tp": mate(j, core)}, device_id_type=MESH)
    pl.semaphore_wait(barrier, nctx - 1 + nz)

    def grad_copy(source, owner, send, target):
        return pltpu.make_async_remote_copy(
            src_ref=source,
            dst_ref=gfull.at[:, shard(owner)],
            send_sem=send,
            recv_sem=g_r.at[owner],
            device_id={"tp": target},
            device_id_type=MESH,
        )

    first_sends = [
        grad_copy(go_h, tp, g_s.at[0], mate(1, core)),
        grad_copy(go_h, tp, g_s.at[1], mate(nz - 1, core)),
        grad_copy(go_h, tp, g_s.at[2], partner),
    ]
    for send in first_sends:
        send.start()

    load_tok.wait()

    half = cols // 2

    def project(i, carry):
        pltpu.make_async_copy(wk_h, w3.at[i], ld.at[1 + i]).wait()

        def piece(n, inner):
            at = pl.ds(pl.multiple_of(n * half, half), half)
            qkv[i, :, at] = dot_nn(tok[...], w3[i, :, at]).astype(BF)
            return inner

        lax.fori_loop(0, 2, piece, 0)

        @pl.when(i == 1)
        def _():
            r = iota((per, rows), 0)
            c = iota((per, rows), 1)
            pick_k = one_hot(c == r * BLOCK + BLOCK - 1)
            pick_v = one_hot(c == (r - own_blocks) * BLOCK + BLOCK - 1)
            pick_k = jnp.where(r < own_blocks, pick_k, jnp.zeros_like(pick_k))
            pick_v = jnp.where(r >= own_blocks, pick_v, jnp.zeros_like(pick_v))
            land[ctx] = (dot_nn(pick_k, qkv[0]) + dot_nn(pick_v, qkv[1])).astype(BF)

            def spread(j, inner):
                pltpu.make_async_remote_copy(
                    src_ref=land.at[ctx],
                    dst_ref=land.at[ctx],
                    send_sem=l_s.at[j - 1],
                    recv_sem=l_r.at[ctx],
                    device_id={"ctx": lax.rem(ctx + j, nctx)},
                    device_id_type=MESH,
                ).start()
                return inner

            lax.fori_loop(1, nctx, spread, 0)

        return carry

    lax.fori_loop(0, 3, project, 0)

    def land_wait(j, carry):
        source = lax.rem(ctx + j, nctx)
        copy = pltpu.make_async_remote_copy(
            src_ref=land.at[ctx],
            dst_ref=land.at[source],
            send_sem=l_s.at[j - 1],
            recv_sem=l_r.at[source],
            device_id={"ctx": source},
            device_id_type=MESH,
        )
        copy.wait_send()
        copy.wait_recv()
        return carry

    def row_half(way):
        return pl.ds(way * (rows // 2), rows // 2)

    def relay(way):
        owner = mate(nz - 1 if way == 0 else 1, core)
        view = gfull.at[row_half(way), shard(owner)]
        return pltpu.make_async_remote_copy(
            src_ref=view,
            dst_ref=view,
            send_sem=h_s.at[way],
            recv_sem=h_r.at[way],
            device_id={"tp": mate(1 if way == 0 else nz - 1, core)},
            device_id_type=MESH,
        )

    def relay_wait(way):
        view = gfull.at[row_half(way), shard(mate(2, core))]
        pltpu.make_async_remote_copy(
            src_ref=view,
            dst_ref=view,
            send_sem=h_s.at[way],
            recv_sem=h_r.at[way],
            device_id={"tp": mate(nz - 1 if way == 0 else 1, core)},
            device_id_type=MESH,
        ).wait_recv()

    lax.fori_loop(1, nctx, land_wait, 0)

    forwards = []

    def pass_shard(owner, slot):
        onward = grad_copy(gfull.at[:, shard(owner)], owner, f_s.at[slot], partner)
        onward.start()
        forwards.append(onward)

    for way in range(2):
        owner = mate(nz - 1 if way == 0 else 1, core)
        grad_copy(gfull.at[:, shard(owner)], owner, f_s.at[way], partner).wait_recv()
        relay(way).start()
        pass_shard(owner, way)

    strip = width // nctx
    own_half = pl.ds(pl.multiple_of(core * (rows // 2), rows // 2), rows // 2)

    def strip_at(i):
        return pl.ds(pl.multiple_of(i * strip, strip), strip)

    def x_copy(j, i, owner):
        return pltpu.make_async_remote_copy(
            src_ref=tok.at[own_half, strip_at(i * nx + lax.rem(x + j, nx))],
            dst_ref=tx_o.at[owner, own_half, strip_at(i)],
            send_sem=tx_s.at[j - 1, i],
            recv_sem=tx_r.at[owner, i],
            device_id={"ctx": y * nx + lax.rem(x + j, nx)},
            device_id_type=MESH,
        )

    def y_copy(j, owner):
        there = lax.rem(y + j, ny)
        return pltpu.make_async_remote_copy(
            src_ref=tok.at[own_half, pl.ds(pl.multiple_of(there * nx * strip, strip), nx * strip)],
            dst_ref=ty_o.at[owner, own_half],
            send_sem=ty_s.at[j - 1],
            recv_sem=ty_r.at[owner],
            device_id={"ctx": there * nx + x},
            device_id_type=MESH,
        )

    def pass_on(ref, owner, send, recv):
        return pltpu.make_async_remote_copy(
            src_ref=ref.at[owner, own_half],
            dst_ref=ref.at[owner, own_half],
            send_sem=send,
            recv_sem=recv,
            device_id={"tp": partner},
            device_id_type=MESH,
        )

    for j in (1, 3, 2):
        for i in range(ny):
            x_copy(j, i, x).start()
        y_copy(j, y).start()
    own_strips = [
        pltpu.make_async_copy(
            tok.at[:, strip_at(i * nx + x)], tx_o.at[x, :, strip_at(i)], t_l.at[i]
        )
        for i in range(ny)
    ]
    own_strips.append(
        pltpu.make_async_copy(
            tok.at[:, pl.ds(pl.multiple_of(y * nx * strip, strip), nx * strip)],
            ty_o.at[y],
            t_l.at[ny],
        )
    )
    for copy in own_strips:
        copy.start()

    b = iota((all_blocks, nctx * per), 0)
    c = iota((all_blocks, nctx * per), 1)
    shift = b // own_blocks * own_blocks
    landed = land[...].reshape(nctx * per, cols)
    lk[...] = dot_nn(one_hot(c == b + shift), landed).astype(BF)
    lv[...] = dot_nn(one_hot(c == b + shift + own_blocks), landed).astype(BF)

    span = PAIR + all_blocks
    doc = doc_ref[...]
    doc_lane = iota(doc.shape, 1)
    doc_wide = jnp.concatenate([jnp.zeros((1, PAIR), jnp.int32), doc], axis=1)

    def forward(sb, carry):
        at = pl.ds(pl.multiple_of(sb * PAIR, PAIR), PAIR)
        row = iota((PAIR, span), 0)
        col = iota((PAIR, span), 1)
        upper = jnp.where(row >= BLOCK, 1, 0)
        col_upper = jnp.where(col >= BLOCK, 1, 0)
        first = ctx * own_blocks + sb * 2
        doc_a = jnp.sum(jnp.where(doc_lane == first, doc, 0), axis=1, keepdims=True)
        doc_b = jnp.sum(jnp.where(doc_lane == first + 1, doc, 0), axis=1, keepdims=True)
        own_doc = jnp.where(row >= BLOCK, doc_b, doc_a)
        near = (col < PAIR) & (upper == col_upper) & (col <= row)
        far = (col >= PAIR) & (col - PAIR < first + upper) & (doc_wide == own_doc)
        mask = near | far
        for h in range(heads):
            hs = pl.ds(h * HDIM, HDIM)
            keys = jnp.concatenate([qkv[0, at, hs], lk[:, hs]], axis=0)
            values = jnp.concatenate([qkv[1, at, hs], lv[:, hs]], axis=0)
            scores = dot_nt(qkv[2, at, hs], keys) * scale
            scores = jnp.where(mask, scores, big_negative)
            top = jnp.max(scores, axis=1, keepdims=True)
            e = jnp.exp(scores - top)
            weight = (e / jnp.sum(e, axis=1, keepdims=True)).astype(BF)
            pw[sb * heads + h] = weight
            attn[at, hs] = dot_nn(weight, values).astype(BF)
        return carry

    lax.fori_loop(0, rows // PAIR, forward, 0)
    out_attn = pltpu.make_async_copy(attn, attn_o, st.at[0])
    out_attn.start()

    load_go.wait()
    load_wo.wait()
    acc[...] = jnp.zeros_like(acc)

    def use_shard(t):
        grads = gfull[:, shard(t)]
        acc[...] += dot_nt(grads, wo[:, shard(t)])
        part = dot_tn(attn[...], grads).astype(BF)
        for k in range(nctx // ntp):
            i = t * (nctx // ntp) + k
            there_y = lax.div(i, nx)
            there_x = lax.rem(i, nx)
            wos[0, there_x, there_y] = part[: cols // 2, k * strip : (k + 1) * strip]
            wos[1, there_y, there_x] = part[cols // 2 :, k * strip : (k + 1) * strip]

    def use_near(i, carry):
        side = jnp.where(lax.rem(i, 2) == 0, core, 1 - core)
        hop = jnp.where(i < 2, 0, jnp.where(i < 4, 1, nz - 1))
        t = mate(hop, side)

        @pl.when((i == 1) | (i == 3) | (i == 5))
        def _():
            grad_copy(gfull.at[:, shard(t)], t, f_s.at[0], partner).wait_recv()

        use_shard(t)
        return carry

    lax.fori_loop(0, 6, use_near, 0)
    for way in range(2):
        relay_wait(way)
    pass_shard(mate(2, core), 2)

    def use_far(i, carry):
        t = mate(2, jnp.where(i == 0, core, 1 - core))

        @pl.when(i == 1)
        def _():
            grad_copy(gfull.at[:, shard(t)], t, f_s.at[2], partner).wait_recv()

        use_shard(t)
        return carry

    lax.fori_loop(0, 2, use_far, 0)
    da[...] = acc[...].astype(BF)
    out_wos = pltpu.make_async_copy(wos, wos_o, st.at[4])
    out_wos.start()

    dlk[...] = jnp.zeros_like(dlk)
    dlv[...] = jnp.zeros_like(dlv)

    def backward(sb, carry):
        at = pl.ds(pl.multiple_of(sb * PAIR, PAIR), PAIR)
        for h in range(heads):
            hs = pl.ds(h * HDIM, HDIM)
            keys = jnp.concatenate([qkv[0, at, hs], lk[:, hs]], axis=0)
            values = jnp.concatenate([qkv[1, at, hs], lv[:, hs]], axis=0)
            weight = pw[sb * heads + h]
            d_out = da[at, hs]
            delta = jnp.sum(
                attn[at, hs].astype(F32) * d_out.astype(F32), axis=1, keepdims=True
            )
            d_weight = dot_nt(d_out, values)
            ds = (weight.astype(F32) * (d_weight - delta)).astype(BF)
            dqv[at, hs] = (dot_nn(ds, keys) * scale).astype(BF)
            d_keys = dot_tn(ds, qkv[2, at, hs]) * scale
            d_values = dot_tn(weight, d_out)
            dkf[at, hs] = d_keys[:PAIR]
            dvf[at, hs] = d_values[:PAIR]
            dlk[:, hs] += d_keys[PAIR:]
            dlv[:, hs] += d_values[PAIR:]
        return carry

    lax.fori_loop(0, rows // PAIR, backward, 0)
    out_dq = pltpu.make_async_copy(dqv, dq_o, st.at[1])
    out_dq.start()

    r = iota((nctx * per, all_blocks), 0)
    b = iota((nctx * per, all_blocks), 1)
    shift = b // own_blocks * own_blocks
    packed = dot_nn(one_hot(r == b + shift), dlk[...].astype(BF)) + dot_nn(
        one_hot(r == b + shift + own_blocks), dlv[...].astype(BF)
    )
    dls[...] = packed.astype(BF).reshape(nctx, per, cols)

    def give(j, carry):
        target = lax.rem(ctx + j, nctx)
        pltpu.make_async_remote_copy(
            src_ref=dls.at[target],
            dst_ref=dlr.at[ctx],
            send_sem=d_s.at[j - 1],
            recv_sem=d_r.at[ctx],
            device_id={"ctx": target},
            device_id_type=MESH,
        ).start()
        return carry

    lax.fori_loop(1, nctx, give, 0)
    dlr[ctx] = dls[ctx]

    for j in range(1, nx):
        owner = lax.rem(x + j, nx)
        for i in range(ny):
            x_copy(j, i, owner).wait_recv()
        pass_on(tx_o, owner, fx_s.at[j - 1], fx_r.at[j - 1]).start()
    for j in range(1, ny):
        owner = lax.rem(y + j, ny)
        y_copy(j, owner).wait_recv()
        pass_on(ty_o, owner, fy_s.at[j - 1], fy_r.at[j - 1]).start()

    def take(j, carry):
        source = lax.rem(ctx + j, nctx)
        copy = pltpu.make_async_remote_copy(
            src_ref=dls.at[source],
            dst_ref=dlr.at[source],
            send_sem=d_s.at[j - 1],
            recv_sem=d_r.at[source],
            device_id={"ctx": source},
            device_id_type=MESH,
        )
        copy.wait_send()
        copy.wait_recv()
        return carry

    lax.fori_loop(1, nctx, take, 0)
    total = jnp.zeros((per, cols), F32)
    for i in range(nctx):
        total = total + dlr[i].astype(F32)
    for i in range(own_blocks):
        last = pl.ds(i * BLOCK + BLOCK - 1, 1)
        dkf[last, :] += total[i : i + 1]
        dvf[last, :] += total[own_blocks + i : own_blocks + i + 1]
    dkv[...] = dkf[...].astype(BF)
    dvv[...] = dvf[...].astype(BF)
    out_dk = pltpu.make_async_copy(dkv, dk_o, st.at[2])
    out_dk.start()
    out_dv = pltpu.make_async_copy(dvv, dv_o, st.at[3])
    out_dv.start()
    for send in first_sends + forwards + [relay(0), relay(1)]:
        send.wait_send()
    for copy in [out_attn, out_dq, out_dk, out_dv, out_wos] + own_strips:
        copy.wait()
    for j in range(1, nx):
        for i in range(ny):
            x_copy(j, i, x).wait_send()
        passed = pass_on(tx_o, lax.rem(x + j, nx), fx_s.at[j - 1], fx_r.at[j - 1])
        passed.wait_send()
        other_half = pl.ds(pl.multiple_of((1 - core) * (rows // 2), rows // 2), rows // 2)
        pltpu.make_async_remote_copy(
            src_ref=tx_o.at[lax.rem(x + j, nx), other_half],
            dst_ref=tx_o.at[lax.rem(x + j, nx), other_half],
            send_sem=fx_s.at[j - 1],
            recv_sem=fx_r.at[j - 1],
            device_id={"tp": partner},
            device_id_type=MESH,
        ).wait_recv()
    for j in range(1, ny):
        y_copy(j, y).wait_send()
        passed = pass_on(ty_o, lax.rem(y + j, ny), fy_s.at[j - 1], fy_r.at[j - 1])
        passed.wait_send()
        other_half = pl.ds(pl.multiple_of((1 - core) * (rows // 2), rows // 2), rows // 2)
        pltpu.make_async_remote_copy(
            src_ref=ty_o.at[lax.rem(y + j, ny), other_half],
            dst_ref=ty_o.at[lax.rem(y + j, ny), other_half],
            send_sem=fy_s.at[j - 1],
            recv_sem=fy_r.at[j - 1],
            device_id={"tp": partner},
            device_id_type=MESH,
        ).wait_recv()


def attention_core(nctx, ntp, nx, tokens, w_query, w_key, w_value, w_out, block_doc, grad_out):
    rows, width = tokens.shape
    cols = w_query.shape[1]
    heads = cols // HDIM
    own_blocks = rows // BLOCK
    all_blocks = nctx * own_blocks
    per = 2 * own_blocks
    units = rows // PAIR * heads
    ny = nctx // nx
    small = jax.ShapeDtypeStruct((rows, cols), BF)
    hbm = pl.BlockSpec(memory_space=pl.ANY)
    dma = pltpu.SemaphoreType.DMA
    return pl.pallas_call(
        functools.partial(core_kernel, nctx, ntp, nx),
        out_shape=(
            small,
            small,
            small,
            small,
            jax.ShapeDtypeStruct((2, nx, ny, cols // 2, width // nctx), BF),
            jax.ShapeDtypeStruct((nx, rows, width // nx), BF),
            jax.ShapeDtypeStruct((ny, rows, width // ny), BF),
        ),
        in_specs=[hbm] * 5 + [pl.BlockSpec(memory_space=pltpu.VMEM), hbm],
        out_specs=(hbm,) * 7,
        scratch_shapes=[
            pltpu.VMEM((rows, width), BF),
            pltpu.VMEM((3, width, cols), BF),
            pltpu.VMEM((cols, width), BF),
            pltpu.VMEM((3, rows, cols), BF),
            pltpu.VMEM((rows, width), BF),
            pltpu.VMEM((nctx, per, cols), BF),
            pltpu.VMEM((all_blocks, cols), BF),
            pltpu.VMEM((all_blocks, cols), BF),
            pltpu.VMEM((units, PAIR, PAIR + all_blocks), BF),
            pltpu.VMEM((rows, cols), BF),
            pltpu.VMEM((rows, cols), BF),
            pltpu.VMEM((rows, cols), BF),
            pltpu.VMEM((rows, cols), BF),
            pltpu.VMEM((rows, cols), BF),
            pltpu.VMEM((rows, cols), F32),
            pltpu.VMEM((rows, cols), F32),
            pltpu.VMEM((all_blocks, cols), F32),
            pltpu.VMEM((all_blocks, cols), F32),
            pltpu.VMEM((nctx, per, cols), BF),
            pltpu.VMEM((nctx, per, cols), BF),
            pltpu.VMEM((2, nx, ny, cols // 2, width // nctx), BF),
            pltpu.VMEM((rows, cols), F32),
            dma((6,)),
            dma((5,)),
            dma((ntp // 2,)),
            dma((ntp,)),
            dma((ntp // 2,)),
            dma((nctx - 1,)),
            dma((nctx,)),
            dma((nctx - 1,)),
            dma((nctx,)),
            dma((nx - 1, ny)),
            dma((nx, ny)),
            dma((ny - 1,)),
            dma((ny,)),
            dma((ny + 1,)),
            dma((nx - 1,)),
            dma((nx - 1,)),
            dma((ny - 1,)),
            dma((ny - 1,)),
            dma((2,)),
            dma((2,)),
        ],
        compiler_params=pltpu.CompilerParams(
            collective_id=1, has_side_effects=True, vmem_limit_bytes=64 * 1024 * 1024 - 65536
        ),
        name="attention_core",
    )(tokens, w_query, w_key, w_value, w_out, block_doc.reshape(1, -1), grad_out)


def grad_kernel(
    nctx,
    ntp,
    nx,
    dq_h,
    dk_h,
    dv_h,
    attn_h,
    wos_h,
    tx_h,
    ty_h,
    wq_h,
    wk_h,
    wv_h,
    wo_h,
    tok_h,
    go_h,
    out_o,
    gt_o,
    gq_o,
    gk_o,
    gv_o,
    gwo_o,
    w3,
    wo,
    dcat,
    attn,
    rest,
    rest_g,
    gq,
    gk,
    gvx,
    gvy,
    o_p,
    o_q,
    o_z,
    o_a,
    d_p,
    d_q,
    d_z,
    d_a,
    sq,
    sk,
    sv,
    rq,
    rk,
    rv,
    oq,
    ok,
    ov,
    wo_own,
    wo_nb,
    wo_far,
    wo_r,
    wo_t,
    wo_u,
    wo_a,
    ld,
    ag_s,
    ag_r,
    op_s,
    op_r,
    oz_s,
    oz_r,
    dp_s,
    dp_r,
    dz_s,
    dz_r,
    rf_s,
    rf_r,
    rs_s,
    rs_r,
    w0_s,
    w0_r,
    w1_s,
    w1_r,
    w2_s,
    w2_r,
):
    ctx = lax.axis_index("ctx")
    tp = lax.axis_index("tp")
    ny = nctx // nx
    nz = ntp // 2
    y = lax.div(ctx, nx)
    x = lax.rem(ctx, nx)
    core = lax.rem(tp, 2)
    z = lax.div(tp, 2)
    partner = tp + 1 - 2 * core
    rows, cols = attn.shape
    width = wo.shape[1]
    strip = width // nctx
    gathered = nx * rows
    half = cols // 2

    def block(t):
        return pl.ds(pl.multiple_of(t * cols, cols), cols)

    def strip_at(i):
        return pl.ds(pl.multiple_of(i * strip, strip), strip)

    def at_x(i):
        return {"ctx": y * nx + i}

    def at_y(i):
        return {"ctx": i * nx + x}

    def remote(source, target, send, recv, where):
        return pltpu.make_async_remote_copy(
            src_ref=source,
            dst_ref=target,
            send_sem=send,
            recv_sem=recv,
            device_id=where,
            device_id_type=MESH,
        )

    loads = [
        pltpu.make_async_copy(attn_h, attn, ld.at[0]),
        pltpu.make_async_copy(wo_h, wo, ld.at[1]),
    ]
    for i, (d_h, w_h) in enumerate(((dq_h, wq_h), (dk_h, wk_h), (dv_h, wv_h))):
        lanes = pl.ds(i * cols, cols)
        loads.append(pltpu.make_async_copy(d_h, dcat.at[:, lanes], ld.at[2 + 2 * i]))
        loads.append(pltpu.make_async_copy(w_h, w3.at[:, lanes], ld.at[3 + 2 * i]))
    loads.append(pltpu.make_async_copy(tok_h.at[:, block(tp)], rest, ld.at[8]))
    loads.append(pltpu.make_async_copy(go_h, rest_g, ld.at[9]))
    lo = pl.ds(0, half)
    hi = pl.ds(half, half)
    gathers = (
        (dq_h, gq, x, at_x, 0),
        (dk_h, gk, y, at_y, 1),
        (dv_h.at[:, lo], gvx, x, at_x, 2),
        (dv_h.at[:, hi], gvy, y, at_y, 3),
    )
    for source, buf, pos, at, i in gathers:
        loads.append(pltpu.make_async_copy(source, buf.at[pos], ld.at[10 + i]))
    rings = ((x, nx, at_x), (y, ny, at_y))
    for side in range(2):
        pos, n, at = rings[side]
        for k, target in ((0, wo_own), (1, wo_nb.at[:, 0]), (n - 1, wo_nb.at[:, 1])):
            loads.append(
                pltpu.make_async_copy(
                    wos_h.at[side, lax.rem(pos + k, n)],
                    target.at[side],
                    ld.at[14 + 3 * side + min(k, 2)],
                )
            )
    for load in loads:
        load.start()

    barrier = pltpu.get_barrier_semaphore()
    for j in range(1, nx):
        pl.semaphore_signal(
            barrier, inc=1, device_id=at_x(lax.rem(x + j, nx)), device_id_type=MESH
        )
    for j in range(1, ny):
        pl.semaphore_signal(
            barrier, inc=1, device_id=at_y(lax.rem(y + j, ny)), device_id_type=MESH
        )
    for j in range(1, nz):
        pl.semaphore_signal(
            barrier,
            inc=1,
            device_id={"tp": lax.rem(z + j, nz) * 2 + core},
            device_id_type=MESH,
        )
    pl.semaphore_signal(barrier, inc=1, device_id={"tp": partner}, device_id_type=MESH)
    pl.semaphore_wait(barrier, nx + ny + nz - 2)

    def near_send(gather, step):
        source, buf, pos, at, i = gather
        n = buf.shape[0]
        there = lax.rem(pos + (1 if step == 0 else n - 1), n)
        return remote(source, buf.at[pos], ag_s.at[i, step], ag_r.at[i, step], at(there))

    def near_recv(gather, step):
        source, buf, pos, at, i = gather
        n = buf.shape[0]
        owner = lax.rem(pos + (n - 1 if step == 0 else 1), n)
        return remote(source, buf.at[owner], ag_s.at[i, step], ag_r.at[i, step], at(owner))

    def relay(gather, step):
        source, buf, pos, at, i = gather
        n = buf.shape[0]
        part = pl.ds(0, rows // 2) if step == 0 else pl.ds(rows // 2, rows // 2)
        owner = lax.rem(pos + (n - 1 if step == 0 else 1), n)
        there = lax.rem(pos + (1 if step == 0 else n - 1), n)
        return remote(
            buf.at[owner, part],
            buf.at[owner, part],
            ag_s.at[i, 2 + step],
            ag_r.at[i, 2 + step],
            at(there),
        )

    def relay_recv(gather, step):
        source, buf, pos, at, i = gather
        n = buf.shape[0]
        part = pl.ds(0, rows // 2) if step == 0 else pl.ds(rows // 2, rows // 2)
        owner = lax.rem(pos + 2, n)
        return remote(
            buf.at[owner, part],
            buf.at[owner, part],
            ag_s.at[i, 2 + step],
            ag_r.at[i, 2 + step],
            at(owner),
        )

    for gather in gathers:
        near_send(gather, 0).start()
        near_send(gather, 1).start()

    subs = (pl.ds(0, nx // 2), pl.ds(nx // 2, nx // 2))

    def far_hop(side, way):
        pos, n, at = rings[side]
        return remote(
            wos_h.at[side, lax.rem(pos + 2, n), subs[way]],
            wo_far.at[side, subs[way]],
            w0_s.at[side, way],
            w0_r.at[side, way],
            at(lax.rem(pos + (1 if way == 0 else n - 1), n)),
        )

    def near_hop(side, way, added):
        pos, n, at = rings[side]
        part = subs[way if added else 1 - way]
        return remote(
            wo_nb.at[side, way, part],
            wo_r.at[side, way, part],
            w1_s.at[side, way, 1 if added else 0],
            w1_r.at[side, way, 1 if added else 0],
            at(lax.rem(pos + (1 if way == 0 else n - 1), n)),
        )

    for way in range(2):
        for side in range(2):
            far_hop(side, way).start()

    def out_chunk(t):
        return dot_nn(attn[...], wo[:, block(t)])

    def tok_chunk(t):
        return dot_nt(dcat[...], w3[block(t), :])

    def to_partner(i, chunk, p, q, p_s, p_r):
        return remote(p.at[i], q.at[i], p_s.at[i], p_r.at[i], {"tp": partner})

    def summed_over_heads(chunk, p, q, zb, acc, p_s, p_r, z_s, z_r):
        def first(i, carry):
            p[i] = chunk(i * 2 + 1 - core).astype(BF)
            to_partner(i, chunk, p, q, p_s, p_r).start()
            return carry

        lax.fori_loop(0, nz, first, 0)

        def second(j, carry):
            i = lax.rem(z + j, nz)
            part = chunk(i * 2 + core)
            copy = to_partner(i, chunk, p, q, p_s, p_r)
            copy.wait_send()
            copy.wait_recv()
            part = part + q[i].astype(F32)

            @pl.when(j < nz)
            def _():
                p[i] = part.astype(BF)
                remote(
                    p.at[i], zb.at[z], z_s.at[j - 1], z_r.at[z], {"tp": i * 2 + core}
                ).start()

            @pl.when(j == nz)
            def _():
                acc[...] = part

            return carry

        lax.fori_loop(1, nz + 1, second, 0)

    def from_heads(p, zb, acc, z_s, z_r):
        total = acc[...]
        for j in range(1, nz):
            i = lax.rem(z + j, nz)
            copy = remote(p.at[i], zb.at[i], z_s.at[j - 1], z_r.at[i], {"tp": i * 2 + core})
            copy.wait_send()
            copy.wait_recv()
            total = total + zb[i].astype(F32)
        return total

    loads[0].wait()
    loads[1].wait()
    summed_over_heads(out_chunk, o_p, o_q, o_z, o_a, op_s, op_r, oz_s, oz_r)
    for load in loads[2:8]:
        load.wait()
    summed_over_heads(tok_chunk, d_p, d_q, d_z, d_a, dp_s, dp_r, dz_s, dz_r)
    t_x = w3.at[pl.ds(0, gathered), pl.ds(0, width // nx)]
    t_y = w3.at[pl.ds(gathered, gathered), pl.ds(0, width // ny)]
    late = []
    for i in range(nx):
        part = pl.ds(i * rows, rows)
        late.append(pltpu.make_async_copy(tx_h.at[i], t_x.at[part], ld.at[20 + i]))
        late.append(pltpu.make_async_copy(ty_h.at[i], t_y.at[part], ld.at[20 + nx + i]))
    for load in late:
        load.start()

    for gather in gathers:
        for step in range(2):
            near_recv(gather, step).wait_recv()
            relay(gather, step).start()

    for load in loads[8:] + late:
        load.wait()

    for side in range(2):
        for way in range(2):
            near_hop(side, way, False).start()
    for side in range(2):
        for way in range(2):
            far_hop(side, way).wait_recv()
            part = subs[way]
            wo_nb[side, way, part] = (
                wo_nb[side, way, part].astype(F32) + wo_far[side, part].astype(F32)
            ).astype(BF)
            near_hop(side, way, True).start()

    sends = (
        (gathers[0], 0, sq, rq, oq, y, at_y, 0),
        (gathers[1], 1, sk, rk, ok, x, at_x, 1),
        (gathers[2], 0, sv.at[:, :, lo], rv.at[:, :, lo], ov.at[:, lo], y, at_y, 2),
        (gathers[3], 1, sv.at[:, :, hi], rv.at[:, :, hi], ov.at[:, hi], x, at_x, 3),
    )
    ends = (pl.ds(0, strip // 2), pl.ds(strip // 2, strip // 2))

    def weight_far(item, way):
        gather, side, s, r, o, pos, at, i = item
        n = nx
        return remote(
            s.at[0, ends[way]],
            r.at[0, ends[way]],
            rf_s.at[i, way],
            rf_r.at[i, way],
            at(lax.rem(pos + (1 if way == 0 else n - 1), n)),
        )

    def weight_near(item, way, added):
        gather, side, s, r, o, pos, at, i = item
        n = nx
        part = ends[way if added else 1 - way]
        return remote(
            s.at[1 + way, part],
            r.at[1 + way, part],
            rs_s.at[i, way, 1 if added else 0],
            rs_r.at[i, way, 1 if added else 0],
            at(lax.rem(pos + (1 if way == 0 else n - 1), n)),
        )

    for item in sends:
        gather, side, s, r, o, pos, at, i = item
        for step in range(2):
            relay_recv(gather, step).wait_recv()
        buf = gather[1]
        n = buf.shape[0]
        base = pl.ds(side * gathered, gathered)

        def weight_piece(k, carry):
            there = lax.rem(pos + 6 - k, n)
            part = dot_tn(
                w3[base, strip_at(there)], buf[...].reshape(gathered, buf.shape[2])
            )

            @pl.when(k == 0)
            def _():
                s[0] = part.astype(BF)
                weight_far(item, 0).start()
                weight_far(item, 1).start()

            @pl.when(k == 1)
            def _():
                s[1] = part.astype(BF)
                weight_near(item, 0, False).start()

            @pl.when(k == 2)
            def _():
                o[...] = part

            @pl.when(k == 3)
            def _():
                s[2] = part.astype(BF)
                weight_near(item, 1, False).start()

            return carry

        lax.fori_loop(0, n, weight_piece, 0)

    for item in sends:
        gather, side, s, r, o, pos, at, i = item
        for way in range(2):
            weight_far(item, way).wait_recv()
            part = ends[way]
            s[1 + way, part] = (
                s[1 + way, part].astype(F32) + r[0, part].astype(F32)
            ).astype(BF)
            weight_near(item, way, True).start()

    out_o[...] = (rest[...].astype(F32) + from_heads(o_p, o_z, o_a, oz_s, oz_r)).astype(BF)
    gt_o[...] = (rest_g[...].astype(F32) + from_heads(d_p, d_z, d_a, dz_s, dz_r)).astype(BF)

    def second_hop(side, there, slot, owner):
        pos, n, at = ((y, ny, at_y), (x, nx, at_x))[side]
        return remote(
            wo_t.at[side, there],
            wo_u.at[side, owner],
            w2_s.at[side, slot],
            w2_r.at[side, owner],
            at(there),
        )

    for side in range(2):
        pos, m = ((y, ny), (x, nx))[side]
        for way in range(2):
            far_hop(side, way).wait_send()
            for added in (False, True):
                copy = near_hop(side, way, added)
                copy.wait_send()
                copy.wait_recv()

        def add_up(j, carry):
            there = lax.rem(pos + j, m)
            total = wo_own[side, there].astype(F32)
            for way in range(2):
                total = total + wo_r[side, way, there].astype(F32)

            @pl.when(j < m)
            def _():
                wo_t[side, there] = total.astype(BF)
                second_hop(side, there, j - 1, pos).start()

            @pl.when(j == m)
            def _():
                wo_a[pl.ds(side * half, half), :] = total

            return carry

        lax.fori_loop(1, m + 1, add_up, 0)

    for item, target in zip(sends, (gq_o, gk_o, gv_o.at[:, lo], gv_o.at[:, hi])):
        gather, side, s, r, o, pos, at, i = item
        for way in range(2):
            weight_far(item, way).wait_send()
            for added in (False, True):
                copy = weight_near(item, way, added)
                copy.wait_send()
                copy.wait_recv()
        target[...] = o[...] + r[1].astype(F32) + r[2].astype(F32)
        for step in range(2):
            near_send(gather, step).wait_send()
            relay(gather, step).wait_send()

    for side in range(2):
        pos, m = ((y, ny), (x, nx))[side]
        total = wo_a[pl.ds(side * half, half), :]
        for j in range(1, m):
            there = lax.rem(pos + j, m)
            copy = second_hop(side, there, j - 1, there)
            copy.wait_send()
            copy.wait_recv()
            total = total + wo_u[side, there].astype(F32)
        gwo_o[pl.ds(side * half, half), :] = total


def gradients(nctx, ntp, nx, core_out, tokens, w_query, w_key, w_value, w_out, grad_out):
    attn, d_query, d_key, d_value, wos, tx, ty = core_out
    rows, width = tokens.shape
    cols = w_query.shape[1]
    ny = nctx // nx
    nz = ntp // 2
    strip = width // nctx
    half = cols // 2
    hbm = pl.BlockSpec(memory_space=pl.ANY)
    vmem = pl.BlockSpec(memory_space=pltpu.VMEM)
    dma = pltpu.SemaphoreType.DMA
    small = jax.ShapeDtypeStruct((rows, cols), BF)
    piece = jax.ShapeDtypeStruct((strip, cols), F32)
    heads_scratch = [
        pltpu.VMEM((nz, rows, cols), BF),
        pltpu.VMEM((nz, rows, cols), BF),
        pltpu.VMEM((nz, rows, cols), BF),
        pltpu.VMEM((rows, cols), F32),
    ]
    return pl.pallas_call(
        functools.partial(grad_kernel, nctx, ntp, nx),
        out_shape=(
            small,
            small,
            piece,
            piece,
            piece,
            jax.ShapeDtypeStruct((cols, strip), F32),
        ),
        in_specs=[hbm] * 13,
        out_specs=(vmem,) * 6,
        scratch_shapes=[
            pltpu.VMEM((width, 3 * cols), BF),
            pltpu.VMEM((cols, width), BF),
            pltpu.VMEM((rows, 3 * cols), BF),
            pltpu.VMEM((rows, cols), BF),
            pltpu.VMEM((rows, cols), BF),
            pltpu.VMEM((rows, cols), BF),
            pltpu.VMEM((nx, rows, cols), BF),
            pltpu.VMEM((ny, rows, cols), BF),
            pltpu.VMEM((nx, rows, half), BF),
            pltpu.VMEM((ny, rows, half), BF),
            *heads_scratch,
            *heads_scratch,
            pltpu.VMEM((3, strip, cols), BF),
            pltpu.VMEM((3, strip, cols), BF),
            pltpu.VMEM((3, strip, cols), BF),
            pltpu.VMEM((3, strip, cols), BF),
            pltpu.VMEM((3, strip, cols), BF),
            pltpu.VMEM((3, strip, cols), BF),
            pltpu.VMEM((strip, cols), F32),
            pltpu.VMEM((strip, cols), F32),
            pltpu.VMEM((strip, cols), F32),
            pltpu.VMEM((2, ny, half, strip), BF),
            pltpu.VMEM((2, 2, ny, half, strip), BF),
            pltpu.VMEM((2, ny, half, strip), BF),
            pltpu.VMEM((2, 2, ny, half, strip), BF),
            pltpu.VMEM((2, ny, half, strip), BF),
            pltpu.VMEM((2, ny, half, strip), BF),
            pltpu.VMEM((cols, strip), F32),
            dma((20 + nx + ny,)),
            dma((4, 4)),
            dma((4, 4)),
            dma((nz,)),
            dma((nz,)),
            dma((nz - 1,)),
            dma((nz,)),
            dma((nz,)),
            dma((nz,)),
            dma((nz - 1,)),
            dma((nz,)),
            dma((4, 2)),
            dma((4, 2)),
            dma((4, 2, 2)),
            dma((4, 2, 2)),
            dma((2, 2)),
            dma((2, 2)),
            dma((2, 2, 2)),
            dma((2, 2, 2)),
            dma((2, nx - 1)),
            dma((2, nx)),
        ],
        compiler_params=pltpu.CompilerParams(
            collective_id=2, has_side_effects=True, vmem_limit_bytes=64 * 1024 * 1024 - 65536
        ),
        name="gradients",
    )(
        d_query,
        d_key,
        d_value,
        attn,
        wos,
        tx,
        ty,
        w_query,
        w_key,
        w_value,
        w_out,
        tokens,
        grad_out,
    )


def settle_kernel(count, *refs):
    ins, outs, bufs = refs[:count], refs[count : 2 * count], refs[2 * count : 3 * count]
    come, go = refs[3 * count :]
    first = [pltpu.make_async_copy(ins[i], bufs[i], come.at[i]) for i in range(count)]
    second = [pltpu.make_async_copy(bufs[i], outs[i], go.at[i]) for i in range(count)]
    for copy in first:
        copy.start()
    for i in range(count):
        first[i].wait()
        second[i].start()
    for copy in second:
        copy.wait()


def settled(arrays):
    count = len(arrays)
    hbm = pl.BlockSpec(memory_space=pl.ANY)
    shapes = [(a.shape, a.dtype) for a in arrays]
    return pl.pallas_call(
        functools.partial(settle_kernel, count),
        out_shape=tuple(jax.ShapeDtypeStruct(*s) for s in shapes),
        in_specs=[hbm] * count,
        out_specs=(hbm,) * count,
        scratch_shapes=[pltpu.VMEM(*s) for s in shapes]
        + [pltpu.SemaphoreType.DMA((count,)), pltpu.SemaphoreType.DMA((count,))],
        name="settled",
    )(*arrays)


def per_device(nctx, ntp, nx, tokens, w_query, w_key, w_value, w_out, block_doc, grad_out):
    core_out = attention_core(
        nctx, ntp, nx, tokens, w_query, w_key, w_value, w_out, block_doc, grad_out
    )
    return settled(
        gradients(nctx, ntp, nx, core_out, tokens, w_query, w_key, w_value, w_out, grad_out)
    )


def solution(mesh):
    in_specs = (
        P("ctx", None),
        P(None, "tp"),
        P(None, "tp"),
        P(None, "tp"),
        P("tp", None),
        P(),
        P("ctx", "tp"),
    )
    out_specs = (
        P("ctx", "tp"),
        P("ctx", "tp"),
        P("ctx", "tp"),
        P("ctx", "tp"),
        P("ctx", "tp"),
        P("tp", "ctx"),
    )
    return jax.shard_map(
        functools.partial(per_device, mesh.shape["ctx"], mesh.shape["tp"], math.isqrt(mesh.shape["ctx"])),
        mesh=mesh,
        in_specs=in_specs,
        out_specs=out_specs,
        check_vma=False,
    )
```

```python
import functools
import math

import jax
import jax.numpy as jnp
from jax import lax
from jax.experimental import pallas as pl
from jax.experimental.pallas import tpu as pltpu
from jax.sharding import PartitionSpec as P

HDIM = 128
BLOCK = 64
PAIR = 2 * BLOCK
MESH = pl.DeviceIdType.MESH
BF = jnp.bfloat16
F32 = jnp.float32
big_negative = -1e30


def dot_nn(a, b):
    return lax.dot_general(a, b, (((1,), (0,)), ((), ())), preferred_element_type=F32)


def dot_nt(a, b):
    return lax.dot_general(a, b, (((1,), (1,)), ((), ())), preferred_element_type=F32)


def dot_tn(a, b):
    return lax.dot_general(a, b, (((0,), (0,)), ((), ())), preferred_element_type=F32)


def iota(shape, dim):
    return lax.broadcasted_iota(jnp.int32, shape, dim)


def one_hot(hit):
    return jnp.where(hit, 1.0, 0.0).astype(BF)


def remote(source, target, send, recv, where):
    return pltpu.make_async_remote_copy(
        src_ref=source,
        dst_ref=target,
        send_sem=send,
        recv_sem=recv,
        device_id=where,
        device_id_type=MESH,
    )


def summed_over_heads(ntp, chunk, p, q, zb, acc, p_s, p_r, z_s, z_r):
    tp = lax.axis_index("tp")
    nz = ntp // 2
    core = lax.rem(tp, 2)
    z = lax.div(tp, 2)
    partner = {"tp": tp + 1 - 2 * core}

    def first(i, carry):
        p[i] = chunk(i * 2 + 1 - core).astype(BF)
        remote(p.at[i], q.at[i], p_s.at[i], p_r.at[i], partner).start()
        return carry

    lax.fori_loop(0, nz, first, 0)

    def second(j, carry):
        i = lax.rem(z + j, nz)
        part = chunk(i * 2 + core)
        copy = remote(p.at[i], q.at[i], p_s.at[i], p_r.at[i], partner)
        copy.wait_send()
        copy.wait_recv()
        part = part + q[i].astype(F32)

        @pl.when(j < nz)
        def _():
            p[i] = part.astype(BF)
            remote(
                p.at[i], zb.at[z], z_s.at[j - 1], z_r.at[z], {"tp": i * 2 + core}
            ).start()

        @pl.when(j == nz)
        def _():
            acc[...] = part

        return carry

    lax.fori_loop(1, nz + 1, second, 0)


def from_heads(ntp, p, zb, acc, z_s, z_r):
    tp = lax.axis_index("tp")
    nz = ntp // 2
    core = lax.rem(tp, 2)
    z = lax.div(tp, 2)
    total = acc[...]
    for j in range(1, nz):
        i = lax.rem(z + j, nz)
        copy = remote(p.at[i], zb.at[i], z_s.at[j - 1], z_r.at[i], {"tp": i * 2 + core})
        copy.wait_send()
        copy.wait_recv()
        total = total + zb[i].astype(F32)
    return total


def core_kernel(
    nctx,
    ntp,
    nx,
    tok_h,
    wq_h,
    wk_h,
    wv_h,
    wo_h,
    doc_ref,
    go_h,
    out_o,
    dq_o,
    dk_o,
    dv_o,
    wos_o,
    wfar_o,
    wr_o,
    tx_o,
    ty_o,
    tok,
    w3,
    wo,
    qkv,
    gfull,
    land,
    lk,
    lv,
    pw,
    attn,
    da,
    dqv,
    dkv,
    dvv,
    dkf,
    dvf,
    dlk,
    dlv,
    dls,
    dlr,
    wos,
    acc,
    o_p,
    o_q,
    o_z,
    o_a,
    outv,
    ld,
    st,
    g_s,
    g_r,
    f_s,
    l_s,
    l_r,
    d_s,
    d_r,
    tx_s,
    tx_r,
    ty_s,
    ty_r,
    t_l,
    fx_s,
    fx_r,
    fy_s,
    fy_r,
    h_s,
    h_r,
    op_s,
    op_r,
    oz_s,
    oz_r,
    w0_s,
    w0_r,
    w1_s,
    w1_r,
):
    ctx = lax.axis_index("ctx")
    ny = nctx // nx
    y = lax.div(ctx, nx)
    x = lax.rem(ctx, nx)
    tp = lax.axis_index("tp")
    nz = ntp // 2
    core = lax.rem(tp, 2)
    z = lax.div(tp, 2)
    partner = tp + 1 - 2 * core
    rows, width = tok.shape
    cols = qkv.shape[2]
    heads = cols // HDIM
    own_blocks = rows // BLOCK
    all_blocks = nctx * own_blocks
    per = 2 * own_blocks
    scale = 1.0 / math.sqrt(HDIM)

    def shard(t):
        return pl.ds(pl.multiple_of(t * cols, cols), cols)

    def mate(j, side):
        return lax.rem(z + j, nz) * 2 + side

    load_tok = pltpu.make_async_copy(tok_h, tok, ld.at[0])
    load_tok.start()
    for i, w_h in enumerate((wk_h, wv_h, wq_h)):
        pltpu.make_async_copy(w_h, w3.at[i], ld.at[1 + i]).start()
    load_wo = pltpu.make_async_copy(wo_h, wo, ld.at[4])
    load_wo.start()
    load_go = pltpu.make_async_copy(go_h, gfull.at[:, shard(tp)], ld.at[5])
    load_go.start()

    barrier = pltpu.get_barrier_semaphore()

    def greet(i, carry):
        pl.semaphore_signal(
            barrier, inc=1, device_id={"ctx": lax.rem(ctx + i, nctx)}, device_id_type=MESH
        )
        return carry

    lax.fori_loop(1, nctx, greet, 0)
    pl.semaphore_signal(barrier, inc=1, device_id={"tp": partner}, device_id_type=MESH)
    for j in range(1, nz):
        pl.semaphore_signal(barrier, inc=1, device_id={"tp": mate(j, core)}, device_id_type=MESH)
    pl.semaphore_wait(barrier, nctx - 1 + nz)

    def grad_copy(source, owner, send, target):
        return pltpu.make_async_remote_copy(
            src_ref=source,
            dst_ref=gfull.at[:, shard(owner)],
            send_sem=send,
            recv_sem=g_r.at[owner],
            device_id={"tp": target},
            device_id_type=MESH,
        )

    first_sends = [
        grad_copy(go_h, tp, g_s.at[0], mate(1, core)),
        grad_copy(go_h, tp, g_s.at[1], mate(nz - 1, core)),
        grad_copy(go_h, tp, g_s.at[2], partner),
    ]
    for send in first_sends:
        send.start()

    strip = width // nctx
    own_half = pl.ds(pl.multiple_of(core * (rows // 2), rows // 2), rows // 2)

    def strip_at(i):
        return pl.ds(pl.multiple_of(i * strip, strip), strip)

    def x_copy(j, i, owner):
        return pltpu.make_async_remote_copy(
            src_ref=tok_h.at[own_half, strip_at(i * nx + lax.rem(x + j, nx))],
            dst_ref=tx_o.at[owner, own_half, strip_at(i)],
            send_sem=tx_s.at[j - 1, i],
            recv_sem=tx_r.at[owner, i],
            device_id={"ctx": y * nx + lax.rem(x + j, nx)},
            device_id_type=MESH,
        )

    def y_copy(j, owner):
        there = lax.rem(y + j, ny)
        return pltpu.make_async_remote_copy(
            src_ref=tok_h.at[own_half, pl.ds(pl.multiple_of(there * nx * strip, strip), nx * strip)],
            dst_ref=ty_o.at[owner, own_half],
            send_sem=ty_s.at[j - 1],
            recv_sem=ty_r.at[owner],
            device_id={"ctx": there * nx + x},
            device_id_type=MESH,
        )

    def pass_on(ref, owner, send, recv):
        return pltpu.make_async_remote_copy(
            src_ref=ref.at[owner, own_half],
            dst_ref=ref.at[owner, own_half],
            send_sem=send,
            recv_sem=recv,
            device_id={"tp": partner},
            device_id_type=MESH,
        )

    def send_tokens(j):
        for i in range(ny):
            x_copy(j, i, x).start()
        y_copy(j, y).start()

    send_tokens(1)
    send_tokens(3)
    load_tok.wait()

    half = cols // 2

    def project(i, carry):
        pltpu.make_async_copy(wk_h, w3.at[i], ld.at[1 + i]).wait()

        def piece(n, inner):
            at = pl.ds(pl.multiple_of(n * half, half), half)
            qkv[i, :, at] = dot_nn(tok[...], w3[i, :, at]).astype(BF)
            return inner

        lax.fori_loop(0, 2, piece, 0)

        @pl.when(i == 1)
        def _():
            r = iota((per, rows), 0)
            c = iota((per, rows), 1)
            pick_k = one_hot(c == r * BLOCK + BLOCK - 1)
            pick_v = one_hot(c == (r - own_blocks) * BLOCK + BLOCK - 1)
            pick_k = jnp.where(r < own_blocks, pick_k, jnp.zeros_like(pick_k))
            pick_v = jnp.where(r >= own_blocks, pick_v, jnp.zeros_like(pick_v))
            land[ctx] = (dot_nn(pick_k, qkv[0]) + dot_nn(pick_v, qkv[1])).astype(BF)

            def spread(j, inner):
                pltpu.make_async_remote_copy(
                    src_ref=land.at[ctx],
                    dst_ref=land.at[ctx],
                    send_sem=l_s.at[j - 1],
                    recv_sem=l_r.at[ctx],
                    device_id={"ctx": lax.rem(ctx + j, nctx)},
                    device_id_type=MESH,
                ).start()
                return inner

            lax.fori_loop(1, nctx, spread, 0)

        return carry

    lax.fori_loop(0, 3, project, 0)
    send_tokens(2)

    def land_wait(j, carry):
        source = lax.rem(ctx + j, nctx)
        copy = pltpu.make_async_remote_copy(
            src_ref=land.at[ctx],
            dst_ref=land.at[source],
            send_sem=l_s.at[j - 1],
            recv_sem=l_r.at[source],
            device_id={"ctx": source},
            device_id_type=MESH,
        )
        copy.wait_send()
        copy.wait_recv()
        return carry

    def row_half(way):
        return pl.ds(way * (rows // 2), rows // 2)

    def relay(way):
        owner = mate(nz - 1 if way == 0 else 1, core)
        view = gfull.at[row_half(way), shard(owner)]
        return pltpu.make_async_remote_copy(
            src_ref=view,
            dst_ref=view,
            send_sem=h_s.at[way],
            recv_sem=h_r.at[way],
            device_id={"tp": mate(1 if way == 0 else nz - 1, core)},
            device_id_type=MESH,
        )

    def relay_wait(way):
        view = gfull.at[row_half(way), shard(mate(2, core))]
        pltpu.make_async_remote_copy(
            src_ref=view,
            dst_ref=view,
            send_sem=h_s.at[way],
            recv_sem=h_r.at[way],
            device_id={"tp": mate(nz - 1 if way == 0 else 1, core)},
            device_id_type=MESH,
        ).wait_recv()

    lax.fori_loop(1, nctx, land_wait, 0)

    forwards = []

    def pass_shard(owner, slot):
        onward = grad_copy(gfull.at[:, shard(owner)], owner, f_s.at[slot], partner)
        onward.start()
        forwards.append(onward)

    for way in range(2):
        owner = mate(nz - 1 if way == 0 else 1, core)
        grad_copy(gfull.at[:, shard(owner)], owner, f_s.at[way], partner).wait_recv()
        relay(way).start()
        pass_shard(owner, way)

    own_strips = [
        pltpu.make_async_copy(
            tok.at[:, strip_at(i * nx + x)], tx_o.at[x, :, strip_at(i)], t_l.at[i]
        )
        for i in range(ny)
    ]
    own_strips.append(
        pltpu.make_async_copy(
            tok.at[:, pl.ds(pl.multiple_of(y * nx * strip, strip), nx * strip)],
            ty_o.at[y],
            t_l.at[ny],
        )
    )
    for copy in own_strips:
        copy.start()

    b = iota((all_blocks, nctx * per), 0)
    c = iota((all_blocks, nctx * per), 1)
    shift = b // own_blocks * own_blocks
    landed = land[...].reshape(nctx * per, cols)
    lk[...] = dot_nn(one_hot(c == b + shift), landed).astype(BF)
    lv[...] = dot_nn(one_hot(c == b + shift + own_blocks), landed).astype(BF)

    span = PAIR + all_blocks
    doc = doc_ref[...]
    doc_lane = iota(doc.shape, 1)
    doc_wide = jnp.concatenate([jnp.zeros((1, PAIR), jnp.int32), doc], axis=1)

    def forward(sb, carry):
        at = pl.ds(pl.multiple_of(sb * PAIR, PAIR), PAIR)
        row = iota((PAIR, span), 0)
        col = iota((PAIR, span), 1)
        upper = jnp.where(row >= BLOCK, 1, 0)
        col_upper = jnp.where(col >= BLOCK, 1, 0)
        first = ctx * own_blocks + sb * 2
        doc_a = jnp.sum(jnp.where(doc_lane == first, doc, 0), axis=1, keepdims=True)
        doc_b = jnp.sum(jnp.where(doc_lane == first + 1, doc, 0), axis=1, keepdims=True)
        own_doc = jnp.where(row >= BLOCK, doc_b, doc_a)
        near = (col < PAIR) & (upper == col_upper) & (col <= row)
        far = (col >= PAIR) & (col - PAIR < first + upper) & (doc_wide == own_doc)
        mask = near | far
        for h in range(heads):
            hs = pl.ds(h * HDIM, HDIM)
            keys = jnp.concatenate([qkv[0, at, hs], lk[:, hs]], axis=0)
            values = jnp.concatenate([qkv[1, at, hs], lv[:, hs]], axis=0)
            scores = dot_nt(qkv[2, at, hs], keys) * scale
            scores = jnp.where(mask, scores, big_negative)
            top = jnp.max(scores, axis=1, keepdims=True)
            e = jnp.exp(scores - top)
            weight = (e / jnp.sum(e, axis=1, keepdims=True)).astype(BF)
            pw[sb * heads + h] = weight
            attn[at, hs] = dot_nn(weight, values).astype(BF)
        return carry

    lax.fori_loop(0, rows // PAIR, forward, 0)
    load_wo.wait()

    def out_chunk(t):
        return dot_nn(attn[...], wo[:, shard(t)])

    summed_over_heads(ntp, out_chunk, o_p, o_q, o_z, o_a, op_s, op_r, oz_s, oz_r)
    load_go.wait()
    acc[...] = jnp.zeros_like(acc)

    def use_shard(t):
        grads = gfull[:, shard(t)]
        acc[...] += dot_nt(grads, wo[:, shard(t)])
        part = dot_tn(attn[...], grads).astype(BF)
        for k in range(nctx // ntp):
            i = t * (nctx // ntp) + k
            there_y = lax.div(i, nx)
            there_x = lax.rem(i, nx)
            wos[0, there_x, there_y] = part[: cols // 2, k * strip : (k + 1) * strip]
            wos[1, there_y, there_x] = part[cols // 2 :, k * strip : (k + 1) * strip]

    def use_near(i, carry):
        side = jnp.where(lax.rem(i, 2) == 0, core, 1 - core)
        hop = jnp.where(i < 2, 0, jnp.where(i < 4, 1, nz - 1))
        t = mate(hop, side)

        @pl.when((i == 1) | (i == 3) | (i == 5))
        def _():
            grad_copy(gfull.at[:, shard(t)], t, f_s.at[0], partner).wait_recv()

        use_shard(t)
        return carry

    lax.fori_loop(0, 6, use_near, 0)
    for way in range(2):
        relay_wait(way)
    pass_shard(mate(2, core), 2)

    def use_far(i, carry):
        t = mate(2, jnp.where(i == 0, core, 1 - core))

        @pl.when(i == 1)
        def _():
            grad_copy(gfull.at[:, shard(t)], t, f_s.at[2], partner).wait_recv()

        use_shard(t)
        return carry

    lax.fori_loop(0, 2, use_far, 0)
    da[...] = acc[...].astype(BF)
    out_wos = pltpu.make_async_copy(wos, wos_o, st.at[4])
    out_wos.start()
    rings = ((x, nx, lambda i: {"ctx": y * nx + i}), (y, ny, lambda i: {"ctx": i * nx + x}))
    subs = (pl.ds(0, nx // 2), pl.ds(nx // 2, nx // 2))

    def far_hop(side, way):
        pos, n, at = rings[side]
        return remote(
            wos.at[side, lax.rem(pos + 2, n), subs[way]],
            wfar_o.at[side, subs[way]],
            w0_s.at[side, way],
            w0_r.at[side, way],
            at(lax.rem(pos + (1 if way == 0 else n - 1), n)),
        )

    def near_hop(side, way):
        pos, n, at = rings[side]
        there = lax.rem(pos + (1 if way == 0 else n - 1), n)
        return remote(
            wos.at[side, there, subs[1 - way]],
            wr_o.at[side, way, subs[1 - way]],
            w1_s.at[side, way],
            w1_r.at[side, way],
            at(there),
        )

    for way in range(2):
        for side in range(2):
            far_hop(side, way).start()

    dlk[...] = jnp.zeros_like(dlk)
    dlv[...] = jnp.zeros_like(dlv)

    def backward(sb, carry):
        at = pl.ds(pl.multiple_of(sb * PAIR, PAIR), PAIR)
        for h in range(heads):
            hs = pl.ds(h * HDIM, HDIM)
            keys = jnp.concatenate([qkv[0, at, hs], lk[:, hs]], axis=0)
            values = jnp.concatenate([qkv[1, at, hs], lv[:, hs]], axis=0)
            weight = pw[sb * heads + h]
            d_out = da[at, hs]
            delta = jnp.sum(
                attn[at, hs].astype(F32) * d_out.astype(F32), axis=1, keepdims=True
            )
            d_weight = dot_nt(d_out, values)
            ds = (weight.astype(F32) * (d_weight - delta)).astype(BF)
            dqv[at, hs] = (dot_nn(ds, keys) * scale).astype(BF)
            d_keys = dot_tn(ds, qkv[2, at, hs]) * scale
            d_values = dot_tn(weight, d_out)
            dkf[at, hs] = d_keys[:PAIR]
            dvf[at, hs] = d_values[:PAIR]
            dlk[:, hs] += d_keys[PAIR:]
            dlv[:, hs] += d_values[PAIR:]
        return carry

    lax.fori_loop(0, rows // PAIR, backward, 0)
    out_dq = pltpu.make_async_copy(dqv, dq_o, st.at[1])
    out_dq.start()

    r = iota((nctx * per, all_blocks), 0)
    b = iota((nctx * per, all_blocks), 1)
    shift = b // own_blocks * own_blocks
    packed = dot_nn(one_hot(r == b + shift), dlk[...].astype(BF)) + dot_nn(
        one_hot(r == b + shift + own_blocks), dlv[...].astype(BF)
    )
    dls[...] = packed.astype(BF).reshape(nctx, per, cols)

    def give(j, carry):
        target = lax.rem(ctx + j, nctx)
        pltpu.make_async_remote_copy(
            src_ref=dls.at[target],
            dst_ref=dlr.at[ctx],
            send_sem=d_s.at[j - 1],
            recv_sem=d_r.at[ctx],
            device_id={"ctx": target},
            device_id_type=MESH,
        ).start()
        return carry

    lax.fori_loop(1, nctx, give, 0)
    for way in range(2):
        for side in range(2):
            near_hop(side, way).start()
    dlr[ctx] = dls[ctx]

    for j in range(1, nx):
        owner = lax.rem(x + j, nx)
        for i in range(ny):
            x_copy(j, i, owner).wait_recv()
        pass_on(tx_o, owner, fx_s.at[j - 1], fx_r.at[j - 1]).start()
    for j in range(1, ny):
        owner = lax.rem(y + j, ny)
        y_copy(j, owner).wait_recv()
        pass_on(ty_o, owner, fy_s.at[j - 1], fy_r.at[j - 1]).start()

    def take(j, carry):
        source = lax.rem(ctx + j, nctx)
        copy = pltpu.make_async_remote_copy(
            src_ref=dls.at[source],
            dst_ref=dlr.at[source],
            send_sem=d_s.at[j - 1],
            recv_sem=d_r.at[source],
            device_id={"ctx": source},
            device_id_type=MESH,
        )
        copy.wait_send()
        copy.wait_recv()
        return carry

    lax.fori_loop(1, nctx, take, 0)
    total = jnp.zeros((per, cols), F32)
    for i in range(nctx):
        total = total + dlr[i].astype(F32)
    for i in range(own_blocks):
        last = pl.ds(i * BLOCK + BLOCK - 1, 1)
        dkf[last, :] += total[i : i + 1]
        dvf[last, :] += total[own_blocks + i : own_blocks + i + 1]
    dkv[...] = dkf[...].astype(BF)
    dvv[...] = dvf[...].astype(BF)
    out_dk = pltpu.make_async_copy(dkv, dk_o, st.at[2])
    out_dk.start()
    out_dv = pltpu.make_async_copy(dvv, dv_o, st.at[3])
    out_dv.start()
    outv[...] = (
        tok[:, shard(tp)].astype(F32) + from_heads(ntp, o_p, o_z, o_a, oz_s, oz_r)
    ).astype(BF)
    out_out = pltpu.make_async_copy(outv, out_o, st.at[5])
    out_out.start()
    for way in range(2):
        for side in range(2):
            for copy in (far_hop(side, way), near_hop(side, way)):
                copy.wait_send()
                copy.wait_recv()
    for send in first_sends + forwards + [relay(0), relay(1)]:
        send.wait_send()
    for copy in [out_out, out_dq, out_dk, out_dv, out_wos] + own_strips:
        copy.wait()
    for j in range(1, nx):
        for i in range(ny):
            x_copy(j, i, x).wait_send()
        passed = pass_on(tx_o, lax.rem(x + j, nx), fx_s.at[j - 1], fx_r.at[j - 1])
        passed.wait_send()
        other_half = pl.ds(pl.multiple_of((1 - core) * (rows // 2), rows // 2), rows // 2)
        pltpu.make_async_remote_copy(
            src_ref=tx_o.at[lax.rem(x + j, nx), other_half],
            dst_ref=tx_o.at[lax.rem(x + j, nx), other_half],
            send_sem=fx_s.at[j - 1],
            recv_sem=fx_r.at[j - 1],
            device_id={"tp": partner},
            device_id_type=MESH,
        ).wait_recv()
    for j in range(1, ny):
        y_copy(j, y).wait_send()
        passed = pass_on(ty_o, lax.rem(y + j, ny), fy_s.at[j - 1], fy_r.at[j - 1])
        passed.wait_send()
        other_half = pl.ds(pl.multiple_of((1 - core) * (rows // 2), rows // 2), rows // 2)
        pltpu.make_async_remote_copy(
            src_ref=ty_o.at[lax.rem(y + j, ny), other_half],
            dst_ref=ty_o.at[lax.rem(y + j, ny), other_half],
            send_sem=fy_s.at[j - 1],
            recv_sem=fy_r.at[j - 1],
            device_id={"tp": partner},
            device_id_type=MESH,
        ).wait_recv()


def attention_core(nctx, ntp, nx, tokens, w_query, w_key, w_value, w_out, block_doc, grad_out):
    rows, width = tokens.shape
    cols = w_query.shape[1]
    heads = cols // HDIM
    own_blocks = rows // BLOCK
    all_blocks = nctx * own_blocks
    per = 2 * own_blocks
    units = rows // PAIR * heads
    ny = nctx // nx
    small = jax.ShapeDtypeStruct((rows, cols), BF)
    hbm = pl.BlockSpec(memory_space=pl.ANY)
    dma = pltpu.SemaphoreType.DMA
    return pl.pallas_call(
        functools.partial(core_kernel, nctx, ntp, nx),
        out_shape=(
            small,
            small,
            small,
            small,
            jax.ShapeDtypeStruct((2, nx, ny, cols // 2, width // nctx), BF),
            jax.ShapeDtypeStruct((2, ny, cols // 2, width // nctx), BF),
            jax.ShapeDtypeStruct((2, 2, ny, cols // 2, width // nctx), BF),
            jax.ShapeDtypeStruct((nx, rows, width // nx), BF),
            jax.ShapeDtypeStruct((ny, rows, width // ny), BF),
        ),
        in_specs=[hbm] * 5 + [pl.BlockSpec(memory_space=pltpu.VMEM), hbm],
        out_specs=(hbm,) * 9,
        scratch_shapes=[
            pltpu.VMEM((rows, width), BF),
            pltpu.VMEM((3, width, cols), BF),
            pltpu.VMEM((cols, width), BF),
            pltpu.VMEM((3, rows, cols), BF),
            pltpu.VMEM((rows, width), BF),
            pltpu.VMEM((nctx, per, cols), BF),
            pltpu.VMEM((all_blocks, cols), BF),
            pltpu.VMEM((all_blocks, cols), BF),
            pltpu.VMEM((units, PAIR, PAIR + all_blocks), BF),
            pltpu.VMEM((rows, cols), BF),
            pltpu.VMEM((rows, cols), BF),
            pltpu.VMEM((rows, cols), BF),
            pltpu.VMEM((rows, cols), BF),
            pltpu.VMEM((rows, cols), BF),
            pltpu.VMEM((rows, cols), F32),
            pltpu.VMEM((rows, cols), F32),
            pltpu.VMEM((all_blocks, cols), F32),
            pltpu.VMEM((all_blocks, cols), F32),
            pltpu.VMEM((nctx, per, cols), BF),
            pltpu.VMEM((nctx, per, cols), BF),
            pltpu.VMEM((2, nx, ny, cols // 2, width // nctx), BF),
            pltpu.VMEM((rows, cols), F32),
            pltpu.VMEM((ntp // 2, rows, cols), BF),
            pltpu.VMEM((ntp // 2, rows, cols), BF),
            pltpu.VMEM((ntp // 2, rows, cols), BF),
            pltpu.VMEM((rows, cols), F32),
            pltpu.VMEM((rows, cols), BF),
            dma((6,)),
            dma((6,)),
            dma((ntp // 2,)),
            dma((ntp,)),
            dma((ntp // 2,)),
            dma((nctx - 1,)),
            dma((nctx,)),
            dma((nctx - 1,)),
            dma((nctx,)),
            dma((nx - 1, ny)),
            dma((nx, ny)),
            dma((ny - 1,)),
            dma((ny,)),
            dma((ny + 1,)),
            dma((nx - 1,)),
            dma((nx - 1,)),
            dma((ny - 1,)),
            dma((ny - 1,)),
            dma((2,)),
            dma((2,)),
            dma((ntp // 2,)),
            dma((ntp // 2,)),
            dma((ntp // 2 - 1,)),
            dma((ntp // 2,)),
            dma((2, 2)),
            dma((2, 2)),
            dma((2, 2)),
            dma((2, 2)),
        ],
        compiler_params=pltpu.CompilerParams(
            collective_id=1, has_side_effects=True, vmem_limit_bytes=64 * 1024 * 1024 - 65536
        ),
        name="attention_core",
    )(tokens, w_query, w_key, w_value, w_out, block_doc.reshape(1, -1), grad_out)


def grad_kernel(
    nctx,
    ntp,
    nx,
    dq_h,
    dk_h,
    dv_h,
    wos_h,
    wfar_h,
    wr_h,
    tx_h,
    ty_h,
    wq_h,
    wk_h,
    wv_h,
    go_h,
    gt_o,
    gq_o,
    gk_o,
    gv_o,
    gwo_o,
    w3,
    dcat,
    rest_g,
    gq,
    gk,
    gvx,
    gvy,
    d_p,
    d_q,
    d_z,
    d_a,
    sq,
    sk,
    sv,
    rq,
    rk,
    rv,
    oq,
    ok,
    ov,
    wo_own,
    wo_nb,
    wo_far,
    wo_r,
    wo_t,
    wo_u,
    wo_a,
    ld,
    dl,
    ag_s,
    ag_r,
    dp_s,
    dp_r,
    dz_s,
    dz_r,
    rf_s,
    rf_r,
    rs_s,
    rs_r,
    w1_s,
    w1_r,
    w2_s,
    w2_r,
):
    ctx = lax.axis_index("ctx")
    tp = lax.axis_index("tp")
    ny = nctx // nx
    nz = ntp // 2
    y = lax.div(ctx, nx)
    x = lax.rem(ctx, nx)
    core = lax.rem(tp, 2)
    z = lax.div(tp, 2)
    partner = tp + 1 - 2 * core
    rows, cols = rest_g.shape
    width = w3.shape[0]
    strip = width // nctx
    gathered = nx * rows
    half = cols // 2

    def block(t):
        return pl.ds(pl.multiple_of(t * cols, cols), cols)

    def strip_at(i):
        return pl.ds(pl.multiple_of(i * strip, strip), strip)

    def at_x(i):
        return {"ctx": y * nx + i}

    def at_y(i):
        return {"ctx": i * nx + x}

    loads = []
    for i, (d_h, w_h) in enumerate(((dq_h, wq_h), (dk_h, wk_h), (dv_h, wv_h))):
        lanes = pl.ds(i * cols, cols)
        loads.append(pltpu.make_async_copy(d_h, dcat.at[:, lanes], ld.at[2 + 2 * i]))
        loads.append(pltpu.make_async_copy(w_h, w3.at[:, lanes], ld.at[3 + 2 * i]))
    loads.append(pltpu.make_async_copy(go_h, rest_g, ld.at[9]))
    lo = pl.ds(0, half)
    hi = pl.ds(half, half)
    gathers = (
        (dq_h, gq, x, at_x, 0),
        (dk_h, gk, y, at_y, 1),
        (dv_h.at[:, lo], gvx, x, at_x, 2),
        (dv_h.at[:, hi], gvy, y, at_y, 3),
    )
    for source, buf, pos, at, i in gathers:
        loads.append(pltpu.make_async_copy(source, buf.at[pos], ld.at[10 + i]))
    rings = ((x, nx, at_x), (y, ny, at_y))
    for side in range(2):
        pos, n, at = rings[side]
        for k, target in ((0, wo_own), (1, wo_nb.at[:, 0]), (n - 1, wo_nb.at[:, 1])):
            loads.append(
                pltpu.make_async_copy(
                    wos_h.at[side, lax.rem(pos + k, n)],
                    target.at[side],
                    ld.at[14 + 3 * side + min(k, 2)],
                )
            )
    loads.append(pltpu.make_async_copy(wfar_h, wo_far, ld.at[0]))
    subs = (pl.ds(0, nx // 2), pl.ds(nx // 2, nx // 2))
    for side in range(2):
        for way in range(2):
            loads.append(
                pltpu.make_async_copy(
                    wr_h.at[side, way, subs[1 - way]],
                    wo_r.at[side, way, subs[1 - way]],
                    dl.at[side, way],
                )
            )
    for load in loads:
        load.start()

    barrier = pltpu.get_barrier_semaphore()
    for j in range(1, nx):
        pl.semaphore_signal(
            barrier, inc=1, device_id=at_x(lax.rem(x + j, nx)), device_id_type=MESH
        )
    for j in range(1, ny):
        pl.semaphore_signal(
            barrier, inc=1, device_id=at_y(lax.rem(y + j, ny)), device_id_type=MESH
        )
    for j in range(1, nz):
        pl.semaphore_signal(
            barrier,
            inc=1,
            device_id={"tp": lax.rem(z + j, nz) * 2 + core},
            device_id_type=MESH,
        )
    pl.semaphore_signal(barrier, inc=1, device_id={"tp": partner}, device_id_type=MESH)
    pl.semaphore_wait(barrier, nx + ny + nz - 2)

    def near_send(gather, step):
        source, buf, pos, at, i = gather
        n = buf.shape[0]
        there = lax.rem(pos + (1 if step == 0 else n - 1), n)
        return remote(source, buf.at[pos], ag_s.at[i, step], ag_r.at[i, step], at(there))

    def near_recv(gather, step):
        source, buf, pos, at, i = gather
        n = buf.shape[0]
        owner = lax.rem(pos + (n - 1 if step == 0 else 1), n)
        return remote(source, buf.at[owner], ag_s.at[i, step], ag_r.at[i, step], at(owner))

    def relay(gather, step):
        source, buf, pos, at, i = gather
        n = buf.shape[0]
        part = pl.ds(0, rows // 2) if step == 0 else pl.ds(rows // 2, rows // 2)
        owner = lax.rem(pos + (n - 1 if step == 0 else 1), n)
        there = lax.rem(pos + (1 if step == 0 else n - 1), n)
        return remote(
            buf.at[owner, part],
            buf.at[owner, part],
            ag_s.at[i, 2 + step],
            ag_r.at[i, 2 + step],
            at(there),
        )

    def relay_recv(gather, step):
        source, buf, pos, at, i = gather
        n = buf.shape[0]
        part = pl.ds(0, rows // 2) if step == 0 else pl.ds(rows // 2, rows // 2)
        owner = lax.rem(pos + 2, n)
        return remote(
            buf.at[owner, part],
            buf.at[owner, part],
            ag_s.at[i, 2 + step],
            ag_r.at[i, 2 + step],
            at(owner),
        )

    for gather in gathers:
        near_send(gather, 0).start()
        near_send(gather, 1).start()

    def near_hop(side, way):
        pos, n, at = rings[side]
        part = subs[way]
        return remote(
            wo_nb.at[side, way, part],
            wo_r.at[side, way, part],
            w1_s.at[side, way],
            w1_r.at[side, way],
            at(lax.rem(pos + (1 if way == 0 else n - 1), n)),
        )

    def tok_chunk(t):
        return dot_nt(dcat[...], w3[block(t), :])

    for load in loads[:6]:
        load.wait()
    summed_over_heads(ntp, tok_chunk, d_p, d_q, d_z, d_a, dp_s, dp_r, dz_s, dz_r)
    t_x = w3.at[pl.ds(0, gathered), pl.ds(0, width // nx)]
    t_y = w3.at[pl.ds(gathered, gathered), pl.ds(0, width // ny)]
    late = []
    for i in range(nx):
        part = pl.ds(i * rows, rows)
        late.append(pltpu.make_async_copy(tx_h.at[i], t_x.at[part], ld.at[20 + i]))
        late.append(pltpu.make_async_copy(ty_h.at[i], t_y.at[part], ld.at[20 + nx + i]))
    for load in late:
        load.start()

    for gather in gathers:
        for step in range(2):
            near_recv(gather, step).wait_recv()
            relay(gather, step).start()

    for load in loads[6:] + late:
        load.wait()
    for side in range(2):
        for way in range(2):
            part = subs[way]
            wo_nb[side, way, part] = (
                wo_nb[side, way, part].astype(F32) + wo_far[side, part].astype(F32)
            ).astype(BF)
            near_hop(side, way).start()

    sends = (
        (gathers[0], 0, sq, rq, oq, y, at_y, 0),
        (gathers[1], 1, sk, rk, ok, x, at_x, 1),
        (gathers[2], 0, sv.at[:, :, lo], rv.at[:, :, lo], ov.at[:, lo], y, at_y, 2),
        (gathers[3], 1, sv.at[:, :, hi], rv.at[:, :, hi], ov.at[:, hi], x, at_x, 3),
    )
    ends = (pl.ds(0, strip // 2), pl.ds(strip // 2, strip // 2))

    def weight_far(item, way):
        gather, side, s, r, o, pos, at, i = item
        n = nx
        return remote(
            s.at[0, ends[way]],
            r.at[0, ends[way]],
            rf_s.at[i, way],
            rf_r.at[i, way],
            at(lax.rem(pos + (1 if way == 0 else n - 1), n)),
        )

    def weight_near(item, way, added):
        gather, side, s, r, o, pos, at, i = item
        n = nx
        part = ends[way if added else 1 - way]
        return remote(
            s.at[1 + way, part],
            r.at[1 + way, part],
            rs_s.at[i, way, 1 if added else 0],
            rs_r.at[i, way, 1 if added else 0],
            at(lax.rem(pos + (1 if way == 0 else n - 1), n)),
        )

    for item in sends:
        gather, side, s, r, o, pos, at, i = item
        for step in range(2):
            relay_recv(gather, step).wait_recv()
        buf = gather[1]
        n = buf.shape[0]
        base = pl.ds(side * gathered, gathered)

        def weight_piece(k, carry):
            there = lax.rem(pos + 6 - k, n)
            part = dot_tn(
                w3[base, strip_at(there)], buf[...].reshape(gathered, buf.shape[2])
            )

            @pl.when(k == 0)
            def _():
                s[0] = part.astype(BF)
                weight_far(item, 0).start()
                weight_far(item, 1).start()

            @pl.when(k == 1)
            def _():
                s[1] = part.astype(BF)
                weight_near(item, 0, False).start()

            @pl.when(k == 2)
            def _():
                o[...] = part

            @pl.when(k == 3)
            def _():
                s[2] = part.astype(BF)
                weight_near(item, 1, False).start()

            return carry

        lax.fori_loop(0, n, weight_piece, 0)

    for item in sends:
        gather, side, s, r, o, pos, at, i = item
        for way in range(2):
            weight_far(item, way).wait_recv()
            part = ends[way]
            s[1 + way, part] = (
                s[1 + way, part].astype(F32) + r[0, part].astype(F32)
            ).astype(BF)
            weight_near(item, way, True).start()

    gt_o[...] = (rest_g[...].astype(F32) + from_heads(ntp, d_p, d_z, d_a, dz_s, dz_r)).astype(BF)

    def second_hop(side, there, slot, owner):
        pos, n, at = ((y, ny, at_y), (x, nx, at_x))[side]
        return remote(
            wo_t.at[side, there],
            wo_u.at[side, owner],
            w2_s.at[side, slot],
            w2_r.at[side, owner],
            at(there),
        )

    for side in range(2):
        pos, m = ((y, ny), (x, nx))[side]
        for way in range(2):
            copy = near_hop(side, way)
            copy.wait_send()
            copy.wait_recv()

        def add_up(j, carry):
            there = lax.rem(pos + j, m)
            total = wo_own[side, there].astype(F32)
            for way in range(2):
                total = total + wo_r[side, way, there].astype(F32)

            @pl.when(j < m)
            def _():
                wo_t[side, there] = total.astype(BF)
                second_hop(side, there, j - 1, pos).start()

            @pl.when(j == m)
            def _():
                wo_a[pl.ds(side * half, half), :] = total

            return carry

        lax.fori_loop(1, m + 1, add_up, 0)

    for item, target in zip(sends, (gq_o, gk_o, gv_o.at[:, lo], gv_o.at[:, hi])):
        gather, side, s, r, o, pos, at, i = item
        for way in range(2):
            weight_far(item, way).wait_send()
            for added in (False, True):
                copy = weight_near(item, way, added)
                copy.wait_send()
                copy.wait_recv()
        target[...] = o[...] + r[1].astype(F32) + r[2].astype(F32)
        for step in range(2):
            near_send(gather, step).wait_send()
            relay(gather, step).wait_send()

    for side in range(2):
        pos, m = ((y, ny), (x, nx))[side]
        total = wo_a[pl.ds(side * half, half), :]
        for j in range(1, m):
            there = lax.rem(pos + j, m)
            copy = second_hop(side, there, j - 1, there)
            copy.wait_send()
            copy.wait_recv()
            total = total + wo_u[side, there].astype(F32)
        gwo_o[pl.ds(side * half, half), :] = total


def gradients(nctx, ntp, nx, core_out, w_query, w_key, w_value, grad_out):
    d_query, d_key, d_value, wos, wfar, wr, tx, ty = core_out
    rows = grad_out.shape[0]
    width = w_query.shape[0]
    cols = w_query.shape[1]
    ny = nctx // nx
    nz = ntp // 2
    strip = width // nctx
    half = cols // 2
    hbm = pl.BlockSpec(memory_space=pl.ANY)
    vmem = pl.BlockSpec(memory_space=pltpu.VMEM)
    dma = pltpu.SemaphoreType.DMA
    small = jax.ShapeDtypeStruct((rows, cols), BF)
    piece = jax.ShapeDtypeStruct((strip, cols), F32)
    heads_scratch = [
        pltpu.VMEM((nz, rows, cols), BF),
        pltpu.VMEM((nz, rows, cols), BF),
        pltpu.VMEM((nz, rows, cols), BF),
        pltpu.VMEM((rows, cols), F32),
    ]
    return pl.pallas_call(
        functools.partial(grad_kernel, nctx, ntp, nx),
        out_shape=(
            small,
            piece,
            piece,
            piece,
            jax.ShapeDtypeStruct((cols, strip), F32),
        ),
        in_specs=[hbm] * 12,
        out_specs=(vmem,) * 5,
        scratch_shapes=[
            pltpu.VMEM((width, 3 * cols), BF),
            pltpu.VMEM((rows, 3 * cols), BF),
            pltpu.VMEM((rows, cols), BF),
            pltpu.VMEM((nx, rows, cols), BF),
            pltpu.VMEM((ny, rows, cols), BF),
            pltpu.VMEM((nx, rows, half), BF),
            pltpu.VMEM((ny, rows, half), BF),
            *heads_scratch,
            pltpu.VMEM((3, strip, cols), BF),
            pltpu.VMEM((3, strip, cols), BF),
            pltpu.VMEM((3, strip, cols), BF),
            pltpu.VMEM((3, strip, cols), BF),
            pltpu.VMEM((3, strip, cols), BF),
            pltpu.VMEM((3, strip, cols), BF),
            pltpu.VMEM((strip, cols), F32),
            pltpu.VMEM((strip, cols), F32),
            pltpu.VMEM((strip, cols), F32),
            pltpu.VMEM((2, ny, half, strip), BF),
            pltpu.VMEM((2, 2, ny, half, strip), BF),
            pltpu.VMEM((2, ny, half, strip), BF),
            pltpu.VMEM((2, 2, ny, half, strip), BF),
            pltpu.VMEM((2, ny, half, strip), BF),
            pltpu.VMEM((2, ny, half, strip), BF),
            pltpu.VMEM((cols, strip), F32),
            dma((20 + nx + ny,)),
            dma((2, 2)),
            dma((4, 4)),
            dma((4, 4)),
            dma((nz,)),
            dma((nz,)),
            dma((nz - 1,)),
            dma((nz,)),
            dma((4, 2)),
            dma((4, 2)),
            dma((4, 2, 2)),
            dma((4, 2, 2)),
            dma((2, 2)),
            dma((2, 2)),
            dma((2, nx - 1)),
            dma((2, nx)),
        ],
        compiler_params=pltpu.CompilerParams(
            collective_id=2, has_side_effects=True, vmem_limit_bytes=64 * 1024 * 1024 - 65536
        ),
        name="gradients",
    )(
        d_query,
        d_key,
        d_value,
        wos,
        wfar,
        wr,
        tx,
        ty,
        w_query,
        w_key,
        w_value,
        grad_out,
    )


def settle_kernel(count, *refs):
    ins, outs, bufs = refs[:count], refs[count : 2 * count], refs[2 * count : 3 * count]
    come, go = refs[3 * count :]
    first = [pltpu.make_async_copy(ins[i], bufs[i], come.at[i]) for i in range(count)]
    second = [pltpu.make_async_copy(bufs[i], outs[i], go.at[i]) for i in range(count)]
    for copy in first:
        copy.start()
    for i in range(count):
        first[i].wait()
        second[i].start()
    for copy in second:
        copy.wait()


def settled(arrays):
    count = len(arrays)
    hbm = pl.BlockSpec(memory_space=pl.ANY)
    shapes = [(a.shape, a.dtype) for a in arrays]
    return pl.pallas_call(
        functools.partial(settle_kernel, count),
        out_shape=tuple(jax.ShapeDtypeStruct(*s) for s in shapes),
        in_specs=[hbm] * count,
        out_specs=(hbm,) * count,
        scratch_shapes=[pltpu.VMEM(*s) for s in shapes]
        + [pltpu.SemaphoreType.DMA((count,)), pltpu.SemaphoreType.DMA((count,))],
        name="settled",
    )(*arrays)


def per_device(nctx, ntp, nx, tokens, w_query, w_key, w_value, w_out, block_doc, grad_out):
    out, *core_out = attention_core(
        nctx, ntp, nx, tokens, w_query, w_key, w_value, w_out, block_doc, grad_out
    )
    grads = gradients(nctx, ntp, nx, core_out, w_query, w_key, w_value, grad_out)
    return settled((out, *grads))


def solution(mesh):
    in_specs = (
        P("ctx", None),
        P(None, "tp"),
        P(None, "tp"),
        P(None, "tp"),
        P("tp", None),
        P(),
        P("ctx", "tp"),
    )
    out_specs = (
        P("ctx", "tp"),
        P("ctx", "tp"),
        P("ctx", "tp"),
        P("ctx", "tp"),
        P("ctx", "tp"),
        P("tp", "ctx"),
    )
    return jax.shard_map(
        functools.partial(per_device, mesh.shape["ctx"], mesh.shape["tp"], math.isqrt(mesh.shape["ctx"])),
        mesh=mesh,
        in_specs=in_specs,
        out_specs=out_specs,
        check_vma=False,
    )
```

```python
import functools
import math

import jax
import jax.numpy as jnp
from jax import lax
from jax.experimental import pallas as pl
from jax.experimental.pallas import tpu as pltpu
from jax.sharding import PartitionSpec as P

HDIM = 128
BLOCK = 64
PAIR = 2 * BLOCK
MESH = pl.DeviceIdType.MESH
BF = jnp.bfloat16
F32 = jnp.float32
big_negative = -1e30


def dot_nn(a, b):
    return lax.dot_general(a, b, (((1,), (0,)), ((), ())), preferred_element_type=F32)


def dot_nt(a, b):
    return lax.dot_general(a, b, (((1,), (1,)), ((), ())), preferred_element_type=F32)


def dot_tn(a, b):
    return lax.dot_general(a, b, (((0,), (0,)), ((), ())), preferred_element_type=F32)


def iota(shape, dim):
    return lax.broadcasted_iota(jnp.int32, shape, dim)


def one_hot(hit):
    return jnp.where(hit, 1.0, 0.0).astype(BF)


def remote(source, target, send, recv, where):
    return pltpu.make_async_remote_copy(
        src_ref=source,
        dst_ref=target,
        send_sem=send,
        recv_sem=recv,
        device_id=where,
        device_id_type=MESH,
    )


def summed_over_heads(ntp, chunk, p, q, zb, acc, p_s, p_r, z_s, z_r):
    tp = lax.axis_index("tp")
    nz = ntp // 2
    core = lax.rem(tp, 2)
    z = lax.div(tp, 2)
    partner = {"tp": tp + 1 - 2 * core}

    def first(i, carry):
        p[i] = chunk(i * 2 + 1 - core).astype(BF)
        remote(p.at[i], q.at[i], p_s.at[i], p_r.at[i], partner).start()
        return carry

    lax.fori_loop(0, nz, first, 0)

    def second(j, carry):
        i = lax.rem(z + j, nz)
        part = chunk(i * 2 + core)
        copy = remote(p.at[i], q.at[i], p_s.at[i], p_r.at[i], partner)
        copy.wait_send()
        copy.wait_recv()
        part = part + q[i].astype(F32)

        @pl.when(j < nz)
        def _():
            p[i] = part.astype(BF)
            remote(
                p.at[i], zb.at[z], z_s.at[j - 1], z_r.at[z], {"tp": i * 2 + core}
            ).start()

        @pl.when(j == nz)
        def _():
            acc[...] = part

        return carry

    lax.fori_loop(1, nz + 1, second, 0)


def from_heads(ntp, p, zb, acc, z_s, z_r):
    tp = lax.axis_index("tp")
    nz = ntp // 2
    core = lax.rem(tp, 2)
    z = lax.div(tp, 2)
    total = acc[...]
    for j in range(1, nz):
        i = lax.rem(z + j, nz)
        copy = remote(p.at[i], zb.at[i], z_s.at[j - 1], z_r.at[i], {"tp": i * 2 + core})
        copy.wait_send()
        copy.wait_recv()
        total = total + zb[i].astype(F32)
    return total


def core_kernel(
    nctx,
    ntp,
    nx,
    tok_h,
    wq_h,
    wk_h,
    wv_h,
    wo_h,
    doc_ref,
    go_h,
    out_o,
    dq_o,
    dk_o,
    dv_o,
    wos_o,
    wfar_o,
    wr_o,
    tx_o,
    ty_o,
    tok,
    w3,
    wo,
    qkv,
    gfull,
    land,
    lk,
    lv,
    pw,
    attn,
    da,
    dqv,
    dkv,
    dvv,
    dkf,
    dvf,
    dlk,
    dlv,
    dls,
    dlr,
    wos,
    acc,
    o_p,
    o_q,
    o_z,
    o_a,
    outv,
    ld,
    st,
    g_s,
    g_r,
    f_s,
    l_s,
    l_r,
    d_s,
    d_r,
    tx_s,
    tx_r,
    ty_s,
    ty_r,
    t_l,
    fx_s,
    fx_r,
    fy_s,
    fy_r,
    h_s,
    h_r,
    op_s,
    op_r,
    oz_s,
    oz_r,
    w0_s,
    w0_r,
    w1_s,
    w1_r,
):
    ctx = lax.axis_index("ctx")
    ny = nctx // nx
    y = lax.div(ctx, nx)
    x = lax.rem(ctx, nx)
    tp = lax.axis_index("tp")
    nz = ntp // 2
    core = lax.rem(tp, 2)
    z = lax.div(tp, 2)
    partner = tp + 1 - 2 * core
    rows, width = tok.shape
    cols = qkv.shape[2]
    heads = cols // HDIM
    own_blocks = rows // BLOCK
    all_blocks = nctx * own_blocks
    per = 2 * own_blocks
    scale = 1.0 / math.sqrt(HDIM)

    def shard(t):
        return pl.ds(pl.multiple_of(t * cols, cols), cols)

    def mate(j, side):
        return lax.rem(z + j, nz) * 2 + side

    load_tok = pltpu.make_async_copy(tok_h, tok, ld.at[0])
    load_tok.start()
    for i, w_h in enumerate((wk_h, wv_h, wq_h)):
        pltpu.make_async_copy(w_h, w3.at[i], ld.at[1 + i]).start()
    load_wo = pltpu.make_async_copy(wo_h, wo, ld.at[4])
    load_wo.start()
    load_go = pltpu.make_async_copy(go_h, gfull.at[:, shard(tp)], ld.at[5])
    load_go.start()

    barrier = pltpu.get_barrier_semaphore()

    def greet(i, carry):
        pl.semaphore_signal(
            barrier, inc=1, device_id={"ctx": lax.rem(ctx + i, nctx)}, device_id_type=MESH
        )
        return carry

    lax.fori_loop(1, nctx, greet, 0)
    pl.semaphore_signal(barrier, inc=1, device_id={"tp": partner}, device_id_type=MESH)
    for j in range(1, nz):
        pl.semaphore_signal(barrier, inc=1, device_id={"tp": mate(j, core)}, device_id_type=MESH)
    pl.semaphore_wait(barrier, nctx - 1 + nz)

    def grad_copy(source, owner, send, target):
        return pltpu.make_async_remote_copy(
            src_ref=source,
            dst_ref=gfull.at[:, shard(owner)],
            send_sem=send,
            recv_sem=g_r.at[owner],
            device_id={"tp": target},
            device_id_type=MESH,
        )

    first_sends = [
        grad_copy(go_h, tp, g_s.at[0], mate(1, core)),
        grad_copy(go_h, tp, g_s.at[1], mate(nz - 1, core)),
        grad_copy(go_h, tp, g_s.at[2], partner),
    ]
    for send in first_sends:
        send.start()

    strip = width // nctx
    own_half = pl.ds(pl.multiple_of(core * (rows // 2), rows // 2), rows // 2)

    def strip_at(i):
        return pl.ds(pl.multiple_of(i * strip, strip), strip)

    def x_copy(j, i, owner):
        return pltpu.make_async_remote_copy(
            src_ref=tok.at[own_half, strip_at(i * nx + lax.rem(x + j, nx))],
            dst_ref=tx_o.at[owner, own_half, strip_at(i)],
            send_sem=tx_s.at[j - 1, i],
            recv_sem=tx_r.at[owner, i],
            device_id={"ctx": y * nx + lax.rem(x + j, nx)},
            device_id_type=MESH,
        )

    def y_copy(j, owner):
        there = lax.rem(y + j, ny)
        return pltpu.make_async_remote_copy(
            src_ref=tok.at[own_half, pl.ds(pl.multiple_of(there * nx * strip, strip), nx * strip)],
            dst_ref=ty_o.at[owner, own_half],
            send_sem=ty_s.at[j - 1],
            recv_sem=ty_r.at[owner],
            device_id={"ctx": there * nx + x},
            device_id_type=MESH,
        )

    def pass_on(ref, owner, send, recv):
        return pltpu.make_async_remote_copy(
            src_ref=ref.at[owner, own_half],
            dst_ref=ref.at[owner, own_half],
            send_sem=send,
            recv_sem=recv,
            device_id={"tp": partner},
            device_id_type=MESH,
        )

    def send_tokens(j):
        for i in range(ny):
            x_copy(j, i, x).start()
        y_copy(j, y).start()

    load_tok.wait()

    half = cols // 2

    def project(i, carry):
        pltpu.make_async_copy(wk_h, w3.at[i], ld.at[1 + i]).wait()

        def piece(n, inner):
            at = pl.ds(pl.multiple_of(n * half, half), half)
            qkv[i, :, at] = dot_nn(tok[...], w3[i, :, at]).astype(BF)
            return inner

        lax.fori_loop(0, 2, piece, 0)

        @pl.when(i == 1)
        def _():
            r = iota((per, rows), 0)
            c = iota((per, rows), 1)
            pick_k = one_hot(c == r * BLOCK + BLOCK - 1)
            pick_v = one_hot(c == (r - own_blocks) * BLOCK + BLOCK - 1)
            pick_k = jnp.where(r < own_blocks, pick_k, jnp.zeros_like(pick_k))
            pick_v = jnp.where(r >= own_blocks, pick_v, jnp.zeros_like(pick_v))
            land[ctx] = (dot_nn(pick_k, qkv[0]) + dot_nn(pick_v, qkv[1])).astype(BF)

            def spread(j, inner):
                pltpu.make_async_remote_copy(
                    src_ref=land.at[ctx],
                    dst_ref=land.at[ctx],
                    send_sem=l_s.at[j - 1],
                    recv_sem=l_r.at[ctx],
                    device_id={"ctx": lax.rem(ctx + j, nctx)},
                    device_id_type=MESH,
                ).start()
                return inner

            lax.fori_loop(1, nctx, spread, 0)

        return carry

    lax.fori_loop(0, 3, project, 0)

    def land_wait(j, carry):
        source = lax.rem(ctx + j, nctx)
        copy = pltpu.make_async_remote_copy(
            src_ref=land.at[ctx],
            dst_ref=land.at[source],
            send_sem=l_s.at[j - 1],
            recv_sem=l_r.at[source],
            device_id={"ctx": source},
            device_id_type=MESH,
        )
        copy.wait_send()
        copy.wait_recv()
        return carry

    def row_half(way):
        return pl.ds(way * (rows // 2), rows // 2)

    def relay(way):
        owner = mate(nz - 1 if way == 0 else 1, core)
        view = gfull.at[row_half(way), shard(owner)]
        return pltpu.make_async_remote_copy(
            src_ref=view,
            dst_ref=view,
            send_sem=h_s.at[way],
            recv_sem=h_r.at[way],
            device_id={"tp": mate(1 if way == 0 else nz - 1, core)},
            device_id_type=MESH,
        )

    def relay_wait(way):
        view = gfull.at[row_half(way), shard(mate(2, core))]
        pltpu.make_async_remote_copy(
            src_ref=view,
            dst_ref=view,
            send_sem=h_s.at[way],
            recv_sem=h_r.at[way],
            device_id={"tp": mate(nz - 1 if way == 0 else 1, core)},
            device_id_type=MESH,
        ).wait_recv()

    lax.fori_loop(1, nctx, land_wait, 0)
    send_tokens(1)
    send_tokens(3)
    send_tokens(2)
    forwards = []

    def pass_shard(owner, slot):
        onward = grad_copy(gfull.at[:, shard(owner)], owner, f_s.at[slot], partner)
        onward.start()
        forwards.append(onward)

    for way in range(2):
        owner = mate(nz - 1 if way == 0 else 1, core)
        grad_copy(gfull.at[:, shard(owner)], owner, f_s.at[way], partner).wait_recv()
        relay(way).start()
        pass_shard(owner, way)


    own_strips = [
        pltpu.make_async_copy(
            tok.at[:, strip_at(i * nx + x)], tx_o.at[x, :, strip_at(i)], t_l.at[i]
        )
        for i in range(ny)
    ]
    own_strips.append(
        pltpu.make_async_copy(
            tok.at[:, pl.ds(pl.multiple_of(y * nx * strip, strip), nx * strip)],
            ty_o.at[y],
            t_l.at[ny],
        )
    )
    for copy in own_strips:
        copy.start()

    b = iota((all_blocks, nctx * per), 0)
    c = iota((all_blocks, nctx * per), 1)
    shift = b // own_blocks * own_blocks
    landed = land[...].reshape(nctx * per, cols)
    lk[...] = dot_nn(one_hot(c == b + shift), landed).astype(BF)
    lv[...] = dot_nn(one_hot(c == b + shift + own_blocks), landed).astype(BF)

    span = PAIR + all_blocks
    doc = doc_ref[...]
    doc_lane = iota(doc.shape, 1)
    doc_wide = jnp.concatenate([jnp.zeros((1, PAIR), jnp.int32), doc], axis=1)

    def forward(sb, carry):
        at = pl.ds(pl.multiple_of(sb * PAIR, PAIR), PAIR)
        row = iota((PAIR, span), 0)
        col = iota((PAIR, span), 1)
        upper = jnp.where(row >= BLOCK, 1, 0)
        col_upper = jnp.where(col >= BLOCK, 1, 0)
        first = ctx * own_blocks + sb * 2
        doc_a = jnp.sum(jnp.where(doc_lane == first, doc, 0), axis=1, keepdims=True)
        doc_b = jnp.sum(jnp.where(doc_lane == first + 1, doc, 0), axis=1, keepdims=True)
        own_doc = jnp.where(row >= BLOCK, doc_b, doc_a)
        near = (col < PAIR) & (upper == col_upper) & (col <= row)
        far = (col >= PAIR) & (col - PAIR < first + upper) & (doc_wide == own_doc)
        mask = near | far
        for h in range(heads):
            hs = pl.ds(h * HDIM, HDIM)
            keys = jnp.concatenate([qkv[0, at, hs], lk[:, hs]], axis=0)
            values = jnp.concatenate([qkv[1, at, hs], lv[:, hs]], axis=0)
            scores = dot_nt(qkv[2, at, hs], keys) * scale
            scores = jnp.where(mask, scores, big_negative)
            top = jnp.max(scores, axis=1, keepdims=True)
            e = jnp.exp(scores - top)
            weight = (e / jnp.sum(e, axis=1, keepdims=True)).astype(BF)
            pw[sb * heads + h] = weight
            attn[at, hs] = dot_nn(weight, values).astype(BF)
        return carry

    lax.fori_loop(0, rows // PAIR, forward, 0)
    load_wo.wait()

    def out_chunk(t):
        return dot_nn(attn[...], wo[:, shard(t)])

    summed_over_heads(ntp, out_chunk, o_p, o_q, o_z, o_a, op_s, op_r, oz_s, oz_r)
    load_go.wait()

    def use_chip(hop, fresh):
        chip = lax.rem(z + hop, nz)
        both = pl.ds(pl.multiple_of(chip * 2 * cols, 2 * cols), 2 * cols)
        grads = gfull[:, both]
        product = dot_nt(grads, wo[:, both])
        if fresh:
            acc[...] = product
        else:
            acc[...] += product
        part = dot_tn(attn[...], grads).astype(BF)
        each = 2 * (nctx // ntp)
        for k in range(each):
            i = chip * each + k
            there_y = lax.div(i, nx)
            there_x = lax.rem(i, nx)
            wos[0, there_x, there_y] = part[: cols // 2, k * strip : (k + 1) * strip]
            wos[1, there_y, there_x] = part[cols // 2 :, k * strip : (k + 1) * strip]

    def other_core(hop, slot):
        t = mate(hop, 1 - core)
        grad_copy(gfull.at[:, shard(t)], t, f_s.at[slot], partner).wait_recv()

    other_core(0, 0)
    use_chip(0, True)

    def use_near(i, carry):
        hop = 1 + (nz - 2) * i
        other_core(hop, 0)
        use_chip(hop, False)
        return carry

    lax.fori_loop(0, 2, use_near, 0)
    for way in range(2):
        relay_wait(way)
    pass_shard(mate(2, core), 2)
    other_core(2, 2)
    use_chip(2, False)
    da[...] = acc[...].astype(BF)
    out_wos = pltpu.make_async_copy(wos, wos_o, st.at[4])
    out_wos.start()
    rings = ((x, nx, lambda i: {"ctx": y * nx + i}), (y, ny, lambda i: {"ctx": i * nx + x}))
    subs = (pl.ds(0, nx // 2), pl.ds(nx // 2, nx // 2))

    def far_hop(side, way):
        pos, n, at = rings[side]
        return remote(
            wos.at[side, lax.rem(pos + 2, n), subs[way]],
            wfar_o.at[side, subs[way]],
            w0_s.at[side, way],
            w0_r.at[side, way],
            at(lax.rem(pos + (1 if way == 0 else n - 1), n)),
        )

    def near_hop(side, way):
        pos, n, at = rings[side]
        there = lax.rem(pos + (1 if way == 0 else n - 1), n)
        return remote(
            wos.at[side, there, subs[1 - way]],
            wr_o.at[side, way, subs[1 - way]],
            w1_s.at[side, way],
            w1_r.at[side, way],
            at(there),
        )

    for way in range(2):
        for side in range(2):
            far_hop(side, way).start()

    dlk[...] = jnp.zeros_like(dlk)
    dlv[...] = jnp.zeros_like(dlv)

    def backward(sb, carry):
        at = pl.ds(pl.multiple_of(sb * PAIR, PAIR), PAIR)
        for h in range(heads):
            hs = pl.ds(h * HDIM, HDIM)
            keys = jnp.concatenate([qkv[0, at, hs], lk[:, hs]], axis=0)
            values = jnp.concatenate([qkv[1, at, hs], lv[:, hs]], axis=0)
            weight = pw[sb * heads + h]
            d_out = da[at, hs]
            delta = jnp.sum(
                attn[at, hs].astype(F32) * d_out.astype(F32), axis=1, keepdims=True
            )
            d_weight = dot_nt(d_out, values)
            ds = (weight.astype(F32) * (d_weight - delta)).astype(BF)
            dqv[at, hs] = (dot_nn(ds, keys) * scale).astype(BF)
            d_keys = dot_tn(ds, qkv[2, at, hs]) * scale
            d_values = dot_tn(weight, d_out)
            dkf[at, hs] = d_keys[:PAIR]
            dvf[at, hs] = d_values[:PAIR]
            dlk[:, hs] += d_keys[PAIR:]
            dlv[:, hs] += d_values[PAIR:]
        return carry

    lax.fori_loop(0, rows // PAIR, backward, 0)
    out_dq = pltpu.make_async_copy(dqv, dq_o, st.at[1])
    out_dq.start()

    r = iota((nctx * per, all_blocks), 0)
    b = iota((nctx * per, all_blocks), 1)
    shift = b // own_blocks * own_blocks
    packed = dot_nn(one_hot(r == b + shift), dlk[...].astype(BF)) + dot_nn(
        one_hot(r == b + shift + own_blocks), dlv[...].astype(BF)
    )
    dls[...] = packed.astype(BF).reshape(nctx, per, cols)

    def give(j, carry):
        target = lax.rem(ctx + j, nctx)
        pltpu.make_async_remote_copy(
            src_ref=dls.at[target],
            dst_ref=dlr.at[ctx],
            send_sem=d_s.at[j - 1],
            recv_sem=d_r.at[ctx],
            device_id={"ctx": target},
            device_id_type=MESH,
        ).start()
        return carry

    lax.fori_loop(1, nctx, give, 0)
    for way in range(2):
        for side in range(2):
            near_hop(side, way).start()
    dlr[ctx] = dls[ctx]

    for j in range(1, nx):
        owner = lax.rem(x + j, nx)
        for i in range(ny):
            x_copy(j, i, owner).wait_recv()
        pass_on(tx_o, owner, fx_s.at[j - 1], fx_r.at[j - 1]).start()
    for j in range(1, ny):
        owner = lax.rem(y + j, ny)
        y_copy(j, owner).wait_recv()
        pass_on(ty_o, owner, fy_s.at[j - 1], fy_r.at[j - 1]).start()

    def take(j, carry):
        source = lax.rem(ctx + j, nctx)
        copy = pltpu.make_async_remote_copy(
            src_ref=dls.at[source],
            dst_ref=dlr.at[source],
            send_sem=d_s.at[j - 1],
            recv_sem=d_r.at[source],
            device_id={"ctx": source},
            device_id_type=MESH,
        )
        copy.wait_send()
        copy.wait_recv()
        return carry

    lax.fori_loop(1, nctx, take, 0)
    total = jnp.zeros((per, cols), F32)
    for i in range(nctx):
        total = total + dlr[i].astype(F32)
    for i in range(own_blocks):
        last = pl.ds(i * BLOCK + BLOCK - 1, 1)
        dkf[last, :] += total[i : i + 1]
        dvf[last, :] += total[own_blocks + i : own_blocks + i + 1]
    dkv[...] = dkf[...].astype(BF)
    dvv[...] = dvf[...].astype(BF)
    out_dk = pltpu.make_async_copy(dkv, dk_o, st.at[2])
    out_dk.start()
    out_dv = pltpu.make_async_copy(dvv, dv_o, st.at[3])
    out_dv.start()
    outv[...] = (
        tok[:, shard(tp)].astype(F32) + from_heads(ntp, o_p, o_z, o_a, oz_s, oz_r)
    ).astype(BF)
    out_out = pltpu.make_async_copy(outv, out_o, st.at[5])
    out_out.start()
    for way in range(2):
        for side in range(2):
            for copy in (far_hop(side, way), near_hop(side, way)):
                copy.wait_send()
                copy.wait_recv()
    for send in first_sends + forwards + [relay(0), relay(1)]:
        send.wait_send()
    for copy in [out_out, out_dq, out_dk, out_dv, out_wos] + own_strips:
        copy.wait()
    for j in range(1, nx):
        for i in range(ny):
            x_copy(j, i, x).wait_send()
        passed = pass_on(tx_o, lax.rem(x + j, nx), fx_s.at[j - 1], fx_r.at[j - 1])
        passed.wait_send()
        other_half = pl.ds(pl.multiple_of((1 - core) * (rows // 2), rows // 2), rows // 2)
        pltpu.make_async_remote_copy(
            src_ref=tx_o.at[lax.rem(x + j, nx), other_half],
            dst_ref=tx_o.at[lax.rem(x + j, nx), other_half],
            send_sem=fx_s.at[j - 1],
            recv_sem=fx_r.at[j - 1],
            device_id={"tp": partner},
            device_id_type=MESH,
        ).wait_recv()
    for j in range(1, ny):
        y_copy(j, y).wait_send()
        passed = pass_on(ty_o, lax.rem(y + j, ny), fy_s.at[j - 1], fy_r.at[j - 1])
        passed.wait_send()
        other_half = pl.ds(pl.multiple_of((1 - core) * (rows // 2), rows // 2), rows // 2)
        pltpu.make_async_remote_copy(
            src_ref=ty_o.at[lax.rem(y + j, ny), other_half],
            dst_ref=ty_o.at[lax.rem(y + j, ny), other_half],
            send_sem=fy_s.at[j - 1],
            recv_sem=fy_r.at[j - 1],
            device_id={"tp": partner},
            device_id_type=MESH,
        ).wait_recv()


def attention_core(nctx, ntp, nx, tokens, w_query, w_key, w_value, w_out, block_doc, grad_out):
    rows, width = tokens.shape
    cols = w_query.shape[1]
    heads = cols // HDIM
    own_blocks = rows // BLOCK
    all_blocks = nctx * own_blocks
    per = 2 * own_blocks
    units = rows // PAIR * heads
    ny = nctx // nx
    small = jax.ShapeDtypeStruct((rows, cols), BF)
    hbm = pl.BlockSpec(memory_space=pl.ANY)
    dma = pltpu.SemaphoreType.DMA
    return pl.pallas_call(
        functools.partial(core_kernel, nctx, ntp, nx),
        out_shape=(
            small,
            small,
            small,
            small,
            jax.ShapeDtypeStruct((2, nx, ny, cols // 2, width // nctx), BF),
            jax.ShapeDtypeStruct((2, ny, cols // 2, width // nctx), BF),
            jax.ShapeDtypeStruct((2, 2, ny, cols // 2, width // nctx), BF),
            jax.ShapeDtypeStruct((nx, rows, width // nx), BF),
            jax.ShapeDtypeStruct((ny, rows, width // ny), BF),
        ),
        in_specs=[hbm] * 5 + [pl.BlockSpec(memory_space=pltpu.VMEM), hbm],
        out_specs=(hbm,) * 9,
        scratch_shapes=[
            pltpu.VMEM((rows, width), BF),
            pltpu.VMEM((3, width, cols), BF),
            pltpu.VMEM((cols, width), BF),
            pltpu.VMEM((3, rows, cols), BF),
            pltpu.VMEM((rows, width), BF),
            pltpu.VMEM((nctx, per, cols), BF),
            pltpu.VMEM((all_blocks, cols), BF),
            pltpu.VMEM((all_blocks, cols), BF),
            pltpu.VMEM((units, PAIR, PAIR + all_blocks), BF),
            pltpu.VMEM((rows, cols), BF),
            pltpu.VMEM((rows, cols), BF),
            pltpu.VMEM((rows, cols), BF),
            pltpu.VMEM((rows, cols), BF),
            pltpu.VMEM((rows, cols), BF),
            pltpu.VMEM((rows, cols), F32),
            pltpu.VMEM((rows, cols), F32),
            pltpu.VMEM((all_blocks, cols), F32),
            pltpu.VMEM((all_blocks, cols), F32),
            pltpu.VMEM((nctx, per, cols), BF),
            pltpu.VMEM((nctx, per, cols), BF),
            pltpu.VMEM((2, nx, ny, cols // 2, width // nctx), BF),
            pltpu.VMEM((rows, cols), F32),
            pltpu.VMEM((ntp // 2, rows, cols), BF),
            pltpu.VMEM((ntp // 2, rows, cols), BF),
            pltpu.VMEM((ntp // 2, rows, cols), BF),
            pltpu.VMEM((rows, cols), F32),
            pltpu.VMEM((rows, cols), BF),
            dma((6,)),
            dma((6,)),
            dma((ntp // 2,)),
            dma((ntp,)),
            dma((ntp // 2,)),
            dma((nctx - 1,)),
            dma((nctx,)),
            dma((nctx - 1,)),
            dma((nctx,)),
            dma((nx - 1, ny)),
            dma((nx, ny)),
            dma((ny - 1,)),
            dma((ny,)),
            dma((ny + 1,)),
            dma((nx - 1,)),
            dma((nx - 1,)),
            dma((ny - 1,)),
            dma((ny - 1,)),
            dma((2,)),
            dma((2,)),
            dma((ntp // 2,)),
            dma((ntp // 2,)),
            dma((ntp // 2 - 1,)),
            dma((ntp // 2,)),
            dma((2, 2)),
            dma((2, 2)),
            dma((2, 2)),
            dma((2, 2)),
        ],
        compiler_params=pltpu.CompilerParams(
            collective_id=1, has_side_effects=True, vmem_limit_bytes=64 * 1024 * 1024 - 65536
        ),
        name="attention_core",
    )(tokens, w_query, w_key, w_value, w_out, block_doc.reshape(1, -1), grad_out)


def grad_kernel(
    nctx,
    ntp,
    nx,
    dq_h,
    dk_h,
    dv_h,
    wos_h,
    wfar_h,
    wr_h,
    tx_h,
    ty_h,
    wq_h,
    wk_h,
    wv_h,
    go_h,
    gt_o,
    gq_o,
    gk_o,
    gv_o,
    gwo_o,
    w3,
    dcat,
    rest_g,
    gq,
    gk,
    gvx,
    gvy,
    d_p,
    d_q,
    d_z,
    d_a,
    sq,
    sk,
    sv,
    rq,
    rk,
    rv,
    oq,
    ok,
    ov,
    wo_own,
    wo_nb,
    wo_far,
    wo_r,
    wo_t,
    wo_u,
    wo_a,
    ld,
    dl,
    ag_s,
    ag_r,
    dp_s,
    dp_r,
    dz_s,
    dz_r,
    rf_s,
    rf_r,
    rs_s,
    rs_r,
    w1_s,
    w1_r,
    w2_s,
    w2_r,
):
    ctx = lax.axis_index("ctx")
    tp = lax.axis_index("tp")
    ny = nctx // nx
    nz = ntp // 2
    y = lax.div(ctx, nx)
    x = lax.rem(ctx, nx)
    core = lax.rem(tp, 2)
    z = lax.div(tp, 2)
    partner = tp + 1 - 2 * core
    rows, cols = rest_g.shape
    width = w3.shape[0]
    strip = width // nctx
    gathered = nx * rows
    half = cols // 2

    def block(t):
        return pl.ds(pl.multiple_of(t * cols, cols), cols)

    def strip_at(i):
        return pl.ds(pl.multiple_of(i * strip, strip), strip)

    def at_x(i):
        return {"ctx": y * nx + i}

    def at_y(i):
        return {"ctx": i * nx + x}

    loads = []
    for i, (d_h, w_h) in enumerate(((dq_h, wq_h), (dk_h, wk_h), (dv_h, wv_h))):
        lanes = pl.ds(i * cols, cols)
        loads.append(pltpu.make_async_copy(d_h, dcat.at[:, lanes], ld.at[2 + 2 * i]))
        loads.append(pltpu.make_async_copy(w_h, w3.at[:, lanes], ld.at[3 + 2 * i]))
    loads.append(pltpu.make_async_copy(go_h, rest_g, ld.at[9]))
    lo = pl.ds(0, half)
    hi = pl.ds(half, half)
    gathers = (
        (dq_h, gq, x, at_x, 0),
        (dk_h, gk, y, at_y, 1),
        (dv_h.at[:, lo], gvx, x, at_x, 2),
        (dv_h.at[:, hi], gvy, y, at_y, 3),
    )
    for source, buf, pos, at, i in gathers:
        loads.append(pltpu.make_async_copy(source, buf.at[pos], ld.at[10 + i]))
    rings = ((x, nx, at_x), (y, ny, at_y))
    for side in range(2):
        pos, n, at = rings[side]
        for k, target in ((0, wo_own), (1, wo_nb.at[:, 0]), (n - 1, wo_nb.at[:, 1])):
            loads.append(
                pltpu.make_async_copy(
                    wos_h.at[side, lax.rem(pos + k, n)],
                    target.at[side],
                    ld.at[14 + 3 * side + min(k, 2)],
                )
            )
    loads.append(pltpu.make_async_copy(wfar_h, wo_far, ld.at[0]))
    subs = (pl.ds(0, nx // 2), pl.ds(nx // 2, nx // 2))
    for side in range(2):
        for way in range(2):
            loads.append(
                pltpu.make_async_copy(
                    wr_h.at[side, way, subs[1 - way]],
                    wo_r.at[side, way, subs[1 - way]],
                    dl.at[side, way],
                )
            )
    for load in loads:
        load.start()

    barrier = pltpu.get_barrier_semaphore()
    for j in range(1, nx):
        pl.semaphore_signal(
            barrier, inc=1, device_id=at_x(lax.rem(x + j, nx)), device_id_type=MESH
        )
    for j in range(1, ny):
        pl.semaphore_signal(
            barrier, inc=1, device_id=at_y(lax.rem(y + j, ny)), device_id_type=MESH
        )
    for j in range(1, nz):
        pl.semaphore_signal(
            barrier,
            inc=1,
            device_id={"tp": lax.rem(z + j, nz) * 2 + core},
            device_id_type=MESH,
        )
    pl.semaphore_signal(barrier, inc=1, device_id={"tp": partner}, device_id_type=MESH)
    pl.semaphore_wait(barrier, nx + ny + nz - 2)

    def near_send(gather, step):
        source, buf, pos, at, i = gather
        n = buf.shape[0]
        there = lax.rem(pos + (1 if step == 0 else n - 1), n)
        return remote(source, buf.at[pos], ag_s.at[i, step], ag_r.at[i, step], at(there))

    def near_recv(gather, step):
        source, buf, pos, at, i = gather
        n = buf.shape[0]
        owner = lax.rem(pos + (n - 1 if step == 0 else 1), n)
        return remote(source, buf.at[owner], ag_s.at[i, step], ag_r.at[i, step], at(owner))

    def relay(gather, step):
        source, buf, pos, at, i = gather
        n = buf.shape[0]
        part = pl.ds(0, rows // 2) if step == 0 else pl.ds(rows // 2, rows // 2)
        owner = lax.rem(pos + (n - 1 if step == 0 else 1), n)
        there = lax.rem(pos + (1 if step == 0 else n - 1), n)
        return remote(
            buf.at[owner, part],
            buf.at[owner, part],
            ag_s.at[i, 2 + step],
            ag_r.at[i, 2 + step],
            at(there),
        )

    def relay_recv(gather, step):
        source, buf, pos, at, i = gather
        n = buf.shape[0]
        part = pl.ds(0, rows // 2) if step == 0 else pl.ds(rows // 2, rows // 2)
        owner = lax.rem(pos + 2, n)
        return remote(
            buf.at[owner, part],
            buf.at[owner, part],
            ag_s.at[i, 2 + step],
            ag_r.at[i, 2 + step],
            at(owner),
        )

    for gather in gathers:
        near_send(gather, 0).start()
        near_send(gather, 1).start()

    def near_hop(side, way):
        pos, n, at = rings[side]
        part = subs[way]
        return remote(
            wo_nb.at[side, way, part],
            wo_r.at[side, way, part],
            w1_s.at[side, way],
            w1_r.at[side, way],
            at(lax.rem(pos + (1 if way == 0 else n - 1), n)),
        )

    def tok_chunk(t):
        return dot_nt(dcat[...], w3[block(t), :])

    for load in loads[:6]:
        load.wait()
    summed_over_heads(ntp, tok_chunk, d_p, d_q, d_z, d_a, dp_s, dp_r, dz_s, dz_r)
    t_x = w3.at[pl.ds(0, gathered), pl.ds(0, width // nx)]
    t_y = w3.at[pl.ds(gathered, gathered), pl.ds(0, width // ny)]
    late = []
    for i in range(nx):
        part = pl.ds(i * rows, rows)
        late.append(pltpu.make_async_copy(tx_h.at[i], t_x.at[part], ld.at[20 + i]))
        late.append(pltpu.make_async_copy(ty_h.at[i], t_y.at[part], ld.at[20 + nx + i]))
    for load in late:
        load.start()

    for gather in gathers:
        for step in range(2):
            near_recv(gather, step).wait_recv()
            relay(gather, step).start()

    for load in loads[6:] + late:
        load.wait()
    for side in range(2):
        for way in range(2):
            part = subs[way]
            wo_nb[side, way, part] = (
                wo_nb[side, way, part].astype(F32) + wo_far[side, part].astype(F32)
            ).astype(BF)
            near_hop(side, way).start()

    sends = (
        (gathers[0], 0, sq, rq, oq, y, at_y, 0),
        (gathers[1], 1, sk, rk, ok, x, at_x, 1),
        (gathers[2], 0, sv.at[:, :, lo], rv.at[:, :, lo], ov.at[:, lo], y, at_y, 2),
        (gathers[3], 1, sv.at[:, :, hi], rv.at[:, :, hi], ov.at[:, hi], x, at_x, 3),
    )
    ends = (pl.ds(0, strip // 2), pl.ds(strip // 2, strip // 2))

    def weight_far(item, way):
        gather, side, s, r, o, pos, at, i = item
        n = nx
        return remote(
            s.at[0, ends[way]],
            r.at[0, ends[way]],
            rf_s.at[i, way],
            rf_r.at[i, way],
            at(lax.rem(pos + (1 if way == 0 else n - 1), n)),
        )

    def weight_near(item, way, added):
        gather, side, s, r, o, pos, at, i = item
        n = nx
        part = ends[way if added else 1 - way]
        return remote(
            s.at[1 + way, part],
            r.at[1 + way, part],
            rs_s.at[i, way, 1 if added else 0],
            rs_r.at[i, way, 1 if added else 0],
            at(lax.rem(pos + (1 if way == 0 else n - 1), n)),
        )

    for item in sends:
        gather, side, s, r, o, pos, at, i = item
        for step in range(2):
            relay_recv(gather, step).wait_recv()
        buf = gather[1]
        n = buf.shape[0]
        base = pl.ds(side * gathered, gathered)

        def weight_piece(k, carry):
            there = lax.rem(pos + 6 - k, n)
            part = dot_tn(
                w3[base, strip_at(there)], buf[...].reshape(gathered, buf.shape[2])
            )

            @pl.when(k == 0)
            def _():
                s[0] = part.astype(BF)
                weight_far(item, 0).start()
                weight_far(item, 1).start()

            @pl.when(k == 1)
            def _():
                s[1] = part.astype(BF)
                weight_near(item, 0, False).start()

            @pl.when(k == 2)
            def _():
                o[...] = part

            @pl.when(k == 3)
            def _():
                s[2] = part.astype(BF)
                weight_near(item, 1, False).start()

            return carry

        lax.fori_loop(0, n, weight_piece, 0)

    for item in sends:
        gather, side, s, r, o, pos, at, i = item
        for way in range(2):
            weight_far(item, way).wait_recv()
            part = ends[way]
            s[1 + way, part] = (
                s[1 + way, part].astype(F32) + r[0, part].astype(F32)
            ).astype(BF)
            weight_near(item, way, True).start()

    gt_o[...] = (rest_g[...].astype(F32) + from_heads(ntp, d_p, d_z, d_a, dz_s, dz_r)).astype(BF)

    def second_hop(side, there, slot, owner):
        pos, n, at = ((y, ny, at_y), (x, nx, at_x))[side]
        return remote(
            wo_t.at[side, there],
            wo_u.at[side, owner],
            w2_s.at[side, slot],
            w2_r.at[side, owner],
            at(there),
        )

    for side in range(2):
        pos, m = ((y, ny), (x, nx))[side]
        for way in range(2):
            copy = near_hop(side, way)
            copy.wait_send()
            copy.wait_recv()

        def add_up(j, carry):
            there = lax.rem(pos + j, m)
            total = wo_own[side, there].astype(F32)
            for way in range(2):
                total = total + wo_r[side, way, there].astype(F32)

            @pl.when(j < m)
            def _():
                wo_t[side, there] = total.astype(BF)
                second_hop(side, there, j - 1, pos).start()

            @pl.when(j == m)
            def _():
                wo_a[pl.ds(side * half, half), :] = total

            return carry

        lax.fori_loop(1, m + 1, add_up, 0)

    for item, target in zip(sends, (gq_o, gk_o, gv_o.at[:, lo], gv_o.at[:, hi])):
        gather, side, s, r, o, pos, at, i = item
        for way in range(2):
            weight_far(item, way).wait_send()
            for added in (False, True):
                copy = weight_near(item, way, added)
                copy.wait_send()
                copy.wait_recv()
        target[...] = o[...] + r[1].astype(F32) + r[2].astype(F32)
        for step in range(2):
            near_send(gather, step).wait_send()
            relay(gather, step).wait_send()

    for side in range(2):
        pos, m = ((y, ny), (x, nx))[side]
        total = wo_a[pl.ds(side * half, half), :]
        for j in range(1, m):
            there = lax.rem(pos + j, m)
            copy = second_hop(side, there, j - 1, there)
            copy.wait_send()
            copy.wait_recv()
            total = total + wo_u[side, there].astype(F32)
        gwo_o[pl.ds(side * half, half), :] = total


def gradients(nctx, ntp, nx, core_out, w_query, w_key, w_value, grad_out):
    d_query, d_key, d_value, wos, wfar, wr, tx, ty = core_out
    rows = grad_out.shape[0]
    width = w_query.shape[0]
    cols = w_query.shape[1]
    ny = nctx // nx
    nz = ntp // 2
    strip = width // nctx
    half = cols // 2
    hbm = pl.BlockSpec(memory_space=pl.ANY)
    vmem = pl.BlockSpec(memory_space=pltpu.VMEM)
    dma = pltpu.SemaphoreType.DMA
    small = jax.ShapeDtypeStruct((rows, cols), BF)
    piece = jax.ShapeDtypeStruct((strip, cols), F32)
    heads_scratch = [
        pltpu.VMEM((nz, rows, cols), BF),
        pltpu.VMEM((nz, rows, cols), BF),
        pltpu.VMEM((nz, rows, cols), BF),
        pltpu.VMEM((rows, cols), F32),
    ]
    return pl.pallas_call(
        functools.partial(grad_kernel, nctx, ntp, nx),
        out_shape=(
            small,
            piece,
            piece,
            piece,
            jax.ShapeDtypeStruct((cols, strip), F32),
        ),
        in_specs=[hbm] * 12,
        out_specs=(vmem,) * 5,
        scratch_shapes=[
            pltpu.VMEM((width, 3 * cols), BF),
            pltpu.VMEM((rows, 3 * cols), BF),
            pltpu.VMEM((rows, cols), BF),
            pltpu.VMEM((nx, rows, cols), BF),
            pltpu.VMEM((ny, rows, cols), BF),
            pltpu.VMEM((nx, rows, half), BF),
            pltpu.VMEM((ny, rows, half), BF),
            *heads_scratch,
            pltpu.VMEM((3, strip, cols), BF),
            pltpu.VMEM((3, strip, cols), BF),
            pltpu.VMEM((3, strip, cols), BF),
            pltpu.VMEM((3, strip, cols), BF),
            pltpu.VMEM((3, strip, cols), BF),
            pltpu.VMEM((3, strip, cols), BF),
            pltpu.VMEM((strip, cols), F32),
            pltpu.VMEM((strip, cols), F32),
            pltpu.VMEM((strip, cols), F32),
            pltpu.VMEM((2, ny, half, strip), BF),
            pltpu.VMEM((2, 2, ny, half, strip), BF),
            pltpu.VMEM((2, ny, half, strip), BF),
            pltpu.VMEM((2, 2, ny, half, strip), BF),
            pltpu.VMEM((2, ny, half, strip), BF),
            pltpu.VMEM((2, ny, half, strip), BF),
            pltpu.VMEM((cols, strip), F32),
            dma((20 + nx + ny,)),
            dma((2, 2)),
            dma((4, 4)),
            dma((4, 4)),
            dma((nz,)),
            dma((nz,)),
            dma((nz - 1,)),
            dma((nz,)),
            dma((4, 2)),
            dma((4, 2)),
            dma((4, 2, 2)),
            dma((4, 2, 2)),
            dma((2, 2)),
            dma((2, 2)),
            dma((2, nx - 1)),
            dma((2, nx)),
        ],
        compiler_params=pltpu.CompilerParams(
            collective_id=2, has_side_effects=True, vmem_limit_bytes=64 * 1024 * 1024 - 65536
        ),
        name="gradients",
    )(
        d_query,
        d_key,
        d_value,
        wos,
        wfar,
        wr,
        tx,
        ty,
        w_query,
        w_key,
        w_value,
        grad_out,
    )


def settle_kernel(count, *refs):
    ins, outs, bufs = refs[:count], refs[count : 2 * count], refs[2 * count : 3 * count]
    come, go = refs[3 * count :]
    first = [pltpu.make_async_copy(ins[i], bufs[i], come.at[i]) for i in range(count)]
    second = [pltpu.make_async_copy(bufs[i], outs[i], go.at[i]) for i in range(count)]
    for copy in first:
        copy.start()
    for i in range(count):
        first[i].wait()
        second[i].start()
    for copy in second:
        copy.wait()


def settled(arrays):
    count = len(arrays)
    hbm = pl.BlockSpec(memory_space=pl.ANY)
    shapes = [(a.shape, a.dtype) for a in arrays]
    return pl.pallas_call(
        functools.partial(settle_kernel, count),
        out_shape=tuple(jax.ShapeDtypeStruct(*s) for s in shapes),
        in_specs=[hbm] * count,
        out_specs=(hbm,) * count,
        scratch_shapes=[pltpu.VMEM(*s) for s in shapes]
        + [pltpu.SemaphoreType.DMA((count,)), pltpu.SemaphoreType.DMA((count,))],
        name="settled",
    )(*arrays)


def per_device(nctx, ntp, nx, tokens, w_query, w_key, w_value, w_out, block_doc, grad_out):
    out, *core_out = attention_core(
        nctx, ntp, nx, tokens, w_query, w_key, w_value, w_out, block_doc, grad_out
    )
    grads = gradients(nctx, ntp, nx, core_out, w_query, w_key, w_value, grad_out)
    return settled((out, *grads))


def solution(mesh):
    in_specs = (
        P("ctx", None),
        P(None, "tp"),
        P(None, "tp"),
        P(None, "tp"),
        P("tp", None),
        P(),
        P("ctx", "tp"),
    )
    out_specs = (
        P("ctx", "tp"),
        P("ctx", "tp"),
        P("ctx", "tp"),
        P("ctx", "tp"),
        P("ctx", "tp"),
        P("tp", "ctx"),
    )
    return jax.shard_map(
        functools.partial(per_device, mesh.shape["ctx"], mesh.shape["tp"], math.isqrt(mesh.shape["ctx"])),
        mesh=mesh,
        in_specs=in_specs,
        out_specs=out_specs,
        check_vma=False,
    )
```

```python
import functools
import math

import jax
import jax.numpy as jnp
from jax import lax
from jax.experimental import pallas as pl
from jax.experimental.pallas import tpu as pltpu
from jax.sharding import PartitionSpec as P

HDIM = 128
BLOCK = 64
PAIR = 2 * BLOCK
MESH = pl.DeviceIdType.MESH
BF = jnp.bfloat16
F32 = jnp.float32
big_negative = -1e30


def dot_nn(a, b):
    return lax.dot_general(a, b, (((1,), (0,)), ((), ())), preferred_element_type=F32)


def dot_nt(a, b):
    return lax.dot_general(a, b, (((1,), (1,)), ((), ())), preferred_element_type=F32)


def dot_tn(a, b):
    return lax.dot_general(a, b, (((0,), (0,)), ((), ())), preferred_element_type=F32)


def iota(shape, dim):
    return lax.broadcasted_iota(jnp.int32, shape, dim)


def one_hot(hit):
    return jnp.where(hit, 1.0, 0.0).astype(BF)


def remote(source, target, send, recv, where):
    return pltpu.make_async_remote_copy(
        src_ref=source,
        dst_ref=target,
        send_sem=send,
        recv_sem=recv,
        device_id=where,
        device_id_type=MESH,
    )


def summed_over_heads(ntp, chunk, p, q, zb, acc, p_s, p_r, z_s, z_r):
    tp = lax.axis_index("tp")
    nz = ntp // 2
    core = lax.rem(tp, 2)
    z = lax.div(tp, 2)
    partner = {"tp": tp + 1 - 2 * core}

    def first(i, carry):
        p[i] = chunk(i * 2 + 1 - core).astype(BF)
        remote(p.at[i], q.at[i], p_s.at[i], p_r.at[i], partner).start()
        return carry

    lax.fori_loop(0, nz, first, 0)

    def second(j, carry):
        i = lax.rem(z + j, nz)
        part = chunk(i * 2 + core)
        copy = remote(p.at[i], q.at[i], p_s.at[i], p_r.at[i], partner)
        copy.wait_send()
        copy.wait_recv()
        part = part + q[i].astype(F32)

        @pl.when(j < nz)
        def _():
            p[i] = part.astype(BF)
            remote(
                p.at[i], zb.at[z], z_s.at[j - 1], z_r.at[z], {"tp": i * 2 + core}
            ).start()

        @pl.when(j == nz)
        def _():
            acc[...] = part

        return carry

    lax.fori_loop(1, nz + 1, second, 0)


def from_heads(ntp, p, zb, acc, z_s, z_r):
    tp = lax.axis_index("tp")
    nz = ntp // 2
    core = lax.rem(tp, 2)
    z = lax.div(tp, 2)
    total = acc[...]
    for j in range(1, nz):
        i = lax.rem(z + j, nz)
        copy = remote(p.at[i], zb.at[i], z_s.at[j - 1], z_r.at[i], {"tp": i * 2 + core})
        copy.wait_send()
        copy.wait_recv()
        total = total + zb[i].astype(F32)
    return total


def core_kernel(
    nctx,
    ntp,
    nx,
    tok_h,
    wq_h,
    wk_h,
    wv_h,
    wo_h,
    doc_ref,
    go_h,
    out_o,
    dq_o,
    dk_o,
    dv_o,
    wos_o,
    wfar_o,
    wr_o,
    tx_o,
    ty_o,
    tok,
    w3,
    wo,
    qkv,
    gfull,
    land,
    lk,
    lv,
    pw,
    attn,
    da,
    dqv,
    dkv,
    dvv,
    dkf,
    dvf,
    dlk,
    dlv,
    dls,
    dlr,
    wos,
    acc,
    o_p,
    o_q,
    o_z,
    o_a,
    outv,
    ld,
    st,
    g_s,
    g_r,
    f_s,
    l_s,
    l_r,
    d_s,
    d_r,
    tx_s,
    tx_r,
    ty_s,
    ty_r,
    t_l,
    fx_s,
    fx_r,
    fy_s,
    fy_r,
    h_s,
    h_r,
    op_s,
    op_r,
    oz_s,
    oz_r,
    w0_s,
    w0_r,
    w1_s,
    w1_r,
):
    ctx = lax.axis_index("ctx")
    ny = nctx // nx
    y = lax.div(ctx, nx)
    x = lax.rem(ctx, nx)
    tp = lax.axis_index("tp")
    nz = ntp // 2
    core = lax.rem(tp, 2)
    z = lax.div(tp, 2)
    partner = tp + 1 - 2 * core
    rows, width = tok.shape
    cols = qkv.shape[2]
    heads = cols // HDIM
    own_blocks = rows // BLOCK
    all_blocks = nctx * own_blocks
    per = 2 * own_blocks
    scale = 1.0 / math.sqrt(HDIM)

    def shard(t):
        return pl.ds(pl.multiple_of(t * cols, cols), cols)

    def mate(j, side):
        return lax.rem(z + j, nz) * 2 + side

    barrier = pltpu.get_barrier_semaphore()

    def greet(i, carry):
        pl.semaphore_signal(
            barrier, inc=1, device_id={"ctx": lax.rem(ctx + i, nctx)}, device_id_type=MESH
        )
        return carry

    lax.fori_loop(1, nctx, greet, 0)
    pl.semaphore_signal(barrier, inc=1, device_id={"tp": partner}, device_id_type=MESH)
    for j in range(1, nz):
        pl.semaphore_signal(barrier, inc=1, device_id={"tp": mate(j, core)}, device_id_type=MESH)

    load_tok = pltpu.make_async_copy(tok_h, tok, ld.at[0])
    load_tok.start()
    for i, w_h in enumerate((wk_h, wv_h, wq_h)):
        pltpu.make_async_copy(w_h, w3.at[i], ld.at[1 + i]).start()
    load_wo = pltpu.make_async_copy(wo_h, wo, ld.at[4])
    load_wo.start()
    load_go = pltpu.make_async_copy(go_h, gfull.at[:, shard(tp)], ld.at[5])
    load_go.start()

    pl.semaphore_wait(barrier, nctx - 1 + nz)

    def grad_copy(source, owner, send, target):
        return pltpu.make_async_remote_copy(
            src_ref=source,
            dst_ref=gfull.at[:, shard(owner)],
            send_sem=send,
            recv_sem=g_r.at[owner],
            device_id={"tp": target},
            device_id_type=MESH,
        )

    first_sends = [
        grad_copy(go_h, tp, g_s.at[0], mate(1, core)),
        grad_copy(go_h, tp, g_s.at[1], mate(nz - 1, core)),
        grad_copy(go_h, tp, g_s.at[2], partner),
    ]
    for send in first_sends:
        send.start()

    strip = width // nctx
    own_half = pl.ds(pl.multiple_of(core * (rows // 2), rows // 2), rows // 2)

    def strip_at(i):
        return pl.ds(pl.multiple_of(i * strip, strip), strip)

    def x_copy(j, i, owner):
        return pltpu.make_async_remote_copy(
            src_ref=tok.at[own_half, strip_at(i * nx + lax.rem(x + j, nx))],
            dst_ref=tx_o.at[owner, own_half, strip_at(i)],
            send_sem=tx_s.at[j - 1, i],
            recv_sem=tx_r.at[owner, i],
            device_id={"ctx": y * nx + lax.rem(x + j, nx)},
            device_id_type=MESH,
        )

    def y_copy(j, owner):
        there = lax.rem(y + j, ny)
        return pltpu.make_async_remote_copy(
            src_ref=tok.at[own_half, pl.ds(pl.multiple_of(there * nx * strip, strip), nx * strip)],
            dst_ref=ty_o.at[owner, own_half],
            send_sem=ty_s.at[j - 1],
            recv_sem=ty_r.at[owner],
            device_id={"ctx": there * nx + x},
            device_id_type=MESH,
        )

    def pass_on(ref, owner, send, recv):
        return pltpu.make_async_remote_copy(
            src_ref=ref.at[owner, own_half],
            dst_ref=ref.at[owner, own_half],
            send_sem=send,
            recv_sem=recv,
            device_id={"tp": partner},
            device_id_type=MESH,
        )

    def send_tokens(j):
        for i in range(ny):
            x_copy(j, i, x).start()
        y_copy(j, y).start()

    load_tok.wait()

    half = cols // 2

    def project(i, carry):
        pltpu.make_async_copy(wk_h, w3.at[i], ld.at[1 + i]).wait()

        def piece(n, inner):
            at = pl.ds(pl.multiple_of(n * half, half), half)
            qkv[i, :, at] = dot_nn(tok[...], w3[i, :, at]).astype(BF)
            return inner

        lax.fori_loop(0, 2, piece, 0)

        @pl.when(i == 1)
        def _():
            r = iota((per, rows), 0)
            c = iota((per, rows), 1)
            pick_k = one_hot(c == r * BLOCK + BLOCK - 1)
            pick_v = one_hot(c == (r - own_blocks) * BLOCK + BLOCK - 1)
            pick_k = jnp.where(r < own_blocks, pick_k, jnp.zeros_like(pick_k))
            pick_v = jnp.where(r >= own_blocks, pick_v, jnp.zeros_like(pick_v))
            land[ctx] = (dot_nn(pick_k, qkv[0]) + dot_nn(pick_v, qkv[1])).astype(BF)

            def spread(j, inner):
                pltpu.make_async_remote_copy(
                    src_ref=land.at[ctx],
                    dst_ref=land.at[ctx],
                    send_sem=l_s.at[j - 1],
                    recv_sem=l_r.at[ctx],
                    device_id={"ctx": lax.rem(ctx + j, nctx)},
                    device_id_type=MESH,
                ).start()
                return inner

            lax.fori_loop(1, nctx, spread, 0)

        return carry

    lax.fori_loop(0, 3, project, 0)

    def land_wait(j, carry):
        source = lax.rem(ctx + j, nctx)
        copy = pltpu.make_async_remote_copy(
            src_ref=land.at[ctx],
            dst_ref=land.at[source],
            send_sem=l_s.at[j - 1],
            recv_sem=l_r.at[source],
            device_id={"ctx": source},
            device_id_type=MESH,
        )
        copy.wait_send()
        copy.wait_recv()
        return carry

    def row_half(way):
        return pl.ds(way * (rows // 2), rows // 2)

    def relay(way):
        owner = mate(nz - 1 if way == 0 else 1, core)
        view = gfull.at[row_half(way), shard(owner)]
        return pltpu.make_async_remote_copy(
            src_ref=view,
            dst_ref=view,
            send_sem=h_s.at[way],
            recv_sem=h_r.at[way],
            device_id={"tp": mate(1 if way == 0 else nz - 1, core)},
            device_id_type=MESH,
        )

    def relay_wait(way):
        view = gfull.at[row_half(way), shard(mate(2, core))]
        pltpu.make_async_remote_copy(
            src_ref=view,
            dst_ref=view,
            send_sem=h_s.at[way],
            recv_sem=h_r.at[way],
            device_id={"tp": mate(nz - 1 if way == 0 else 1, core)},
            device_id_type=MESH,
        ).wait_recv()

    lax.fori_loop(1, nctx, land_wait, 0)
    send_tokens(1)
    send_tokens(3)
    send_tokens(2)
    forwards = []

    def pass_shard(owner, slot):
        onward = grad_copy(gfull.at[:, shard(owner)], owner, f_s.at[slot], partner)
        onward.start()
        forwards.append(onward)

    for way in range(2):
        owner = mate(nz - 1 if way == 0 else 1, core)
        grad_copy(gfull.at[:, shard(owner)], owner, f_s.at[way], partner).wait_recv()
        relay(way).start()
        pass_shard(owner, way)


    own_strips = [
        pltpu.make_async_copy(
            tok.at[:, strip_at(i * nx + x)], tx_o.at[x, :, strip_at(i)], t_l.at[i]
        )
        for i in range(ny)
    ]
    own_strips.append(
        pltpu.make_async_copy(
            tok.at[:, pl.ds(pl.multiple_of(y * nx * strip, strip), nx * strip)],
            ty_o.at[y],
            t_l.at[ny],
        )
    )
    for copy in own_strips:
        copy.start()

    b = iota((all_blocks, nctx * per), 0)
    c = iota((all_blocks, nctx * per), 1)
    shift = b // own_blocks * own_blocks
    landed = land[...].reshape(nctx * per, cols)
    lk[...] = dot_nn(one_hot(c == b + shift), landed).astype(BF)
    lv[...] = dot_nn(one_hot(c == b + shift + own_blocks), landed).astype(BF)

    span = PAIR + all_blocks
    doc = doc_ref[...]
    doc_lane = iota(doc.shape, 1)
    doc_wide = jnp.concatenate([jnp.zeros((1, PAIR), jnp.int32), doc], axis=1)

    def forward(sb, carry):
        at = pl.ds(pl.multiple_of(sb * PAIR, PAIR), PAIR)
        row = iota((PAIR, span), 0)
        col = iota((PAIR, span), 1)
        upper = jnp.where(row >= BLOCK, 1, 0)
        col_upper = jnp.where(col >= BLOCK, 1, 0)
        first = ctx * own_blocks + sb * 2
        doc_a = jnp.sum(jnp.where(doc_lane == first, doc, 0), axis=1, keepdims=True)
        doc_b = jnp.sum(jnp.where(doc_lane == first + 1, doc, 0), axis=1, keepdims=True)
        own_doc = jnp.where(row >= BLOCK, doc_b, doc_a)
        near = (col < PAIR) & (upper == col_upper) & (col <= row)
        far = (col >= PAIR) & (col - PAIR < first + upper) & (doc_wide == own_doc)
        mask = near | far
        for h in range(heads):
            hs = pl.ds(h * HDIM, HDIM)
            keys = jnp.concatenate([qkv[0, at, hs], lk[:, hs]], axis=0)
            values = jnp.concatenate([qkv[1, at, hs], lv[:, hs]], axis=0)
            scores = dot_nt(qkv[2, at, hs], keys) * scale
            scores = jnp.where(mask, scores, big_negative)
            top = jnp.max(scores, axis=1, keepdims=True)
            e = jnp.exp(scores - top)
            weight = (e / jnp.sum(e, axis=1, keepdims=True)).astype(BF)
            pw[sb * heads + h] = weight
            attn[at, hs] = dot_nn(weight, values).astype(BF)
        return carry

    lax.fori_loop(0, rows // PAIR, forward, 0)
    load_wo.wait()

    def out_chunk(t):
        return dot_nn(attn[...], wo[:, shard(t)])

    summed_over_heads(ntp, out_chunk, o_p, o_q, o_z, o_a, op_s, op_r, oz_s, oz_r)
    load_go.wait()

    def use_chip(hop, fresh):
        chip = lax.rem(z + hop, nz)
        both = pl.ds(pl.multiple_of(chip * 2 * cols, 2 * cols), 2 * cols)
        grads = gfull[:, both]
        product = dot_nt(grads, wo[:, both])
        if fresh:
            acc[...] = product
        else:
            acc[...] += product
        part = dot_tn(attn[...], grads).astype(BF)
        each = 2 * (nctx // ntp)
        for k in range(each):
            i = chip * each + k
            there_y = lax.div(i, nx)
            there_x = lax.rem(i, nx)
            wos[0, there_x, there_y] = part[: cols // 2, k * strip : (k + 1) * strip]
            wos[1, there_y, there_x] = part[cols // 2 :, k * strip : (k + 1) * strip]

    def other_core(hop, slot):
        t = mate(hop, 1 - core)
        grad_copy(gfull.at[:, shard(t)], t, f_s.at[slot], partner).wait_recv()

    other_core(0, 0)
    use_chip(0, True)

    def use_near(i, carry):
        hop = 1 + (nz - 2) * i
        other_core(hop, 0)
        use_chip(hop, False)
        return carry

    lax.fori_loop(0, 2, use_near, 0)
    for way in range(2):
        relay_wait(way)
    pass_shard(mate(2, core), 2)
    other_core(2, 2)
    use_chip(2, False)
    da[...] = acc[...].astype(BF)
    out_wos = pltpu.make_async_copy(wos, wos_o, st.at[4])
    out_wos.start()
    rings = ((x, nx, lambda i: {"ctx": y * nx + i}), (y, ny, lambda i: {"ctx": i * nx + x}))
    subs = (pl.ds(0, nx // 2), pl.ds(nx // 2, nx // 2))

    def far_hop(side, way):
        pos, n, at = rings[side]
        return remote(
            wos.at[side, lax.rem(pos + 2, n), subs[way]],
            wfar_o.at[side, subs[way]],
            w0_s.at[side, way],
            w0_r.at[side, way],
            at(lax.rem(pos + (1 if way == 0 else n - 1), n)),
        )

    def near_hop(side, way):
        pos, n, at = rings[side]
        there = lax.rem(pos + (1 if way == 0 else n - 1), n)
        return remote(
            wos.at[side, there, subs[1 - way]],
            wr_o.at[side, way, subs[1 - way]],
            w1_s.at[side, way],
            w1_r.at[side, way],
            at(there),
        )

    for way in range(2):
        for side in range(2):
            far_hop(side, way).start()

    dlk[...] = jnp.zeros_like(dlk)
    dlv[...] = jnp.zeros_like(dlv)

    def backward(sb, carry):
        at = pl.ds(pl.multiple_of(sb * PAIR, PAIR), PAIR)
        for h in range(heads):
            hs = pl.ds(h * HDIM, HDIM)
            keys = jnp.concatenate([qkv[0, at, hs], lk[:, hs]], axis=0)
            values = jnp.concatenate([qkv[1, at, hs], lv[:, hs]], axis=0)
            weight = pw[sb * heads + h]
            d_out = da[at, hs]
            delta = jnp.sum(
                attn[at, hs].astype(F32) * d_out.astype(F32), axis=1, keepdims=True
            )
            d_weight = dot_nt(d_out, values)
            ds = (weight.astype(F32) * (d_weight - delta)).astype(BF)
            dqv[at, hs] = (dot_nn(ds, keys) * scale).astype(BF)
            d_keys = dot_tn(ds, qkv[2, at, hs]) * scale
            d_values = dot_tn(weight, d_out)
            dkf[at, hs] = d_keys[:PAIR]
            dvf[at, hs] = d_values[:PAIR]
            dlk[:, hs] += d_keys[PAIR:]
            dlv[:, hs] += d_values[PAIR:]
        return carry

    lax.fori_loop(0, rows // PAIR, backward, 0)
    out_dq = pltpu.make_async_copy(dqv, dq_o, st.at[1])
    out_dq.start()

    r = iota((nctx * per, all_blocks), 0)
    b = iota((nctx * per, all_blocks), 1)
    shift = b // own_blocks * own_blocks
    packed = dot_nn(one_hot(r == b + shift), dlk[...].astype(BF)) + dot_nn(
        one_hot(r == b + shift + own_blocks), dlv[...].astype(BF)
    )
    dls[...] = packed.astype(BF).reshape(nctx, per, cols)

    def give(j, carry):
        target = lax.rem(ctx + j, nctx)
        pltpu.make_async_remote_copy(
            src_ref=dls.at[target],
            dst_ref=dlr.at[ctx],
            send_sem=d_s.at[j - 1],
            recv_sem=d_r.at[ctx],
            device_id={"ctx": target},
            device_id_type=MESH,
        ).start()
        return carry

    lax.fori_loop(1, nctx, give, 0)
    for way in range(2):
        for side in range(2):
            near_hop(side, way).start()
    dlr[ctx] = dls[ctx]

    for j in range(1, nx):
        owner = lax.rem(x + j, nx)
        for i in range(ny):
            x_copy(j, i, owner).wait_recv()
        pass_on(tx_o, owner, fx_s.at[j - 1], fx_r.at[j - 1]).start()
    for j in range(1, ny):
        owner = lax.rem(y + j, ny)
        y_copy(j, owner).wait_recv()
        pass_on(ty_o, owner, fy_s.at[j - 1], fy_r.at[j - 1]).start()

    def take(j, carry):
        source = lax.rem(ctx + j, nctx)
        copy = pltpu.make_async_remote_copy(
            src_ref=dls.at[source],
            dst_ref=dlr.at[source],
            send_sem=d_s.at[j - 1],
            recv_sem=d_r.at[source],
            device_id={"ctx": source},
            device_id_type=MESH,
        )
        copy.wait_send()
        copy.wait_recv()
        return carry

    lax.fori_loop(1, nctx, take, 0)
    total = jnp.zeros((per, cols), F32)
    for i in range(nctx):
        total = total + dlr[i].astype(F32)
    for i in range(own_blocks):
        last = pl.ds(i * BLOCK + BLOCK - 1, 1)
        dkf[last, :] += total[i : i + 1]
        dvf[last, :] += total[own_blocks + i : own_blocks + i + 1]
    dkv[...] = dkf[...].astype(BF)
    dvv[...] = dvf[...].astype(BF)
    out_dk = pltpu.make_async_copy(dkv, dk_o, st.at[2])
    out_dk.start()
    out_dv = pltpu.make_async_copy(dvv, dv_o, st.at[3])
    out_dv.start()
    outv[...] = (
        tok[:, shard(tp)].astype(F32) + from_heads(ntp, o_p, o_z, o_a, oz_s, oz_r)
    ).astype(BF)
    out_out = pltpu.make_async_copy(outv, out_o, st.at[5])
    out_out.start()
    for way in range(2):
        for side in range(2):
            for copy in (far_hop(side, way), near_hop(side, way)):
                copy.wait_send()
                copy.wait_recv()
    for send in first_sends + forwards + [relay(0), relay(1)]:
        send.wait_send()
    for copy in [out_out, out_dq, out_dk, out_dv, out_wos] + own_strips:
        copy.wait()
    for j in range(1, nx):
        for i in range(ny):
            x_copy(j, i, x).wait_send()
        passed = pass_on(tx_o, lax.rem(x + j, nx), fx_s.at[j - 1], fx_r.at[j - 1])
        passed.wait_send()
        other_half = pl.ds(pl.multiple_of((1 - core) * (rows // 2), rows // 2), rows // 2)
        pltpu.make_async_remote_copy(
            src_ref=tx_o.at[lax.rem(x + j, nx), other_half],
            dst_ref=tx_o.at[lax.rem(x + j, nx), other_half],
            send_sem=fx_s.at[j - 1],
            recv_sem=fx_r.at[j - 1],
            device_id={"tp": partner},
            device_id_type=MESH,
        ).wait_recv()
    for j in range(1, ny):
        y_copy(j, y).wait_send()
        passed = pass_on(ty_o, lax.rem(y + j, ny), fy_s.at[j - 1], fy_r.at[j - 1])
        passed.wait_send()
        other_half = pl.ds(pl.multiple_of((1 - core) * (rows // 2), rows // 2), rows // 2)
        pltpu.make_async_remote_copy(
            src_ref=ty_o.at[lax.rem(y + j, ny), other_half],
            dst_ref=ty_o.at[lax.rem(y + j, ny), other_half],
            send_sem=fy_s.at[j - 1],
            recv_sem=fy_r.at[j - 1],
            device_id={"tp": partner},
            device_id_type=MESH,
        ).wait_recv()


def attention_core(nctx, ntp, nx, tokens, w_query, w_key, w_value, w_out, block_doc, grad_out):
    rows, width = tokens.shape
    cols = w_query.shape[1]
    heads = cols // HDIM
    own_blocks = rows // BLOCK
    all_blocks = nctx * own_blocks
    per = 2 * own_blocks
    units = rows // PAIR * heads
    ny = nctx // nx
    small = jax.ShapeDtypeStruct((rows, cols), BF)
    hbm = pl.BlockSpec(memory_space=pl.ANY)
    dma = pltpu.SemaphoreType.DMA
    return pl.pallas_call(
        functools.partial(core_kernel, nctx, ntp, nx),
        out_shape=(
            small,
            small,
            small,
            small,
            jax.ShapeDtypeStruct((2, nx, ny, cols // 2, width // nctx), BF),
            jax.ShapeDtypeStruct((2, ny, cols // 2, width // nctx), BF),
            jax.ShapeDtypeStruct((2, 2, ny, cols // 2, width // nctx), BF),
            jax.ShapeDtypeStruct((nx, rows, width // nx), BF),
            jax.ShapeDtypeStruct((ny, rows, width // ny), BF),
        ),
        in_specs=[hbm] * 5 + [pl.BlockSpec(memory_space=pltpu.VMEM), hbm],
        out_specs=(hbm,) * 9,
        scratch_shapes=[
            pltpu.VMEM((rows, width), BF),
            pltpu.VMEM((3, width, cols), BF),
            pltpu.VMEM((cols, width), BF),
            pltpu.VMEM((3, rows, cols), BF),
            pltpu.VMEM((rows, width), BF),
            pltpu.VMEM((nctx, per, cols), BF),
            pltpu.VMEM((all_blocks, cols), BF),
            pltpu.VMEM((all_blocks, cols), BF),
            pltpu.VMEM((units, PAIR, PAIR + all_blocks), BF),
            pltpu.VMEM((rows, cols), BF),
            pltpu.VMEM((rows, cols), BF),
            pltpu.VMEM((rows, cols), BF),
            pltpu.VMEM((rows, cols), BF),
            pltpu.VMEM((rows, cols), BF),
            pltpu.VMEM((rows, cols), F32),
            pltpu.VMEM((rows, cols), F32),
            pltpu.VMEM((all_blocks, cols), F32),
            pltpu.VMEM((all_blocks, cols), F32),
            pltpu.VMEM((nctx, per, cols), BF),
            pltpu.VMEM((nctx, per, cols), BF),
            pltpu.VMEM((2, nx, ny, cols // 2, width // nctx), BF),
            pltpu.VMEM((rows, cols), F32),
            pltpu.VMEM((ntp // 2, rows, cols), BF),
            pltpu.VMEM((ntp // 2, rows, cols), BF),
            pltpu.VMEM((ntp // 2, rows, cols), BF),
            pltpu.VMEM((rows, cols), F32),
            pltpu.VMEM((rows, cols), BF),
            dma((6,)),
            dma((6,)),
            dma((ntp // 2,)),
            dma((ntp,)),
            dma((ntp // 2,)),
            dma((nctx - 1,)),
            dma((nctx,)),
            dma((nctx - 1,)),
            dma((nctx,)),
            dma((nx - 1, ny)),
            dma((nx, ny)),
            dma((ny - 1,)),
            dma((ny,)),
            dma((ny + 1,)),
            dma((nx - 1,)),
            dma((nx - 1,)),
            dma((ny - 1,)),
            dma((ny - 1,)),
            dma((2,)),
            dma((2,)),
            dma((ntp // 2,)),
            dma((ntp // 2,)),
            dma((ntp // 2 - 1,)),
            dma((ntp // 2,)),
            dma((2, 2)),
            dma((2, 2)),
            dma((2, 2)),
            dma((2, 2)),
        ],
        compiler_params=pltpu.CompilerParams(
            collective_id=1, has_side_effects=True, vmem_limit_bytes=64 * 1024 * 1024 - 65536
        ),
        name="attention_core",
    )(tokens, w_query, w_key, w_value, w_out, block_doc.reshape(1, -1), grad_out)


def grad_kernel(
    nctx,
    ntp,
    nx,
    dq_h,
    dk_h,
    dv_h,
    wos_h,
    wfar_h,
    wr_h,
    tx_h,
    ty_h,
    wq_h,
    wk_h,
    wv_h,
    go_h,
    gt_o,
    gq_o,
    gk_o,
    gv_o,
    gwo_o,
    w3,
    dcat,
    rest_g,
    gq,
    gk,
    gvx,
    gvy,
    d_p,
    d_q,
    d_z,
    d_a,
    sq,
    sk,
    sv,
    rq,
    rk,
    rv,
    oq,
    ok,
    ov,
    wo_own,
    wo_nb,
    wo_far,
    wo_r,
    wo_t,
    wo_u,
    wo_a,
    ld,
    dl,
    ag_s,
    ag_r,
    dp_s,
    dp_r,
    dz_s,
    dz_r,
    rf_s,
    rf_r,
    rs_s,
    rs_r,
    w1_s,
    w1_r,
    w2_s,
    w2_r,
):
    ctx = lax.axis_index("ctx")
    tp = lax.axis_index("tp")
    ny = nctx // nx
    nz = ntp // 2
    y = lax.div(ctx, nx)
    x = lax.rem(ctx, nx)
    core = lax.rem(tp, 2)
    z = lax.div(tp, 2)
    partner = tp + 1 - 2 * core
    rows, cols = rest_g.shape
    width = w3.shape[0]
    strip = width // nctx
    gathered = nx * rows
    half = cols // 2

    def block(t):
        return pl.ds(pl.multiple_of(t * cols, cols), cols)

    def strip_at(i):
        return pl.ds(pl.multiple_of(i * strip, strip), strip)

    def at_x(i):
        return {"ctx": y * nx + i}

    def at_y(i):
        return {"ctx": i * nx + x}

    barrier = pltpu.get_barrier_semaphore()
    for j in range(1, nx):
        pl.semaphore_signal(
            barrier, inc=1, device_id=at_x(lax.rem(x + j, nx)), device_id_type=MESH
        )
    for j in range(1, ny):
        pl.semaphore_signal(
            barrier, inc=1, device_id=at_y(lax.rem(y + j, ny)), device_id_type=MESH
        )
    for j in range(1, nz):
        pl.semaphore_signal(
            barrier,
            inc=1,
            device_id={"tp": lax.rem(z + j, nz) * 2 + core},
            device_id_type=MESH,
        )
    pl.semaphore_signal(barrier, inc=1, device_id={"tp": partner}, device_id_type=MESH)

    loads = []
    for i, (d_h, w_h) in enumerate(((dq_h, wq_h), (dk_h, wk_h), (dv_h, wv_h))):
        lanes = pl.ds(i * cols, cols)
        loads.append(pltpu.make_async_copy(d_h, dcat.at[:, lanes], ld.at[2 + 2 * i]))
        loads.append(pltpu.make_async_copy(w_h, w3.at[:, lanes], ld.at[3 + 2 * i]))
    loads.append(pltpu.make_async_copy(go_h, rest_g, ld.at[9]))
    lo = pl.ds(0, half)
    hi = pl.ds(half, half)
    gathers = (
        (dq_h, gq, x, at_x, 0),
        (dk_h, gk, y, at_y, 1),
        (dv_h.at[:, lo], gvx, x, at_x, 2),
        (dv_h.at[:, hi], gvy, y, at_y, 3),
    )
    for source, buf, pos, at, i in gathers:
        loads.append(pltpu.make_async_copy(source, buf.at[pos], ld.at[10 + i]))
    rings = ((x, nx, at_x), (y, ny, at_y))
    for side in range(2):
        pos, n, at = rings[side]
        for k, target in ((0, wo_own), (1, wo_nb.at[:, 0]), (n - 1, wo_nb.at[:, 1])):
            loads.append(
                pltpu.make_async_copy(
                    wos_h.at[side, lax.rem(pos + k, n)],
                    target.at[side],
                    ld.at[14 + 3 * side + min(k, 2)],
                )
            )
    loads.append(pltpu.make_async_copy(wfar_h, wo_far, ld.at[0]))
    subs = (pl.ds(0, nx // 2), pl.ds(nx // 2, nx // 2))
    for side in range(2):
        for way in range(2):
            loads.append(
                pltpu.make_async_copy(
                    wr_h.at[side, way, subs[1 - way]],
                    wo_r.at[side, way, subs[1 - way]],
                    dl.at[side, way],
                )
            )
    for load in loads:
        load.start()

    pl.semaphore_wait(barrier, nx + ny + nz - 2)

    def near_send(gather, step):
        source, buf, pos, at, i = gather
        n = buf.shape[0]
        there = lax.rem(pos + (1 if step == 0 else n - 1), n)
        return remote(source, buf.at[pos], ag_s.at[i, step], ag_r.at[i, step], at(there))

    def near_recv(gather, step):
        source, buf, pos, at, i = gather
        n = buf.shape[0]
        owner = lax.rem(pos + (n - 1 if step == 0 else 1), n)
        return remote(source, buf.at[owner], ag_s.at[i, step], ag_r.at[i, step], at(owner))

    def relay(gather, step):
        source, buf, pos, at, i = gather
        n = buf.shape[0]
        part = pl.ds(0, rows // 2) if step == 0 else pl.ds(rows // 2, rows // 2)
        owner = lax.rem(pos + (n - 1 if step == 0 else 1), n)
        there = lax.rem(pos + (1 if step == 0 else n - 1), n)
        return remote(
            buf.at[owner, part],
            buf.at[owner, part],
            ag_s.at[i, 2 + step],
            ag_r.at[i, 2 + step],
            at(there),
        )

    def relay_recv(gather, step):
        source, buf, pos, at, i = gather
        n = buf.shape[0]
        part = pl.ds(0, rows // 2) if step == 0 else pl.ds(rows // 2, rows // 2)
        owner = lax.rem(pos + 2, n)
        return remote(
            buf.at[owner, part],
            buf.at[owner, part],
            ag_s.at[i, 2 + step],
            ag_r.at[i, 2 + step],
            at(owner),
        )

    for gather in gathers:
        near_send(gather, 0).start()
        near_send(gather, 1).start()

    def near_hop(side, way):
        pos, n, at = rings[side]
        part = subs[way]
        return remote(
            wo_nb.at[side, way, part],
            wo_r.at[side, way, part],
            w1_s.at[side, way],
            w1_r.at[side, way],
            at(lax.rem(pos + (1 if way == 0 else n - 1), n)),
        )

    def tok_chunk(t):
        return dot_nt(dcat[...], w3[block(t), :])

    for load in loads[:6]:
        load.wait()
    summed_over_heads(ntp, tok_chunk, d_p, d_q, d_z, d_a, dp_s, dp_r, dz_s, dz_r)
    t_x = w3.at[pl.ds(0, gathered), pl.ds(0, width // nx)]
    t_y = w3.at[pl.ds(gathered, gathered), pl.ds(0, width // ny)]
    late = []
    for i in range(nx):
        part = pl.ds(i * rows, rows)
        late.append(pltpu.make_async_copy(tx_h.at[i], t_x.at[part], ld.at[20 + i]))
        late.append(pltpu.make_async_copy(ty_h.at[i], t_y.at[part], ld.at[20 + nx + i]))
    for load in late:
        load.start()

    for gather in gathers:
        for step in range(2):
            near_recv(gather, step).wait_recv()
            relay(gather, step).start()

    for load in loads[6:] + late:
        load.wait()
    for side in range(2):
        for way in range(2):
            part = subs[way]
            wo_nb[side, way, part] = (
                wo_nb[side, way, part].astype(F32) + wo_far[side, part].astype(F32)
            ).astype(BF)
            near_hop(side, way).start()

    sends = (
        (gathers[0], 0, sq, rq, oq, y, at_y, 0),
        (gathers[1], 1, sk, rk, ok, x, at_x, 1),
        (gathers[2], 0, sv.at[:, :, lo], rv.at[:, :, lo], ov.at[:, lo], y, at_y, 2),
        (gathers[3], 1, sv.at[:, :, hi], rv.at[:, :, hi], ov.at[:, hi], x, at_x, 3),
    )
    ends = (pl.ds(0, strip // 2), pl.ds(strip // 2, strip // 2))

    def weight_far(item, way):
        gather, side, s, r, o, pos, at, i = item
        n = nx
        return remote(
            s.at[0, ends[way]],
            r.at[0, ends[way]],
            rf_s.at[i, way],
            rf_r.at[i, way],
            at(lax.rem(pos + (1 if way == 0 else n - 1), n)),
        )

    def weight_near(item, way, added):
        gather, side, s, r, o, pos, at, i = item
        n = nx
        part = ends[way if added else 1 - way]
        return remote(
            s.at[1 + way, part],
            r.at[1 + way, part],
            rs_s.at[i, way, 1 if added else 0],
            rs_r.at[i, way, 1 if added else 0],
            at(lax.rem(pos + (1 if way == 0 else n - 1), n)),
        )

    for item in sends:
        gather, side, s, r, o, pos, at, i = item
        for step in range(2):
            relay_recv(gather, step).wait_recv()
        buf = gather[1]
        n = buf.shape[0]
        base = pl.ds(side * gathered, gathered)

        def weight_piece(k, carry):
            there = lax.rem(pos + 6 - k, n)
            part = dot_tn(
                w3[base, strip_at(there)], buf[...].reshape(gathered, buf.shape[2])
            )

            @pl.when(k == 0)
            def _():
                s[0] = part.astype(BF)
                weight_far(item, 0).start()
                weight_far(item, 1).start()

            @pl.when(k == 1)
            def _():
                s[1] = part.astype(BF)
                weight_near(item, 0, False).start()

            @pl.when(k == 2)
            def _():
                o[...] = part

            @pl.when(k == 3)
            def _():
                s[2] = part.astype(BF)
                weight_near(item, 1, False).start()

            return carry

        lax.fori_loop(0, n, weight_piece, 0)

    for item in sends:
        gather, side, s, r, o, pos, at, i = item
        for way in range(2):
            weight_far(item, way).wait_recv()
            part = ends[way]
            s[1 + way, part] = (
                s[1 + way, part].astype(F32) + r[0, part].astype(F32)
            ).astype(BF)
            weight_near(item, way, True).start()

    gt_o[...] = (rest_g[...].astype(F32) + from_heads(ntp, d_p, d_z, d_a, dz_s, dz_r)).astype(BF)

    def second_hop(side, there, slot, owner):
        pos, n, at = ((y, ny, at_y), (x, nx, at_x))[side]
        return remote(
            wo_t.at[side, there],
            wo_u.at[side, owner],
            w2_s.at[side, slot],
            w2_r.at[side, owner],
            at(there),
        )

    for side in range(2):
        pos, m = ((y, ny), (x, nx))[side]
        for way in range(2):
            copy = near_hop(side, way)
            copy.wait_send()
            copy.wait_recv()

        def add_up(j, carry):
            there = lax.rem(pos + j, m)
            total = wo_own[side, there].astype(F32)
            for way in range(2):
                total = total + wo_r[side, way, there].astype(F32)

            @pl.when(j < m)
            def _():
                wo_t[side, there] = total.astype(BF)
                second_hop(side, there, j - 1, pos).start()

            @pl.when(j == m)
            def _():
                wo_a[pl.ds(side * half, half), :] = total

            return carry

        lax.fori_loop(1, m + 1, add_up, 0)

    for item, target in zip(sends, (gq_o, gk_o, gv_o.at[:, lo], gv_o.at[:, hi])):
        gather, side, s, r, o, pos, at, i = item
        for way in range(2):
            weight_far(item, way).wait_send()
            for added in (False, True):
                copy = weight_near(item, way, added)
                copy.wait_send()
                copy.wait_recv()
        target[...] = o[...] + r[1].astype(F32) + r[2].astype(F32)
        for step in range(2):
            near_send(gather, step).wait_send()
            relay(gather, step).wait_send()

    for side in range(2):
        pos, m = ((y, ny), (x, nx))[side]
        total = wo_a[pl.ds(side * half, half), :]
        for j in range(1, m):
            there = lax.rem(pos + j, m)
            copy = second_hop(side, there, j - 1, there)
            copy.wait_send()
            copy.wait_recv()
            total = total + wo_u[side, there].astype(F32)
        gwo_o[pl.ds(side * half, half), :] = total


def gradients(nctx, ntp, nx, core_out, w_query, w_key, w_value, grad_out):
    d_query, d_key, d_value, wos, wfar, wr, tx, ty = core_out
    rows = grad_out.shape[0]
    width = w_query.shape[0]
    cols = w_query.shape[1]
    ny = nctx // nx
    nz = ntp // 2
    strip = width // nctx
    half = cols // 2
    hbm = pl.BlockSpec(memory_space=pl.ANY)
    vmem = pl.BlockSpec(memory_space=pltpu.VMEM)
    dma = pltpu.SemaphoreType.DMA
    small = jax.ShapeDtypeStruct((rows, cols), BF)
    piece = jax.ShapeDtypeStruct((strip, cols), F32)
    heads_scratch = [
        pltpu.VMEM((nz, rows, cols), BF),
        pltpu.VMEM((nz, rows, cols), BF),
        pltpu.VMEM((nz, rows, cols), BF),
        pltpu.VMEM((rows, cols), F32),
    ]
    return pl.pallas_call(
        functools.partial(grad_kernel, nctx, ntp, nx),
        out_shape=(
            small,
            piece,
            piece,
            piece,
            jax.ShapeDtypeStruct((cols, strip), F32),
        ),
        in_specs=[hbm] * 12,
        out_specs=(vmem,) * 5,
        scratch_shapes=[
            pltpu.VMEM((width, 3 * cols), BF),
            pltpu.VMEM((rows, 3 * cols), BF),
            pltpu.VMEM((rows, cols), BF),
            pltpu.VMEM((nx, rows, cols), BF),
            pltpu.VMEM((ny, rows, cols), BF),
            pltpu.VMEM((nx, rows, half), BF),
            pltpu.VMEM((ny, rows, half), BF),
            *heads_scratch,
            pltpu.VMEM((3, strip, cols), BF),
            pltpu.VMEM((3, strip, cols), BF),
            pltpu.VMEM((3, strip, cols), BF),
            pltpu.VMEM((3, strip, cols), BF),
            pltpu.VMEM((3, strip, cols), BF),
            pltpu.VMEM((3, strip, cols), BF),
            pltpu.VMEM((strip, cols), F32),
            pltpu.VMEM((strip, cols), F32),
            pltpu.VMEM((strip, cols), F32),
            pltpu.VMEM((2, ny, half, strip), BF),
            pltpu.VMEM((2, 2, ny, half, strip), BF),
            pltpu.VMEM((2, ny, half, strip), BF),
            pltpu.VMEM((2, 2, ny, half, strip), BF),
            pltpu.VMEM((2, ny, half, strip), BF),
            pltpu.VMEM((2, ny, half, strip), BF),
            pltpu.VMEM((cols, strip), F32),
            dma((20 + nx + ny,)),
            dma((2, 2)),
            dma((4, 4)),
            dma((4, 4)),
            dma((nz,)),
            dma((nz,)),
            dma((nz - 1,)),
            dma((nz,)),
            dma((4, 2)),
            dma((4, 2)),
            dma((4, 2, 2)),
            dma((4, 2, 2)),
            dma((2, 2)),
            dma((2, 2)),
            dma((2, nx - 1)),
            dma((2, nx)),
        ],
        compiler_params=pltpu.CompilerParams(
            collective_id=2, has_side_effects=True, vmem_limit_bytes=64 * 1024 * 1024 - 65536
        ),
        name="gradients",
    )(
        d_query,
        d_key,
        d_value,
        wos,
        wfar,
        wr,
        tx,
        ty,
        w_query,
        w_key,
        w_value,
        grad_out,
    )


def settle_kernel(count, *refs):
    ins, outs, bufs = refs[:count], refs[count : 2 * count], refs[2 * count : 3 * count]
    come, go = refs[3 * count :]
    first = [pltpu.make_async_copy(ins[i], bufs[i], come.at[i]) for i in range(count)]
    second = [pltpu.make_async_copy(bufs[i], outs[i], go.at[i]) for i in range(count)]
    for copy in first:
        copy.start()
    for i in range(count):
        first[i].wait()
        second[i].start()
    for copy in second:
        copy.wait()


def settled(arrays):
    count = len(arrays)
    hbm = pl.BlockSpec(memory_space=pl.ANY)
    shapes = [(a.shape, a.dtype) for a in arrays]
    return pl.pallas_call(
        functools.partial(settle_kernel, count),
        out_shape=tuple(jax.ShapeDtypeStruct(*s) for s in shapes),
        in_specs=[hbm] * count,
        out_specs=(hbm,) * count,
        scratch_shapes=[pltpu.VMEM(*s) for s in shapes]
        + [pltpu.SemaphoreType.DMA((count,)), pltpu.SemaphoreType.DMA((count,))],
        name="settled",
    )(*arrays)


def per_device(nctx, ntp, nx, tokens, w_query, w_key, w_value, w_out, block_doc, grad_out):
    out, *core_out = attention_core(
        nctx, ntp, nx, tokens, w_query, w_key, w_value, w_out, block_doc, grad_out
    )
    grads = gradients(nctx, ntp, nx, core_out, w_query, w_key, w_value, grad_out)
    return settled((out, *grads))


def solution(mesh):
    in_specs = (
        P("ctx", None),
        P(None, "tp"),
        P(None, "tp"),
        P(None, "tp"),
        P("tp", None),
        P(),
        P("ctx", "tp"),
    )
    out_specs = (
        P("ctx", "tp"),
        P("ctx", "tp"),
        P("ctx", "tp"),
        P("ctx", "tp"),
        P("ctx", "tp"),
        P("tp", "ctx"),
    )
    return jax.shard_map(
        functools.partial(per_device, mesh.shape["ctx"], mesh.shape["tp"], math.isqrt(mesh.shape["ctx"])),
        mesh=mesh,
        in_specs=in_specs,
        out_specs=out_specs,
        check_vma=False,
    )
```
